512 devices in a mesh: pix: 32 (over z_lo, y), mz: 16 (over z_hi, x, core).
Axes of the slice: x: 4, y: 4, z: 16 (z_hi: 2, z_lo: 8; z = z_hi * 8 + z_lo), core: 2. Of those that a mesh axis runs over, the one named last changes fastest.
Arguments:
- spectra: float32 [512, 393216], P('pix', 'mz'), may hold values from 0.05 to 5
- shifts: int32 [512, 192], P('pix', 'mz'), may hold values from -4 to 3
- fractions: float32 [512, 192], P('pix', 'mz'), may hold values from 0 to 1
- pixel_factors: float32 [512, 32], P('pix'), may hold values from 0.05 to 0.5
- spectral_factors: float32 [32, 393216], P(None, ('mz', 'pix')), may hold values from 0.05 to 0.5
Outputs:
- w_update: float32 [512, 32], P('pix')
- h_update: float32 [32, 393216], P(None, ('mz', 'pix'))
The draws below stay inside these ranges and needn't reach their ends.
All inputs are finite; a program needn't handle non-finite values.
Results may differ from the reference program's by a relative error of at most 0.0003.
Values sent between devices are 32-bit elements; how exact they have to be, the bound alone decides.
A program may use at most 64 MiB of HBM per device.

```python
import math
import jax
import jax.numpy as jnp
from jax import lax

P_DEV = 16
SEG = 2048
HALO = 4
RANK = 32
BINS = 393216
SEGS = 192
PIXELS = 512


def with_ends(drawn, key, low, largest):
    longest = drawn.shape.index(max(drawn.shape))
    spots = []
    for shift in (0, 1):
        where = [jax.random.randint(jax.random.fold_in(key, axis), (), 0, length) for axis, length in enumerate(drawn.shape)]
        where[longest] = (where[longest] + shift) % drawn.shape[longest]
        spots.append(tuple(where))
    return drawn.at[spots[0]].set(low).at[spots[1]].set(largest)


def block_scale(stream_key, extent, shards, low, top_value):
    def one(dim, shards_of):
        steps = jax.random.uniform(jax.random.fold_in(jax.random.fold_in(stream_key, 6), dim), (shards_of,), jnp.float32, low / len(shards), top_value / len(shards))
        return jnp.repeat(jnp.exp(steps), extent[dim] // shards_of).reshape((-1,) + (1,) * (len(extent) - dim - 1))

    loudness = one(*shards[0])
    for cut in shards[1:]:
        loudness = loudness * one(*cut)
    return loudness


def setup_inputs(seed: int = 0) -> dict:
    splits = jax.random.split(jax.random.key(seed), 6)
    return {
        "spectra": jnp.clip(jnp.exp(math.log(5.0) - 4.6051702 * jax.random.uniform(splits[0], (PIXELS, BINS), jnp.float32) ** block_scale(splits[0], (PIXELS, BINS), ((0, 32), (1, 16)), -0.2, 0.2)), 0.05, 5.0),
        "shifts": with_ends(jax.random.randint(splits[1], (PIXELS, SEGS), -HALO, HALO), jax.random.fold_in(splits[1], 1), -HALO, HALO - 1).astype(jnp.int32),
        "fractions": jnp.clip(1.0 * jax.random.uniform(splits[2], (PIXELS, SEGS), jnp.float32) ** block_scale(splits[2], (PIXELS, SEGS), ((0, 32), (1, 16)), -0.2, 0.2), 0.0, 1.0),
        "pixel_factors": jnp.clip(jnp.exp(math.log(0.5) - 2.3025851 * jax.random.uniform(splits[3], (PIXELS, RANK), jnp.float32) ** block_scale(splits[3], (PIXELS, RANK), ((0, 32),), -0.2, 0.2)), 0.05, 0.5),
        "spectral_factors": jnp.clip(jnp.exp(math.log(0.5) - 2.3025851 * jax.random.uniform(splits[4], (RANK, BINS), jnp.float32) ** block_scale(splits[4], (RANK, BINS), ((1, 512),), -0.2, 0.2)), 0.05, 0.5),
    }


EPSILON = 1e-6
exact_mode = lax.Precision.HIGHEST


def warp_block(spectra_rows, shift_rows, frac_rows):
    bin_count = spectra_rows.shape[1]
    bin_shift = jnp.repeat(shift_rows, SEG, axis=1)
    bin_frac = jnp.repeat(frac_rows, SEG, axis=1)
    padded = jnp.pad(spectra_rows, ((0, 0), (HALO, HALO)))
    source = jnp.arange(bin_count, dtype=jnp.int32)[None, :] + bin_shift.astype(jnp.int32) + HALO
    lower_term = jnp.take_along_axis(padded, source, axis=1)
    upper_term = jnp.take_along_axis(padded, source + 1, axis=1)
    return (1.0 - bin_frac) * lower_term + bin_frac * upper_term


def reference(spectra, shifts, fractions, pixel_factors, spectral_factors):
    pixel_total = spectra.shape[0]
    groups = pixel_total // P_DEV
    spec_blocks = spectra.reshape(groups, P_DEV, spectra.shape[1])
    shift_blocks = shifts.reshape(groups, P_DEV, shifts.shape[1])
    frac_blocks = fractions.reshape(groups, P_DEV, fractions.shape[1])
    factor_blocks = pixel_factors.reshape(groups, P_DEV, RANK)

    def accumulate(totals, inputs):
        spectra_rows, shift_rows, frac_rows, factor_rows = inputs
        warped = warp_block(spectra_rows, shift_rows, frac_rows)
        numer = totals[0] + jnp.dot(factor_rows.T, warped, precision=exact_mode)
        gram = totals[1] + jnp.dot(factor_rows.T, factor_rows, precision=exact_mode)
        return (numer, gram), None

    start_totals = (jnp.zeros((RANK, spectra.shape[1]), spectra.dtype), jnp.zeros((RANK, RANK), spectra.dtype))
    (numerator, pixel_gram), _ = lax.scan(accumulate, start_totals, (spec_blocks, shift_blocks, frac_blocks, factor_blocks))
    h_update = spectral_factors * numerator / (jnp.dot(pixel_gram, spectral_factors, precision=exact_mode) + EPSILON)

    def project(unused, inputs):
        spectra_rows, shift_rows, frac_rows = inputs
        warped = warp_block(spectra_rows, shift_rows, frac_rows)
        return unused, jnp.dot(warped, h_update.T, precision=exact_mode)

    _, proj_blocks = lax.scan(project, jnp.zeros((), spectra.dtype), (spec_blocks, shift_blocks, frac_blocks))
    proj_sum = proj_blocks.reshape(pixel_total, RANK)
    gram_sum = jnp.dot(h_update, h_update.T, precision=exact_mode)
    w_update = pixel_factors * proj_sum / (jnp.dot(pixel_factors, gram_sum, precision=exact_mode) + EPSILON)
    return w_update, h_update
```

```python
import jax
import jax.numpy as jnp
from jax import lax
from jax.experimental import pallas as pl
from jax.experimental.pallas import tpu as pltpu
from jax.sharding import PartitionSpec as P

SEG = 2048
RANK = 32
EPSILON = 1e-06
ROWS = 16
BINS = 24576
SEGS = BINS // SEG
NZ, NY = 8, 4
OWN = 768
PW = 256
NPZ = OWN // PW
NP = NZ * NPZ
GROUP = NY * ROWS
AHEAD = 10
LAGS = (3, 10, 17, 24)
MESH = pl.DeviceIdType.MESH
F32 = jnp.float32
BF16 = jnp.bfloat16
exact_mode = lax.Precision.HIGHEST
NT = (((1,), (1,)), ((), ()))


def halves(v):
    hi = v.astype(BF16)
    return hi, (v - hi.astype(F32)).astype(BF16)


def kernel(
    x_hbm, sh_ref, fr_ref, f_ref, hin_ref, w_ref, hout_ref,
    xp, shb, frb, ws, wg, wgb, cbuf, cout, hbuf, hc, rbuf, fbuf, lhs, gsend, gbuf, acc,
    t1s, t1r, t2s, t2r, t3s, t3r,
    xsem, halo_s, halo_r, f_s, f_r, hc_s, hc_r, g_s, g_r,
    y_s, y_r, c_s, c_r, h_s, h_r, t1_s, t1_r, t2_s, t2_r, t3_s, t3_r,
):
    p, m = lax.axis_index("pix"), lax.axis_index("mz")
    z, y = lax.div(p, NY), lax.rem(p, NY)
    mh, ml = lax.div(m, 8), lax.rem(m, 8)
    low_side = z < NZ // 2
    inner = jnp.where(low_side, p + NY, p - NY)
    outer = jnp.where(low_side, p - NY, p + NY)
    depth = jnp.where(low_side, NZ // 2 - 1 - z, z - NZ // 2)
    center = depth == 0
    slot = jnp.where(center, 1, 0)
    has_outer = depth < NZ // 2 - 1
    lag = jnp.where(
        depth == 0, LAGS[0], jnp.where(depth == 1, LAGS[1], jnp.where(depth == 2, LAGS[2], LAGS[3]))
    )

    def y_dev(r):
        return (z * NY + lax.rem(y + r, NY), m)

    def m_dev(r):
        return (p, mh * 8 + lax.rem(ml + r, 8))

    far = (p, lax.rem(m + 8, 16))

    def rcopy(src, dst, send, recv, dev):
        return pltpu.make_async_remote_copy(
            src_ref=src, dst_ref=dst, send_sem=send, recv_sem=recv, device_id=dev, device_id_type=MESH
        )

    xcopy = pltpu.make_async_copy(x_hbm, xp.at[:, pl.ds(128, BINS)], xsem)
    xcopy.start()

    barrier = pltpu.get_barrier_semaphore()

    def greet(dev):
        pl.semaphore_signal(barrier, inc=1, device_id=dev, device_id_type=MESH)

    for r in range(1, NY):
        greet(y_dev(r))
    for r in range(1, NZ):
        greet((lax.rem(z + r, NZ) * NY + y, m))
    for r in range(1, 8):
        greet(m_dev(r))
    greet(far)

    @pl.when(m == 7)
    def _():
        greet((p, 8))

    @pl.when(m == 8)
    def _():
        greet((p, 7))

    for s in range(SEGS):
        shb[s] = jnp.broadcast_to(sh_ref[:, s : s + 1], (ROWS, 128))
        frb[s] = jnp.broadcast_to(fr_ref[:, s : s + 1], (ROWS, 128))
    acc[...] = jnp.zeros_like(acc)
    fbuf[y] = f_ref[...]

    @pl.when(m == 0)
    def _():
        xp[:, 0:128] = jnp.zeros((ROWS, 128), F32)

    @pl.when(m == 15)
    def _():
        xp[:, 128 + BINS :] = jnp.zeros((ROWS, 128), F32)

    pl.semaphore_wait(barrier, jnp.where((m == 7) | (m == 8), NY + NZ + 7, NY + NZ + 6))

    f_copies = [
        rcopy(f_ref, fbuf.at[y], f_s.at[r - 1], f_r.at[r - 1], y_dev(r)) for r in range(1, NY)
    ]
    for c in f_copies:
        c.start()
    xcopy.wait()

    to_right = rcopy(
        xp.at[:, pl.ds(BINS, 128)], xp.at[:, pl.ds(0, 128)], halo_s.at[0], halo_r.at[0], (p, m + 1)
    )
    to_left = rcopy(
        xp.at[:, pl.ds(128, 128)], xp.at[:, pl.ds(128 + BINS, 128)], halo_s.at[1], halo_r.at[1], (p, m - 1)
    )

    @pl.when(m < 15)
    def _():
        to_right.start()

    @pl.when(m > 0)
    def _():
        to_left.start()

    def h_part(c, j):
        t = z * NPZ + j
        return rcopy(
            hin_ref.at[:, pl.ds(j * PW, PW)], hc.at[t], hc_s.at[c, j], hc_r.at[t], ((3 + c) * NY + y, m)
        )

    for c in range(2):

        @pl.when(z != 3 + c)
        def _():
            for j in range(NPZ):
                h_part(c, j).start()

        @pl.when(z == 3 + c)
        def _():
            for j in range(NPZ):
                hc[z * NPZ + j] = hin_ref[:, j * PW : (j + 1) * PW]

    def piece(i):
        return lax.rem(i + NPZ, NP)

    def y_copy(r, t):
        return rcopy(ws.at[r - 1, t], wg.at[t, y], y_s.at[r - 1], y_r.at[t, r - 1], y_dev(r))

    def warp_send(i):
        t = piece(i)
        zq, j = lax.div(t, NPZ), lax.rem(t, NPZ)
        for r in range(NY):
            b = zq * (NY * OWN) + lax.rem(y + r, NY) * OWN + j * PW
            v = xp[:, pl.ds(pl.multiple_of(b, 128), PW + 256)]
            s = lax.div(b, SEG)
            reps = (PW + 256) // 128
            d = jnp.concatenate([shb[s]] * reps, axis=1)
            f = jnp.concatenate([frb[s]] * (PW // 128), axis=1)
            width = PW + 256
            v = jnp.where(d < 0, pltpu.roll(v, 4, 1), v)
            v = jnp.where((d & 2) != 0, pltpu.roll(v, width - 2, 1), v)
            v = jnp.where((d & 1) != 0, pltpu.roll(v, width - 1, 1), v)
            lower = v[:, 128 : 128 + PW]
            upper = pltpu.roll(v, width - 1, 1)[:, 128 : 128 + PW]
            out = (1.0 - f) * lower + f * upper
            if r == 0:
                wg[t, y] = out
            else:
                ws[r - 1, t] = out
        for r in range(1, NY):
            y_copy(r, t).start()

    def ahead(i, carry):
        warp_send(i)
        return carry

    lax.fori_loop(0, AHEAD, ahead, 0)

    for c in f_copies:
        c.wait_recv()
    fg = fbuf[...].reshape(GROUP, RANK)
    gy = lax.dot_general(fg, fg, (((0,), (0,)), ((), ())), precision=exact_mode, preferred_element_type=F32)
    gsend[...] = gy
    f_hi, f_lo = halves(fg.T)
    lhs[...] = jnp.concatenate([f_hi, f_hi, f_lo], axis=1)

    def g_part(c):
        return rcopy(gsend, gbuf.at[z], g_s.at[c], g_r.at[z], ((3 + c) * NY + y, m))

    for c in range(2):

        @pl.when(z != 3 + c)
        def _():
            g_part(c).start()

        @pl.when(z == 3 + c)
        def _():
            gbuf[z] = gy

    def c_copy(t):
        return rcopy(cout.at[t], cbuf.at[slot, t], c_s, c_r.at[slot, t], (inner, m))

    def c_wait(s, t):
        rcopy(cout.at[t], cbuf.at[s, t], c_s, c_r.at[s, t], (inner, m)).wait_recv()

    def h_copy(t):
        return rcopy(hbuf.at[t], hbuf.at[t], h_s, h_r.at[t], (outer, m))

    def step(i, carry):
        @pl.when(i + AHEAD < NP)
        def _():
            @pl.when(i + AHEAD == NP - NPZ - 1)
            def _():
                @pl.when(m > 0)
                def _():
                    to_right.wait_recv()

                @pl.when(m < 15)
                def _():
                    to_left.wait_recv()

            warp_send(i + AHEAD)

        @pl.when(i < NP)
        def _():
            t = piece(i)
            for r in range(1, NY):
                y_copy(r, t).wait_recv()
            w_hi, w_lo = halves(wg[t].reshape(GROUP, PW))
            both = jnp.concatenate([w_hi, w_lo], axis=0)
            wgb[t] = both
            n = jnp.dot(lhs[...], jnp.concatenate([both, w_hi], axis=0), preferred_element_type=F32)

            @pl.when(has_outer)
            def _():
                c_wait(0, t)
                cout[t] = n + cbuf[0, t]

            @pl.when(jnp.logical_not(has_outer))
            def _():
                cout[t] = n

            c_copy(t).start()

            @pl.when(center)
            def _():
                @pl.when(i == 0)
                def _():
                    for k in range(NZ):

                        @pl.when(z != k)
                        def _():
                            rcopy(gsend, gbuf.at[k], g_s.at[0], g_r.at[k], (inner, m)).wait_recv()

                    total = gbuf[0]
                    for k in range(1, NZ):
                        total = total + gbuf[k]
                    gsum = total
                    gsend_total(gsum)

                @pl.when(lax.div(t, NPZ) != z)
                def _():
                    rcopy(hc.at[t], hc.at[t], hc_s.at[0, 0], hc_r.at[t], (inner, m)).wait_recv()

                own = hc[t]
                bottom = jnp.dot(gbuf[NZ], own, precision=exact_mode, preferred_element_type=F32) + EPSILON
                rbuf[t] = own / bottom

        k = i - lag

        @pl.when((k >= 0) & (k < NP))
        def _():
            t = piece(k)

            @pl.when(center)
            def _():
                c_wait(1, t)
                hbuf[t] = rbuf[t] * (cout[t] + cbuf[1, t])

            @pl.when(jnp.logical_not(center))
            def _():
                h_copy(t).wait_recv()

            @pl.when(has_outer)
            def _():
                h_copy(t).start()

            h = hbuf[t]
            h_hi, h_lo = halves(h)
            right = jnp.concatenate([h_hi, h_lo], axis=0)
            left = jnp.concatenate([wgb[t], right], axis=0)
            acc[...] += lax.dot_general(left, right, NT, preferred_element_type=F32)

            @pl.when(lax.div(t, NPZ) == z)
            def _():
                hout_ref[:, pl.ds(pl.multiple_of(lax.rem(t, NPZ) * PW, 128), PW)] = h

        return carry

    def gsend_total(total):
        gbuf[NZ] = total

    lax.fori_loop(0, NP + LAGS[-1], step, 0)

    both = acc[:, 0:RANK] + acc[:, RANK : 2 * RANK]
    proj = both[0:GROUP] + both[GROUP : 2 * GROUP]
    base = 2 * GROUP
    gram = both[base : base + RANK] + both[base + RANK : base + 2 * RANK]
    for k in range(NY):
        t1s[k] = jnp.concatenate(
            [proj[k * ROWS : (k + 1) * ROWS], gram[0:ROWS], gram[ROWS : 2 * ROWS], jnp.zeros((ROWS, 32), F32)],
            axis=1,
        )
    t1_copies = [
        rcopy(t1s.at[lax.rem(y + r, NY)], t1r.at[y], t1_s.at[r - 1], t1_r.at[r - 1], y_dev(r))
        for r in range(1, NY)
    ]
    for c in t1_copies:
        c.start()
    t1r[y] = t1s[y]
    for c in t1_copies:
        c.wait_recv()
    part = t1r[0]
    for k in range(1, NY):
        part = part + t1r[k]
    t2s[...] = part
    t2_copies = [
        rcopy(t2s, t2r.at[ml], t2_s.at[r - 1], t2_r.at[r - 1], m_dev(r)) for r in range(1, 8)
    ]
    for c in t2_copies:
        c.start()
    t2r[ml] = part
    for c in t2_copies:
        c.wait_recv()
    part = t2r[0]
    for k in range(1, 8):
        part = part + t2r[k]
    t3s[...] = part
    t3_copy = rcopy(t3s, t3r, t3_s, t3_r, far)
    t3_copy.start()
    t3_copy.wait_recv()
    total = part + t3r[...]
    gram_sum = jnp.concatenate([total[:, 32:64], total[:, 64:96]], axis=0)
    f = f_ref[...]
    bottom = jnp.dot(f, gram_sum, precision=exact_mode, preferred_element_type=F32) + EPSILON
    w_ref[...] = f * total[:, 0:32] / bottom

    for c in f_copies + t1_copies + t2_copies + [t3_copy]:
        c.wait_send()

    @pl.when(m < 15)
    def _():
        to_right.wait_send()

    @pl.when(m > 0)
    def _():
        to_left.wait_send()

    for c in range(2):

        @pl.when(z != 3 + c)
        def _():
            for j in range(NPZ):
                h_part(c, j).wait_send()
            g_part(c).wait_send()

    for r in range(1, NY):
        rcopy(ws.at[r - 1], ws.at[r - 1], y_s.at[r - 1], y_s.at[r - 1], y_dev(r)).wait_send()
    rcopy(cout, cout, c_s, c_s, (inner, m)).wait_send()

    @pl.when(has_outer)
    def _():
        rcopy(hbuf, hbuf, h_s, h_s, (outer, m)).wait_send()


def body(spectra, shifts, fractions, pixel_factors, spectral_factors):
    vmem = pl.BlockSpec(memory_space=pltpu.VMEM)
    dma = pltpu.SemaphoreType.DMA
    return pl.pallas_call(
        kernel,
        out_shape=(
            jax.ShapeDtypeStruct((ROWS, RANK), F32),
            jax.ShapeDtypeStruct((RANK, OWN), F32),
        ),
        in_specs=[pl.BlockSpec(memory_space=pl.ANY)] + [vmem] * 4,
        out_specs=(vmem, vmem),
        scratch_shapes=[
            pltpu.VMEM((ROWS, BINS + 256), F32),
            pltpu.VMEM((SEGS, ROWS, 128), jnp.int32),
            pltpu.VMEM((SEGS, ROWS, 128), F32),
            pltpu.VMEM((NY - 1, NP, ROWS, PW), F32),
            pltpu.VMEM((NP, NY, ROWS, PW), F32),
            pltpu.VMEM((NP, 2 * GROUP, PW), BF16),
            pltpu.VMEM((2, NP, RANK, PW), F32),
            pltpu.VMEM((NP, RANK, PW), F32),
            pltpu.VMEM((NP, RANK, PW), F32),
            pltpu.VMEM((NP, RANK, PW), F32),
            pltpu.VMEM((NP, RANK, PW), F32),
            pltpu.VMEM((NY, ROWS, RANK), F32),
            pltpu.VMEM((RANK, 3 * GROUP), BF16),
            pltpu.VMEM((RANK, RANK), F32),
            pltpu.VMEM((NZ + 1, RANK, RANK), F32),
            pltpu.VMEM((2 * GROUP + 2 * RANK, 2 * RANK), F32),
            pltpu.VMEM((NY, ROWS, 128), F32),
            pltpu.VMEM((NY, ROWS, 128), F32),
            pltpu.VMEM((ROWS, 128), F32),
            pltpu.VMEM((8, ROWS, 128), F32),
            pltpu.VMEM((ROWS, 128), F32),
            pltpu.VMEM((ROWS, 128), F32),
            dma(()),
            dma((2,)),
            dma((2,)),
            dma((NY - 1,)),
            dma((NY - 1,)),
            dma((2, NPZ)),
            dma((NP,)),
            dma((2,)),
            dma((NZ,)),
            dma((NY - 1,)),
            dma((NP, NY - 1)),
            dma(()),
            dma((2, NP)),
            dma(()),
            dma((NP,)),
            dma((NY - 1,)),
            dma((NY - 1,)),
            dma((7,)),
            dma((7,)),
            dma(()),
            dma(()),
        ],
        compiler_params=pltpu.CompilerParams(
            collective_id=0, has_side_effects=True, vmem_limit_bytes=48 * 1024 * 1024
        ),
    )(spectra, shifts, fractions, pixel_factors, spectral_factors)


def solution(mesh):
    return jax.shard_map(
        body,
        mesh=mesh,
        in_specs=(
            P("pix", "mz"),
            P("pix", "mz"),
            P("pix", "mz"),
            P("pix", None),
            P(None, ("mz", "pix")),
        ),
        out_specs=(P("pix", None), P(None, ("mz", "pix"))),
        check_vma=False,
    )
```

```python
import jax
import jax.numpy as jnp
from jax import lax
from jax.experimental import pallas as pl
from jax.experimental.pallas import tpu as pltpu
from jax.sharding import PartitionSpec as P

SEG = 2048
RANK = 32
EPSILON = 1e-06
ROWS = 16
BINS = 24576
SEGS = BINS // SEG
NZ, NY = 8, 4
OWN = 768
PW = 256
NPZ = OWN // PW
NP = NZ * NPZ
GROUP = NY * ROWS
FIRST = 14
AHEAD = 10
LAGS = (5, 13, 21, 24)
PEERS = 32
MESH = pl.DeviceIdType.MESH
F32 = jnp.float32
BF16 = jnp.bfloat16
exact_mode = lax.Precision.HIGHEST
NT = (((1,), (1,)), ((), ()))


def halves(v):
    hi = v.astype(BF16)
    return hi, (v - hi.astype(F32)).astype(BF16)


def kernel(
    x_hbm, sh_hbm, fr_hbm, f_hbm, hin_hbm, w_ref, hout_ref,
    sh_ref, fr_ref, f_ref, hin_ref,
    xp, shb, frb, ws, wg, wgb, cbuf, cout, hbuf, hc, rbuf, fbuf, lhs, gsend, gbuf, acc,
    t1s, t1r, t3s, t3r,
    xsem, halo_s, halo_r, f_s, f_r, hc_s, hc_r, g_s, g_r,
    y_s, y_r, c_s, c_r, h_s, h_r, t1_s, t1_r, t3_s, t3_r,
):
    p, m = lax.axis_index("pix"), lax.axis_index("mz")
    z, y = lax.div(p, NY), lax.rem(p, NY)
    mh, ml = lax.div(m, 8), lax.rem(m, 8)
    low_side = z < NZ // 2
    inner = jnp.where(low_side, p + NY, p - NY)
    outer = jnp.where(low_side, p - NY, p + NY)
    depth = jnp.where(low_side, NZ // 2 - 1 - z, z - NZ // 2)
    center = depth == 0
    slot = jnp.where(center, 1, 0)
    has_outer = depth < NZ // 2 - 1
    lag = jnp.where(
        depth == 0, LAGS[0], jnp.where(depth == 1, LAGS[1], jnp.where(depth == 2, LAGS[2], LAGS[3]))
    )

    def y_dev(r):
        return (z * NY + lax.rem(y + r, NY), m)

    def m_dev(r):
        return (p, mh * 8 + lax.rem(ml + r, 8))

    far = (p, lax.rem(m + 8, 16))

    def rcopy(src, dst, send, recv, dev):
        return pltpu.make_async_remote_copy(
            src_ref=src, dst_ref=dst, send_sem=send, recv_sem=recv, device_id=dev, device_id_type=MESH
        )

    loads = [
        pltpu.make_async_copy(a, b, xsem.at[k])
        for k, (a, b) in enumerate(
            (
                (sh_hbm, sh_ref),
                (fr_hbm, fr_ref),
                (x_hbm, xp.at[:, pl.ds(128, BINS)]),
                (f_hbm, f_ref),
                (hin_hbm, hin_ref),
            )
        )
    ]
    for c in loads:
        c.start()

    barrier = pltpu.get_barrier_semaphore()

    def greet(dev):
        pl.semaphore_signal(barrier, inc=1, device_id=dev, device_id_type=MESH)

    def plane_dev(k):
        return (
            z * NY + lax.rem(y + lax.div(k, 8), NY),
            mh * 8 + lax.rem(ml + lax.rem(k, 8), 8),
        )

    for k in range(1, PEERS):
        greet(plane_dev(k))
    half = lax.div(z, NZ // 2) * (NZ // 2)
    for r in range(1, NZ // 2):
        greet(((half + lax.rem(z + r, NZ // 2)) * NY + y, m))
    greet(far)

    @pl.when(center)
    def _():
        greet((inner, m))

    @pl.when(m == 7)
    def _():
        greet((p, 8))

    @pl.when(m == 8)
    def _():
        greet((p, 7))

    acc[...] = jnp.zeros_like(acc)

    @pl.when(m == 0)
    def _():
        xp[:, 0:128] = jnp.zeros((ROWS, 128), F32)

    @pl.when(m == 15)
    def _():
        xp[:, 128 + BINS :] = jnp.zeros((ROWS, 128), F32)

    loads[0].wait()
    loads[1].wait()
    for s in range(SEGS):
        shb[s] = jnp.broadcast_to(sh_ref[:, s : s + 1], (ROWS, 128))
        frb[s] = jnp.broadcast_to(fr_ref[:, s : s + 1], (ROWS, 128))

    with jax.named_scope("xwait"):
        loads[2].wait()

    def piece(i):
        return lax.rem(i + NPZ, NP)

    def y_copy(r, t):
        return rcopy(ws.at[r - 1, t], wg.at[t, y], y_s.at[r - 1], y_r.at[t, r - 1], y_dev(r))

    def warp(i):
        t = piece(i)
        zq, j = lax.div(t, NPZ), lax.rem(t, NPZ)
        for r in range(NY):
            b = zq * (NY * OWN) + lax.rem(y + r, NY) * OWN + j * PW
            v = xp[:, pl.ds(pl.multiple_of(b, 128), PW + 256)]
            s = lax.div(b, SEG)
            reps = (PW + 256) // 128
            d = jnp.concatenate([shb[s]] * reps, axis=1)
            f = jnp.concatenate([frb[s]] * (PW // 128), axis=1)
            width = PW + 256
            v = jnp.where(d < 0, pltpu.roll(v, 4, 1), v)
            v = jnp.where((d & 2) != 0, pltpu.roll(v, width - 2, 1), v)
            v = jnp.where((d & 1) != 0, pltpu.roll(v, width - 1, 1), v)
            lower = v[:, 128 : 128 + PW]
            upper = pltpu.roll(v, width - 1, 1)[:, 128 : 128 + PW]
            out = (1.0 - f) * lower + f * upper
            if r == 0:
                wg[t, y] = out
            else:
                ws[r - 1, t] = out

    def send(i):
        t = piece(i)
        for r in range(1, NY):
            y_copy(r, t).start()

    def warp_early(i, carry):
        warp(i)
        return carry

    def send_early(i, carry):
        send(i)
        return carry

    with jax.named_scope("warps"):
        lax.fori_loop(0, FIRST, warp_early, 0)
    loads[3].wait()
    loads[4].wait()
    fbuf[y] = f_ref[...]
    with jax.named_scope("barrier"):
        pl.semaphore_wait(
            barrier,
            PEERS + NZ // 2 - 1 + jnp.where(center, 1, 0) + jnp.where((m == 7) | (m == 8), 1, 0),
        )

    f_copies = [
        rcopy(f_ref, fbuf.at[y], f_s.at[r - 1], f_r.at[r - 1], y_dev(r)) for r in range(1, NY)
    ]
    for c in f_copies:
        c.start()
    lax.fori_loop(0, FIRST, send_early, 0)

    to_right = rcopy(
        xp.at[:, pl.ds(BINS, 128)], xp.at[:, pl.ds(0, 128)], halo_s.at[0], halo_r.at[0], (p, m + 1)
    )
    to_left = rcopy(
        xp.at[:, pl.ds(128, 128)], xp.at[:, pl.ds(128 + BINS, 128)], halo_s.at[1], halo_r.at[1], (p, m - 1)
    )

    @pl.when(m < 15)
    def _():
        to_right.start()

    @pl.when(m > 0)
    def _():
        to_left.start()

    near = jnp.where(low_side, NZ // 2 - 1, NZ // 2)

    def h_part(j):
        t = z * NPZ + j
        dev = (jnp.where(center, inner, near * NY + y), m)
        return rcopy(hin_ref.at[:, pl.ds(j * PW, PW)], hc.at[t], hc_s, hc_r.at[t], dev)

    def h_relay(t):
        return rcopy(hc.at[t], hc.at[t], hc_s, hc_r.at[t], (inner, m))

    for j in range(NPZ):
        h_part(j).start()

    @pl.when(center)
    def _():
        for j in range(NPZ):
            hc[z * NPZ + j] = hin_ref[:, j * PW : (j + 1) * PW]

    with jax.named_scope("fwait"):
        for c in f_copies:
            c.wait_recv()
    fg = fbuf[...].reshape(GROUP, RANK)
    gy = lax.dot_general(fg, fg, (((0,), (0,)), ((), ())), precision=exact_mode, preferred_element_type=F32)
    f_hi, f_lo = halves(fg.T)
    lhs[...] = jnp.concatenate([f_hi, f_hi, f_lo], axis=1)

    g_half = rcopy(gsend, gbuf.at[z], g_s, g_r.at[z], (near * NY + y, m))
    g_other = rcopy(gsend, gbuf.at[NZ], g_s, g_r.at[NZ], (inner, m))

    def outward(k):
        return jnp.where(low_side, NZ // 2 - 1 - k, NZ // 2 + k)

    @pl.when(jnp.logical_not(center))
    def _():
        gsend[...] = gy
        g_half.start()

    @pl.when(center)
    def _():
        total = gy
        for k in range(1, NZ // 2):
            zk = outward(k)
            rcopy(gsend, gbuf.at[zk], g_s, g_r.at[zk], (inner, m)).wait_recv()
            total = total + gbuf[zk]
        gsend[...] = total
        g_other.start()
        with jax.named_scope("relay"):
            for k in range(1, NZ // 2):
                for j in range(NPZ):
                    t = outward(k) * NPZ + j
                    h_relay(t).wait_recv()
                    h_relay(t).start()
        g_other.wait_recv()
        gbuf[NZ + 1] = total + gbuf[NZ]

    def c_copy(t):
        return rcopy(cout.at[t], cbuf.at[slot, t], c_s, c_r.at[slot, t], (inner, m))

    def c_wait(s, t):
        rcopy(cout.at[t], cbuf.at[s, t], c_s, c_r.at[s, t], (inner, m)).wait_recv()

    def h_copy(t):
        return rcopy(hbuf.at[t], hbuf.at[t], h_s, h_r.at[t], (outer, m))

    def step(i, carry):
        @pl.when((i >= FIRST - AHEAD) & (i + AHEAD < NP))
        def _():
            @pl.when(i + AHEAD == NP - NPZ - 1)
            def _():
                @pl.when(m > 0)
                def _():
                    to_right.wait_recv()

                @pl.when(m < 15)
                def _():
                    to_left.wait_recv()

            warp(i + AHEAD)
            send(i + AHEAD)

        @pl.when(i < NP)
        def _():
            t = piece(i)
            with jax.named_scope("ywait"):
                for r in range(1, NY):
                    y_copy(r, t).wait_recv()
            w_hi, w_lo = halves(wg[t].reshape(GROUP, PW))
            both = jnp.concatenate([w_hi, w_lo], axis=0)
            wgb[t] = both
            n = jnp.dot(lhs[...], jnp.concatenate([both, w_hi], axis=0), preferred_element_type=F32)

            @pl.when(has_outer)
            def _():
                with jax.named_scope("cwait"):
                    c_wait(0, t)
                cout[t] = n + cbuf[0, t]

            @pl.when(jnp.logical_not(has_outer))
            def _():
                cout[t] = n

            c_copy(t).start()

            @pl.when(center)
            def _():
                @pl.when(lax.div(t, NPZ * (NZ // 2)) != lax.div(z, NZ // 2))
                def _():
                    with jax.named_scope("hcwait"):
                        h_relay(t).wait_recv()

                own = hc[t]
                bottom = jnp.dot(gbuf[NZ + 1], own, precision=exact_mode, preferred_element_type=F32) + EPSILON
                rbuf[t] = own / bottom

        k = i - lag

        @pl.when((k >= 0) & (k < NP))
        def _():
            t = piece(k)

            @pl.when(center)
            def _():
                with jax.named_scope("xcwait"):
                    c_wait(1, t)
                hbuf[t] = rbuf[t] * (cout[t] + cbuf[1, t])

            @pl.when(jnp.logical_not(center))
            def _():
                with jax.named_scope("hwait"):
                    h_copy(t).wait_recv()

            @pl.when(has_outer)
            def _():
                h_copy(t).start()

            h = hbuf[t]
            h_hi, h_lo = halves(h)
            right = jnp.concatenate([h_hi, h_lo], axis=0)
            left = jnp.concatenate([wgb[t], right], axis=0)
            acc[...] += lax.dot_general(left, right, NT, preferred_element_type=F32)

            @pl.when(lax.div(t, NPZ) == z)
            def _():
                hout_ref[:, pl.ds(pl.multiple_of(lax.rem(t, NPZ) * PW, 128), PW)] = h

        return carry

    lax.fori_loop(0, NP + LAGS[-1], step, 0)

    both = acc[:, 0:RANK] + acc[:, RANK : 2 * RANK]
    proj = both[0:GROUP] + both[GROUP : 2 * GROUP]
    base = 2 * GROUP
    gram = both[base : base + RANK] + both[base + RANK : base + 2 * RANK]
    for k in range(NY):
        t1s[k] = jnp.concatenate(
            [proj[k * ROWS : (k + 1) * ROWS], gram[0:ROWS], gram[ROWS : 2 * ROWS], jnp.zeros((ROWS, 32), F32)],
            axis=1,
        )

    me = y * 8 + ml

    def t_copy(k):
        return rcopy(
            t1s.at[lax.rem(y + lax.div(k, 8), NY)], t1r.at[me], t1_s.at[k], t1_r.at[k], plane_dev(k)
        )

    def t_start(k, carry):
        t_copy(k).start()
        return carry

    def t_recv(k, carry):
        t_copy(k).wait_recv()
        return carry

    def t_sent(k, carry):
        t_copy(k).wait_send()
        return carry

    lax.fori_loop(1, PEERS, t_start, 0)
    t1r[me] = t1s[y]
    with jax.named_scope("t1wait"):
        lax.fori_loop(1, PEERS, t_recv, 0)
    part = t1r[0]
    for k in range(1, PEERS):
        part = part + t1r[k]
    t3s[...] = part
    t3_copy = rcopy(t3s, t3r, t3_s, t3_r, far)
    t3_copy.start()
    with jax.named_scope("t3wait"):
        t3_copy.wait_recv()
    total = part + t3r[...]
    gram_sum = jnp.concatenate([total[:, 32:64], total[:, 64:96]], axis=0)
    f = f_ref[...]
    bottom = jnp.dot(f, gram_sum, precision=exact_mode, preferred_element_type=F32) + EPSILON
    w_ref[...] = f * total[:, 0:32] / bottom

    for c in f_copies + [t3_copy]:
        c.wait_send()
    lax.fori_loop(1, PEERS, t_sent, 0)

    @pl.when(m < 15)
    def _():
        to_right.wait_send()

    @pl.when(m > 0)
    def _():
        to_left.wait_send()

    g_half.wait_send()
    def hc_sent(pieces):
        part = hc.at[pl.ds(0, pieces)]
        rcopy(part, part, hc_s, hc_s, (inner, m)).wait_send()

    @pl.when(center)
    def _():
        hc_sent(NPZ * (NZ // 2))

    @pl.when(jnp.logical_not(center))
    def _():
        hc_sent(NPZ)

    for r in range(1, NY):
        rcopy(ws.at[r - 1], ws.at[r - 1], y_s.at[r - 1], y_s.at[r - 1], y_dev(r)).wait_send()
    rcopy(cout, cout, c_s, c_s, (inner, m)).wait_send()

    @pl.when(has_outer)
    def _():
        rcopy(hbuf, hbuf, h_s, h_s, (outer, m)).wait_send()


def body(spectra, shifts, fractions, pixel_factors, spectral_factors):
    vmem = pl.BlockSpec(memory_space=pltpu.VMEM)
    dma = pltpu.SemaphoreType.DMA
    return pl.pallas_call(
        kernel,
        out_shape=(
            jax.ShapeDtypeStruct((ROWS, RANK), F32),
            jax.ShapeDtypeStruct((RANK, OWN), F32),
        ),
        in_specs=[pl.BlockSpec(memory_space=pltpu.HBM)] * 5,
        out_specs=(vmem, vmem),
        scratch_shapes=[
            pltpu.VMEM((ROWS, SEGS), jnp.int32),
            pltpu.VMEM((ROWS, SEGS), F32),
            pltpu.VMEM((ROWS, RANK), F32),
            pltpu.VMEM((RANK, OWN), F32),
            pltpu.VMEM((ROWS, BINS + 256), F32),
            pltpu.VMEM((SEGS, ROWS, 128), jnp.int32),
            pltpu.VMEM((SEGS, ROWS, 128), F32),
            pltpu.VMEM((NY - 1, NP, ROWS, PW), F32),
            pltpu.VMEM((NP, NY, ROWS, PW), F32),
            pltpu.VMEM((NP, 2 * GROUP, PW), BF16),
            pltpu.VMEM((2, NP, RANK, PW), F32),
            pltpu.VMEM((NP, RANK, PW), F32),
            pltpu.VMEM((NP, RANK, PW), F32),
            pltpu.VMEM((NP, RANK, PW), F32),
            pltpu.VMEM((NP, RANK, PW), F32),
            pltpu.VMEM((NY, ROWS, RANK), F32),
            pltpu.VMEM((RANK, 3 * GROUP), BF16),
            pltpu.VMEM((RANK, RANK), F32),
            pltpu.VMEM((NZ + 2, RANK, RANK), F32),
            pltpu.VMEM((2 * GROUP + 2 * RANK, 2 * RANK), F32),
            pltpu.VMEM((NY, ROWS, 128), F32),
            pltpu.VMEM((PEERS, ROWS, 128), F32),
            pltpu.VMEM((ROWS, 128), F32),
            pltpu.VMEM((ROWS, 128), F32),
            dma((5,)),
            dma((2,)),
            dma((2,)),
            dma((NY - 1,)),
            dma((NY - 1,)),
            dma(()),
            dma((NP,)),
            dma(()),
            dma((NZ + 1,)),
            dma((NY - 1,)),
            dma((NP, NY - 1)),
            dma(()),
            dma((2, NP)),
            dma(()),
            dma((NP,)),
            dma((PEERS,)),
            dma((PEERS,)),
            dma(()),
            dma(()),
        ],
        compiler_params=pltpu.CompilerParams(
            collective_id=0, has_side_effects=True, vmem_limit_bytes=48 * 1024 * 1024
        ),
    )(spectra, shifts, fractions, pixel_factors, spectral_factors)


def solution(mesh):
    return jax.shard_map(
        body,
        mesh=mesh,
        in_specs=(
            P("pix", "mz"),
            P("pix", "mz"),
            P("pix", "mz"),
            P("pix", None),
            P(None, ("mz", "pix")),
        ),
        out_specs=(P("pix", None), P(None, ("mz", "pix"))),
        check_vma=False,
    )
```

```python
import jax
import jax.numpy as jnp
from jax import lax
from jax.experimental import pallas as pl
from jax.experimental.pallas import tpu as pltpu
from jax.sharding import PartitionSpec as P

SEG = 2048
RANK = 32
EPSILON = 1e-06
ROWS = 16
BINS = 24576
SEGS = BINS // SEG
NZ, NY = 8, 4
OWN = 768
PW = 256
NPZ = OWN // PW
NP = NZ * NPZ
GROUP = NY * ROWS
LAGS = (5, 13, 21, 24)
CHUNK = 1024
GROUP_BINS = NY * OWN
EARLY = 6
PEERS = 32
MESH = pl.DeviceIdType.MESH
F32 = jnp.float32
BF16 = jnp.bfloat16
exact_mode = lax.Precision.HIGHEST
NT = (((1,), (1,)), ((), ()))


def halves(v):
    hi = v.astype(BF16)
    return hi, (v - hi.astype(F32)).astype(BF16)


def kernel(
    x_hbm, sh_hbm, fr_hbm, f_hbm, hin_hbm, w_ref, hout_ref,
    sh_ref, fr_ref, f_ref, hin_ref,
    xp, shb, frb, ws, wg, wgb, cbuf, cout, hbuf, hc, rbuf, fbuf, lhs, gsend, gbuf, acc,
    t1s, t1r, t3s, t3r,
    xsem, halo_s, halo_r, f_s, f_r, hc_s, hc_r, g_s, g_r,
    y_s, y_r, c_s, c_r, h_s, h_r, t1_s, t1_r, t3_s, t3_r,
):
    p, m = lax.axis_index("pix"), lax.axis_index("mz")
    z, y = lax.div(p, NY), lax.rem(p, NY)
    mh, ml = lax.div(m, 8), lax.rem(m, 8)
    low_side = z < NZ // 2
    inner = jnp.where(low_side, p + NY, p - NY)
    outer = jnp.where(low_side, p - NY, p + NY)
    depth = jnp.where(low_side, NZ // 2 - 1 - z, z - NZ // 2)
    center = depth == 0
    slot = jnp.where(center, 1, 0)
    has_outer = depth < NZ // 2 - 1
    lag = jnp.where(
        depth == 0, LAGS[0], jnp.where(depth == 1, LAGS[1], jnp.where(depth == 2, LAGS[2], LAGS[3]))
    )

    def y_dev(r):
        return (z * NY + lax.rem(y + r, NY), m)

    def m_dev(r):
        return (p, mh * 8 + lax.rem(ml + r, 8))

    far = (p, lax.rem(m + 8, 16))

    def rcopy(src, dst, send, recv, dev):
        return pltpu.make_async_remote_copy(
            src_ref=src, dst_ref=dst, send_sem=send, recv_sem=recv, device_id=dev, device_id_type=MESH
        )

    small = [
        pltpu.make_async_copy(a, b, xsem.at[k])
        for k, (a, b) in enumerate(
            ((sh_hbm, sh_ref), (fr_hbm, fr_ref), (f_hbm, f_ref), (hin_hbm, hin_ref))
        )
    ]
    lo, hi = GROUP_BINS - 128, 2 * GROUP_BINS + 128
    parts = [
        pltpu.make_async_copy(
            x_hbm.at[:, pl.ds(a, b - a)], xp.at[:, pl.ds(128 + a, b - a)], xsem.at[4 + k]
        )
        for k, (a, b) in enumerate(((lo, hi), (hi, BINS), (0, lo)))
    ]
    for c in small[:2] + parts + small[2:]:
        c.start()

    barrier = pltpu.get_barrier_semaphore()

    def greet(dev):
        pl.semaphore_signal(barrier, inc=1, device_id=dev, device_id_type=MESH)

    def plane_dev(k):
        return (
            z * NY + lax.rem(y + lax.div(k, 8), NY),
            mh * 8 + lax.rem(ml + lax.rem(k, 8), 8),
        )

    for k in range(1, PEERS):
        greet(plane_dev(k))
    half = lax.div(z, NZ // 2) * (NZ // 2)
    for r in range(1, NZ // 2):
        greet(((half + lax.rem(z + r, NZ // 2)) * NY + y, m))
    greet(far)

    @pl.when(center)
    def _():
        greet((inner, m))

    @pl.when(m == 7)
    def _():
        greet((p, 8))

    @pl.when(m == 8)
    def _():
        greet((p, 7))

    acc[...] = jnp.zeros_like(acc)

    @pl.when(m == 0)
    def _():
        xp[:, 0:128] = jnp.zeros((ROWS, 128), F32)

    @pl.when(m == 15)
    def _():
        xp[:, 128 + BINS :] = jnp.zeros((ROWS, 128), F32)

    small[0].wait()
    small[1].wait()
    for s in range(SEGS):
        shb[s] = jnp.broadcast_to(sh_ref[:, s : s + 1], (ROWS, 128))
        frb[s] = jnp.broadcast_to(fr_ref[:, s : s + 1], (ROWS, 128))

    def piece(i):
        return lax.rem(i + NPZ, NP)

    def own_bins(t):
        return first_bin(0, t)

    def first_bin(r, t):
        zq, j = lax.div(t, NPZ), lax.rem(t, NPZ)
        return pl.multiple_of(zq * GROUP_BINS + lax.rem(y + r, NY) * OWN + j * PW, 128)

    def warp(c):
        width = CHUNK + 256
        b = pl.multiple_of(c * CHUNK, 128)
        v = xp[:, pl.ds(b, width)]
        seg = lax.div(b, SEG)
        d = jnp.concatenate([shb[seg]] * (width // 128), axis=1)
        f = jnp.concatenate([frb[seg]] * (CHUNK // 128), axis=1)
        v = jnp.where(d < 0, pltpu.roll(v, 4, 1), v)
        v = jnp.where((d & 2) != 0, pltpu.roll(v, width - 2, 1), v)
        v = jnp.where((d & 1) != 0, pltpu.roll(v, width - 1, 1), v)
        lower = v[:, 128 : 128 + CHUNK]
        upper = pltpu.roll(v, width - 1, 1)[:, 128 : 128 + CHUNK]
        ws[:, pl.ds(b, CHUNK)] = (1.0 - f) * lower + f * upper

    def warp_group(g):
        zq = lax.rem(g + 1, NZ)

        def one(k, carry):
            warp(zq * (GROUP_BINS // CHUNK) + k)
            return carry

        lax.fori_loop(0, GROUP_BINS // CHUNK, one, 0)

    def y_copy(r, t):
        src = ws.at[:, pl.ds(first_bin(r, t), PW)]
        return rcopy(src, wg.at[t, NY - r - 1], y_s.at[r - 1], y_r.at[t, NY - r - 1], y_dev(r))

    def send_group(g):
        zq = lax.rem(g + 1, NZ)
        for j in range(NPZ):
            for r in range(1, NY):
                y_copy(r, zq * NPZ + j).start()

    parts[0].wait()
    with jax.named_scope("warps"):
        warp_group(0)
    small[2].wait()
    fbuf[0] = f_ref[...]
    with jax.named_scope("barrier"):
        pl.semaphore_wait(
            barrier,
            PEERS + NZ // 2 - 1 + jnp.where(center, 1, 0) + jnp.where((m == 7) | (m == 8), 1, 0),
        )

    f_copies = [
        rcopy(f_ref, fbuf.at[NY - r], f_s.at[r - 1], f_r.at[NY - r - 1], y_dev(r)) for r in range(1, NY)
    ]
    for c in f_copies:
        c.start()
    send_group(0)
    parts[1].wait()
    parts[2].wait()
    small[3].wait()

    to_right = rcopy(
        xp.at[:, pl.ds(BINS, 128)], xp.at[:, pl.ds(0, 128)], halo_s.at[0], halo_r.at[0], (p, m + 1)
    )
    to_left = rcopy(
        xp.at[:, pl.ds(128, 128)], xp.at[:, pl.ds(128 + BINS, 128)], halo_s.at[1], halo_r.at[1], (p, m - 1)
    )

    @pl.when(m < 15)
    def _():
        to_right.start()

    @pl.when(m > 0)
    def _():
        to_left.start()

    near = jnp.where(low_side, NZ // 2 - 1, NZ // 2)

    def h_part(j):
        t = z * NPZ + j
        dev = (jnp.where(center, inner, near * NY + y), m)
        return rcopy(hin_ref.at[:, pl.ds(j * PW, PW)], hc.at[t], hc_s, hc_r.at[t], dev)

    def h_relay(t):
        return rcopy(hc.at[t], hc.at[t], hc_s, hc_r.at[t], (inner, m))

    for j in range(NPZ):
        h_part(j).start()

    @pl.when(center)
    def _():
        for j in range(NPZ):
            hc[z * NPZ + j] = hin_ref[:, j * PW : (j + 1) * PW]

    def early(g, carry):
        warp_group(g)
        send_group(g)
        return carry

    with jax.named_scope("warps"):
        lax.fori_loop(1, EARLY, early, 0)

    with jax.named_scope("fwait"):
        for c in f_copies:
            c.wait_recv()
    fg = fbuf[...].reshape(GROUP, RANK)
    gy = lax.dot_general(fg, fg, (((0,), (0,)), ((), ())), precision=exact_mode, preferred_element_type=F32)
    f_hi, f_lo = halves(fg.T)
    lhs[...] = jnp.concatenate([f_hi, f_hi, f_lo], axis=1)

    g_half = rcopy(gsend, gbuf.at[z], g_s, g_r.at[z], (near * NY + y, m))
    g_other = rcopy(gsend, gbuf.at[NZ], g_s, g_r.at[NZ], (inner, m))

    def outward(k):
        return jnp.where(low_side, NZ // 2 - 1 - k, NZ // 2 + k)

    @pl.when(jnp.logical_not(center))
    def _():
        gsend[...] = gy
        g_half.start()

    @pl.when(center)
    def _():
        total = gy
        for k in range(1, NZ // 2):
            zk = outward(k)
            rcopy(gsend, gbuf.at[zk], g_s, g_r.at[zk], (inner, m)).wait_recv()
            total = total + gbuf[zk]
        gsend[...] = total
        g_other.start()
        with jax.named_scope("relay"):
            for k in range(1, NZ // 2):
                for j in range(NPZ):
                    t = outward(k) * NPZ + j
                    h_relay(t).wait_recv()
                    h_relay(t).start()
        g_other.wait_recv()
        gbuf[NZ + 1] = total + gbuf[NZ]

    def c_copy(t):
        return rcopy(cout.at[t], cbuf.at[slot, t], c_s, c_r.at[slot, t], (inner, m))

    def c_wait(s, t):
        rcopy(cout.at[t], cbuf.at[s, t], c_s, c_r.at[s, t], (inner, m)).wait_recv()

    def h_copy(t):
        return rcopy(hbuf.at[t], hbuf.at[t], h_s, h_r.at[t], (outer, m))

    def step(i, carry):
        @pl.when(i == 8)
        def _():
            @pl.when(m < 15)
            def _():
                to_left.wait_recv()

            warp_group(NZ - 2)
            send_group(NZ - 2)

        @pl.when(i == 11)
        def _():
            @pl.when(m > 0)
            def _():
                to_right.wait_recv()

            warp_group(NZ - 1)
            send_group(NZ - 1)

        @pl.when(i < NP)
        def _():
            t = piece(i)
            with jax.named_scope("ywait"):
                for r in range(1, NY):
                    y_copy(r, t).wait_recv()
            mine = ws[:, pl.ds(own_bins(t), PW)]
            w_hi, w_lo = halves(jnp.concatenate([mine, wg[t].reshape(GROUP - ROWS, PW)], axis=0))
            both = jnp.concatenate([w_hi, w_lo], axis=0)
            wgb[t] = both
            n = jnp.dot(lhs[...], jnp.concatenate([both, w_hi], axis=0), preferred_element_type=F32)

            @pl.when(has_outer)
            def _():
                with jax.named_scope("cwait"):
                    c_wait(0, t)
                cout[t] = n + cbuf[0, t]

            @pl.when(jnp.logical_not(has_outer))
            def _():
                cout[t] = n

            c_copy(t).start()

            @pl.when(center)
            def _():
                @pl.when(lax.div(t, NPZ * (NZ // 2)) != lax.div(z, NZ // 2))
                def _():
                    with jax.named_scope("hcwait"):
                        h_relay(t).wait_recv()

                own = hc[t]
                bottom = jnp.dot(gbuf[NZ + 1], own, precision=exact_mode, preferred_element_type=F32) + EPSILON
                rbuf[t] = own / bottom

        k = i - lag

        @pl.when((k >= 0) & (k < NP))
        def _():
            t = piece(k)

            @pl.when(center)
            def _():
                with jax.named_scope("xcwait"):
                    c_wait(1, t)
                hbuf[t] = rbuf[t] * (cout[t] + cbuf[1, t])

            @pl.when(jnp.logical_not(center))
            def _():
                with jax.named_scope("hwait"):
                    h_copy(t).wait_recv()

            @pl.when(has_outer)
            def _():
                h_copy(t).start()

            h = hbuf[t]
            h_hi, h_lo = halves(h)
            right = jnp.concatenate([h_hi, h_lo], axis=0)
            left = jnp.concatenate([wgb[t], right], axis=0)
            acc[...] += lax.dot_general(left, right, NT, preferred_element_type=F32)

            @pl.when(lax.div(t, NPZ) == z)
            def _():
                hout_ref[:, pl.ds(pl.multiple_of(lax.rem(t, NPZ) * PW, 128), PW)] = h

        return carry

    lax.fori_loop(0, NP + LAGS[-1], step, 0)

    both = acc[:, 0:RANK] + acc[:, RANK : 2 * RANK]
    proj = both[0:GROUP] + both[GROUP : 2 * GROUP]
    base = 2 * GROUP
    gram = both[base : base + RANK] + both[base + RANK : base + 2 * RANK]
    for k in range(NY):
        t1s[k, 0:8] = jnp.concatenate([gram[8 * q : 8 * q + 8] for q in range(4)], axis=1)
        rows = proj[k * ROWS : (k + 1) * ROWS]
        t1s[k, 8:12] = jnp.concatenate([rows[4 * q : 4 * q + 4] for q in range(4)], axis=1)

    me = y * 8 + ml

    def t_copy(k):
        return rcopy(
            t1s.at[lax.div(k, 8)], t1r.at[me], t1_s.at[k], t1_r.at[k], plane_dev(k)
        )

    def t_start(k, carry):
        t_copy(k).start()
        return carry

    def t_recv(k, carry):
        t_copy(k).wait_recv()
        return carry

    def t_sent(k, carry):
        t_copy(k).wait_send()
        return carry

    lax.fori_loop(1, PEERS, t_start, 0)
    t1r[me] = t1s[0]
    with jax.named_scope("t1wait"):
        lax.fori_loop(1, PEERS, t_recv, 0)
    part = t1r[0]
    for k in range(1, PEERS):
        part = part + t1r[k]
    t3s[...] = part
    t3_copy = rcopy(t3s, t3r, t3_s, t3_r, far)
    t3_copy.start()
    with jax.named_scope("t3wait"):
        t3_copy.wait_recv()
    total = part + t3r[...]
    gram_sum = jnp.concatenate([total[0:8, 32 * q : 32 * q + 32] for q in range(4)], axis=0)
    proj_sum = jnp.concatenate([total[8:12, 32 * q : 32 * q + 32] for q in range(4)], axis=0)
    f = f_ref[...]
    bottom = jnp.dot(f, gram_sum, precision=exact_mode, preferred_element_type=F32) + EPSILON
    w_ref[...] = f * proj_sum / bottom

    for c in f_copies + [t3_copy]:
        c.wait_send()
    lax.fori_loop(1, PEERS, t_sent, 0)

    @pl.when(m < 15)
    def _():
        to_right.wait_send()

    @pl.when(m > 0)
    def _():
        to_left.wait_send()

    g_half.wait_send()
    def hc_sent(pieces):
        part = hc.at[pl.ds(0, pieces)]
        rcopy(part, part, hc_s, hc_s, (inner, m)).wait_send()

    @pl.when(center)
    def _():
        hc_sent(NPZ * (NZ // 2))

    @pl.when(jnp.logical_not(center))
    def _():
        hc_sent(NPZ)

    for r in range(1, NY):
        rcopy(wg.at[:, r - 1], wg.at[:, r - 1], y_s.at[r - 1], y_s.at[r - 1], y_dev(r)).wait_send()
    rcopy(cout, cout, c_s, c_s, (inner, m)).wait_send()

    @pl.when(has_outer)
    def _():
        rcopy(hbuf, hbuf, h_s, h_s, (outer, m)).wait_send()


def body(spectra, shifts, fractions, pixel_factors, spectral_factors):
    vmem = pl.BlockSpec(memory_space=pltpu.VMEM)
    dma = pltpu.SemaphoreType.DMA
    return pl.pallas_call(
        kernel,
        out_shape=(
            jax.ShapeDtypeStruct((ROWS, RANK), F32),
            jax.ShapeDtypeStruct((RANK, OWN), F32),
        ),
        in_specs=[pl.BlockSpec(memory_space=pltpu.HBM)] * 5,
        out_specs=(vmem, vmem),
        scratch_shapes=[
            pltpu.VMEM((ROWS, SEGS), jnp.int32),
            pltpu.VMEM((ROWS, SEGS), F32),
            pltpu.VMEM((ROWS, RANK), F32),
            pltpu.VMEM((RANK, OWN), F32),
            pltpu.VMEM((ROWS, BINS + 256), F32),
            pltpu.VMEM((SEGS, ROWS, 128), jnp.int32),
            pltpu.VMEM((SEGS, ROWS, 128), F32),
            pltpu.VMEM((ROWS, BINS), F32),
            pltpu.VMEM((NP, NY - 1, ROWS, PW), F32),
            pltpu.VMEM((NP, 2 * GROUP, PW), BF16),
            pltpu.VMEM((2, NP, RANK, PW), F32),
            pltpu.VMEM((NP, RANK, PW), F32),
            pltpu.VMEM((NP, RANK, PW), F32),
            pltpu.VMEM((NP, RANK, PW), F32),
            pltpu.VMEM((NP, RANK, PW), F32),
            pltpu.VMEM((NY, ROWS, RANK), F32),
            pltpu.VMEM((RANK, 3 * GROUP), BF16),
            pltpu.VMEM((RANK, RANK), F32),
            pltpu.VMEM((NZ + 2, RANK, RANK), F32),
            pltpu.VMEM((2 * GROUP + 2 * RANK, 2 * RANK), F32),
            pltpu.VMEM((NY, 12, 128), F32),
            pltpu.VMEM((PEERS, 12, 128), F32),
            pltpu.VMEM((12, 128), F32),
            pltpu.VMEM((12, 128), F32),
            dma((7,)),
            dma((2,)),
            dma((2,)),
            dma((NY - 1,)),
            dma((NY - 1,)),
            dma(()),
            dma((NP,)),
            dma(()),
            dma((NZ + 1,)),
            dma((NY - 1,)),
            dma((NP, NY - 1)),
            dma(()),
            dma((2, NP)),
            dma(()),
            dma((NP,)),
            dma((PEERS,)),
            dma((PEERS,)),
            dma(()),
            dma(()),
        ],
        compiler_params=pltpu.CompilerParams(
            collective_id=0, has_side_effects=True, vmem_limit_bytes=66_000_000
        ),
    )(spectra, shifts, fractions, pixel_factors, spectral_factors)


def solution(mesh):
    return jax.shard_map(
        body,
        mesh=mesh,
        in_specs=(
            P("pix", "mz"),
            P("pix", "mz"),
            P("pix", "mz"),
            P("pix", None),
            P(None, ("mz", "pix")),
        ),
        out_specs=(P("pix", None), P(None, ("mz", "pix"))),
        check_vma=False,
    )
```

```python
import jax
import jax.numpy as jnp
from jax import lax
from jax.experimental import pallas as pl
from jax.experimental.pallas import tpu as pltpu
from jax.sharding import PartitionSpec as P

SEG = 2048
RANK = 32
EPSILON = 1e-06
ROWS = 16
BINS = 24576
SEGS = BINS // SEG
NZ, NY = 8, 4
OWN = 768
PW = 256
NPZ = OWN // PW
NP = NZ * NPZ
GROUP = NY * ROWS
LAGS = (7, 16, 24, 24)
SUB = 2
SUB_ROWS = RANK // SUB
DIRECT = 2
CHUNK = 1024
GROUP_BINS = NY * OWN
EARLY = 6
PEERS = 32
MESH = pl.DeviceIdType.MESH
F32 = jnp.float32
BF16 = jnp.bfloat16
exact_mode = lax.Precision.HIGHEST
NT = (((1,), (1,)), ((), ()))


def halves(v):
    hi = v.astype(BF16)
    return hi, (v - hi.astype(F32)).astype(BF16)


def kernel(
    x_hbm, sh_hbm, fr_hbm, f_hbm, hin_hbm, w_ref, hout_ref,
    sh_ref, fr_ref, f_ref, hin_ref,
    xp, shb, frb, ws, wg, wgb, cbuf, cout, hbuf, hc, rbuf, fbuf, lhs, gsend, gbuf, acc,
    grams, t1s, t1r, t3s, t3r, row_s, row_r,
    xsem, halo_s, halo_r, f_s, f_r, hc_s, hc_r, g_s, g_r,
    y_s, y_r, c_s, c_r, h_s, h_r, t1_s, t1_r, t3_s, t3_r, r_s, r_r,
):
    p, m = lax.axis_index("pix"), lax.axis_index("mz")
    z, y = lax.div(p, NY), lax.rem(p, NY)
    mh, ml = lax.div(m, 8), lax.rem(m, 8)
    low_side = z < NZ // 2
    inner = jnp.where(low_side, p + NY, p - NY)
    outer = jnp.where(low_side, p - NY, p + NY)
    depth = jnp.where(low_side, NZ // 2 - 1 - z, z - NZ // 2)
    center = depth == 0
    slot = jnp.where(center, 1, 0)
    has_outer = depth < NZ // 2 - 1
    lag = jnp.where(
        depth == 0, LAGS[0], jnp.where(depth == 1, LAGS[1], jnp.where(depth == 2, LAGS[2], LAGS[3]))
    )

    def y_dev(r):
        return (z * NY + lax.rem(y + r, NY), m)

    def m_dev(r):
        return (p, mh * 8 + lax.rem(ml + r, 8))

    far = (p, lax.rem(m + 8, 16))

    def rcopy(src, dst, send, recv, dev):
        return pltpu.make_async_remote_copy(
            src_ref=src, dst_ref=dst, send_sem=send, recv_sem=recv, device_id=dev, device_id_type=MESH
        )

    small = [
        pltpu.make_async_copy(a, b, xsem.at[k])
        for k, (a, b) in enumerate(
            ((sh_hbm, sh_ref), (fr_hbm, fr_ref), (f_hbm, f_ref), (hin_hbm, hin_ref))
        )
    ]
    lo, hi = GROUP_BINS - 128, 2 * GROUP_BINS + 128
    parts = [
        pltpu.make_async_copy(
            x_hbm.at[:, pl.ds(a, b - a)], xp.at[:, pl.ds(128 + a, b - a)], xsem.at[4 + k]
        )
        for k, (a, b) in enumerate(((lo, hi), (hi, BINS), (0, lo)))
    ]
    for c in small[:2] + parts + small[2:]:
        c.start()

    barrier = pltpu.get_barrier_semaphore()

    def greet(dev):
        pl.semaphore_signal(barrier, inc=1, device_id=dev, device_id_type=MESH)

    def plane_dev(k):
        return (
            z * NY + lax.rem(y + lax.div(k, 8), NY),
            mh * 8 + lax.rem(ml + lax.rem(k, 8), 8),
        )

    for k in range(1, PEERS):
        greet(plane_dev(k))
    def line_dev(k):
        other = lax.rem(mh + lax.div(k, NZ), 2)
        return (lax.rem(z + k, NZ) * NY + y, other * 8 + ml)

    for k in range(1, 2 * NZ):
        greet(line_dev(k))

    @pl.when(m == 7)
    def _():
        greet((p, 8))

    @pl.when(m == 8)
    def _():
        greet((p, 7))

    acc[...] = jnp.zeros_like(acc)

    @pl.when(m == 0)
    def _():
        xp[:, 0:128] = jnp.zeros((ROWS, 128), F32)

    @pl.when(m == 15)
    def _():
        xp[:, 128 + BINS :] = jnp.zeros((ROWS, 128), F32)

    small[0].wait()
    small[1].wait()
    for s in range(SEGS):
        shb[s] = jnp.broadcast_to(sh_ref[:, s : s + 1], (ROWS, 128))
        frb[s] = jnp.broadcast_to(fr_ref[:, s : s + 1], (ROWS, 128))

    def piece(i):
        return lax.rem(i + NPZ, NP)

    def own_bins(t):
        return first_bin(0, t)

    def first_bin(r, t):
        zq, j = lax.div(t, NPZ), lax.rem(t, NPZ)
        return pl.multiple_of(zq * GROUP_BINS + lax.rem(y + r, NY) * OWN + j * PW, 128)

    def warp(c):
        width = CHUNK + 256
        b = pl.multiple_of(c * CHUNK, 128)
        seg = lax.div(b, SEG)
        d, f = shb[seg], frb[seg]

        def wide(v, lanes):
            return jnp.concatenate([v] * (lanes // 128), axis=1)

        v = xp[:, pl.ds(b, width)]
        v = jnp.where(wide(d, width) < 0, pltpu.roll(v, 4, 1), v)
        shifted = [v] + [pltpu.roll(v, width - k, 1) for k in range(1, 5)]
        shifted = [u[:, 128 : 128 + CHUNK] for u in shifted]
        rest = wide(d & 3, CHUNK)
        high, odd = rest >= 2, (rest & 1) != 0

        def pick(k):
            return jnp.where(
                high,
                jnp.where(odd, shifted[k + 3], shifted[k + 2]),
                jnp.where(odd, shifted[k + 1], shifted[k]),
            )

        f = wide(f, CHUNK)
        ws[:, pl.ds(b, CHUNK)] = (1.0 - f) * pick(0) + f * pick(1)

    def warp_group(g):
        zq = lax.rem(g + 1, NZ)

        for k in range(GROUP_BINS // CHUNK):
            warp(zq * (GROUP_BINS // CHUNK) + k)

    def y_copy(r, t):
        src = ws.at[:, pl.ds(first_bin(r, t), PW)]
        return rcopy(src, wg.at[t, NY - r - 1], y_s.at[r - 1], y_r.at[t, NY - r - 1], y_dev(r))

    def send_group(g):
        zq = lax.rem(g + 1, NZ)
        for j in range(NPZ):
            for r in range(1, NY):
                y_copy(r, zq * NPZ + j).start()

    parts[0].wait()
    with jax.named_scope("warps"):
        warp_group(0)
    small[2].wait()
    fbuf[0] = f_ref[...]
    with jax.named_scope("barrier"):
        pl.semaphore_wait(
            barrier,
            PEERS - 1 + 2 * NZ - 1 + jnp.where((m == 7) | (m == 8), 1, 0),
        )

    f_copies = [
        rcopy(f_ref, fbuf.at[NY - r], f_s.at[r - 1], f_r.at[NY - r - 1], y_dev(r)) for r in range(1, NY)
    ]
    for c in f_copies:
        c.start()
    send_group(0)
    parts[1].wait()
    parts[2].wait()
    small[3].wait()

    to_right = rcopy(
        xp.at[:, pl.ds(BINS, 128)], xp.at[:, pl.ds(0, 128)], halo_s.at[0], halo_r.at[0], (p, m + 1)
    )
    to_left = rcopy(
        xp.at[:, pl.ds(128, 128)], xp.at[:, pl.ds(128 + BINS, 128)], halo_s.at[1], halo_r.at[1], (p, m - 1)
    )

    @pl.when(m < 15)
    def _():
        to_right.start()

    @pl.when(m > 0)
    def _():
        to_left.start()

    near = jnp.where(low_side, NZ // 2 - 1, NZ // 2)

    def h_part(j):
        t = z * NPZ + j
        dev = (jnp.where(center, inner, near * NY + y), m)
        return rcopy(hin_ref.at[:, pl.ds(j * PW, PW)], hc.at[t], hc_s, hc_r.at[t], dev)

    def h_relay(t):
        return rcopy(hc.at[t], hc.at[t], hc_s, hc_r.at[t], (inner, m))

    for j in range(NPZ):
        h_part(j).start()

    @pl.when(center)
    def _():
        for j in range(NPZ):
            hc[z * NPZ + j] = hin_ref[:, j * PW : (j + 1) * PW]

    def early(g, carry):
        warp_group(g)
        send_group(g)
        return carry

    with jax.named_scope("warps"):
        lax.fori_loop(1, EARLY, early, 0)

    with jax.named_scope("fwait"):
        for c in f_copies:
            c.wait_recv()
    fg = fbuf[...].reshape(GROUP, RANK)
    gy = lax.dot_general(fg, fg, (((0,), (0,)), ((), ())), precision=exact_mode, preferred_element_type=F32)
    f_hi, f_lo = halves(fg.T)
    lhs[...] = jnp.concatenate([f_hi, f_hi, f_lo], axis=1)

    g_half = rcopy(gsend, gbuf.at[z], g_s, g_r.at[z], (near * NY + y, m))
    g_other = rcopy(gsend, gbuf.at[NZ], g_s, g_r.at[NZ], (inner, m))

    def outward(k):
        return jnp.where(low_side, NZ // 2 - 1 - k, NZ // 2 + k)

    @pl.when(jnp.logical_not(center))
    def _():
        gsend[...] = gy
        g_half.start()

    @pl.when(center)
    def _():
        total = gy
        for k in range(1, NZ // 2):
            zk = outward(k)
            rcopy(gsend, gbuf.at[zk], g_s, g_r.at[zk], (inner, m)).wait_recv()
            total = total + gbuf[zk]
        gsend[...] = total
        g_other.start()
        with jax.named_scope("relay"):
            for k in range(1, NZ // 2):
                for j in range(NPZ):
                    t = outward(k) * NPZ + j
                    h_relay(t).wait_recv()
                    h_relay(t).start()
        g_other.wait_recv()
        gbuf[NZ + 1] = total + gbuf[NZ]

    def rows_of(q):
        return pl.ds(q * SUB_ROWS, SUB_ROWS)

    def c_copy(t, q, s):
        return rcopy(
            cout.at[t, rows_of(q)], cbuf.at[s, t, rows_of(q)], c_s, c_r.at[s, t, q], (inner, m)
        )

    def h_copy(t, q, dev):
        part = hbuf.at[t, rows_of(q)]
        return rcopy(part, part, h_s, h_r.at[t, q], dev)

    def step(i, carry):
        @pl.when(i == 8)
        def _():
            @pl.when(m < 15)
            def _():
                to_left.wait_recv()

            warp_group(NZ - 2)
            send_group(NZ - 2)

        @pl.when(i == 11)
        def _():
            @pl.when(m > 0)
            def _():
                to_right.wait_recv()

            warp_group(NZ - 1)
            send_group(NZ - 1)

        @pl.when(i < NP)
        def _():
            t = piece(i)
            with jax.named_scope("ywait"):
                for r in range(1, NY):
                    y_copy(r, t).wait_recv()
            mine = ws[:, pl.ds(own_bins(t), PW)]
            w_hi, w_lo = halves(jnp.concatenate([mine, wg[t].reshape(GROUP - ROWS, PW)], axis=0))
            both = jnp.concatenate([w_hi, w_lo], axis=0)
            wgb[t] = both
            n = jnp.dot(lhs[...], jnp.concatenate([both, w_hi], axis=0), preferred_element_type=F32)

            @pl.when(has_outer)
            def _():
                for q in range(SUB):
                    with jax.named_scope("cwait"):
                        c_copy(t, q, 0).wait_recv()
                    part = n[q * SUB_ROWS : (q + 1) * SUB_ROWS]
                    cout[t, rows_of(q)] = part + cbuf[0, t, rows_of(q)]
                    c_copy(t, q, slot).start()

            @pl.when(jnp.logical_not(has_outer))
            def _():
                cout[t] = n
                for q in range(SUB):
                    c_copy(t, q, slot).start()

            @pl.when(center)
            def _():
                @pl.when(lax.div(t, NPZ * (NZ // 2)) != lax.div(z, NZ // 2))
                def _():
                    with jax.named_scope("hcwait"):
                        h_relay(t).wait_recv()

                own = hc[t]
                bottom = jnp.dot(gbuf[NZ + 1], own, precision=exact_mode, preferred_element_type=F32) + EPSILON
                rbuf[t] = own / bottom

        k = i - lag

        @pl.when((k >= 0) & (k < NP))
        def _():
            t = piece(k)

            @pl.when(center)
            def _():
                for q in range(SUB):
                    with jax.named_scope("xcwait"):
                        c_copy(t, q, 1).wait_recv()
                    r = rows_of(q)
                    hbuf[t, r] = rbuf[t, r] * (cout[t, r] + cbuf[1, t, r])
                    h_copy(t, q, (outer, m)).start()

                    @pl.when(k >= NP - DIRECT)
                    def _():
                        for far_out in (2, 3):
                            h_copy(t, q, (outward(far_out) * NY + y, m)).start()

            @pl.when(jnp.logical_not(center))
            def _():
                for q in range(SUB):
                    with jax.named_scope("hwait"):
                        h_copy(t, q, (outer, m)).wait_recv()

                    @pl.when(has_outer & (k < NP - DIRECT))
                    def _():
                        h_copy(t, q, (outer, m)).start()

            h = hbuf[t]
            h_hi, h_lo = halves(h)
            right = jnp.concatenate([h_hi, h_lo], axis=0)
            left = jnp.concatenate([wgb[t], right], axis=0)
            acc[...] += lax.dot_general(left, right, NT, preferred_element_type=F32)

            @pl.when(lax.div(t, NPZ) == z)
            def _():
                hout_ref[:, pl.ds(pl.multiple_of(lax.rem(t, NPZ) * PW, 128), PW)] = h

        return carry

    lax.fori_loop(0, NP + LAGS[-1], step, 0)

    both = acc[:, 0:RANK] + acc[:, RANK : 2 * RANK]
    proj = both[0:GROUP] + both[GROUP : 2 * GROUP]
    base = 2 * GROUP
    gram = both[base : base + RANK] + both[base + RANK : base + 2 * RANK]
    grams[...] = jnp.concatenate([gram[8 * q : 8 * q + 8] for q in range(4)], axis=1)
    my_gram = grams[pl.ds(z, 1)]
    for k in range(NY):
        rows = proj[k * ROWS : (k + 1) * ROWS]
        t1s[k, 0:4] = jnp.concatenate([rows[4 * q : 4 * q + 4] for q in range(4)], axis=1)
        t1s[k, 4:5] = my_gram

    me = y * 8 + ml

    def t_copy(k):
        return rcopy(
            t1s.at[lax.div(k, 8)], t1r.at[me], t1_s.at[k], t1_r.at[k], plane_dev(k)
        )

    def t_start(k, carry):
        t_copy(k).start()
        return carry

    def t_recv(k, carry):
        t_copy(k).wait_recv()
        return carry

    def t_sent(k, carry):
        t_copy(k).wait_send()
        return carry

    lax.fori_loop(1, PEERS, t_start, 0)
    t1r[me] = t1s[0]
    with jax.named_scope("t1wait"):
        lax.fori_loop(1, PEERS, t_recv, 0)
    part = t1r[0]
    for k in range(1, PEERS):
        part = part + t1r[k]
    t3s[...] = part[0:4]
    row_s[...] = part[4:5]
    t3_copy = rcopy(t3s, t3r, t3_s, t3_r, far)
    t3_copy.start()
    here = mh * NZ + z

    def row_copy(k):
        return rcopy(row_s, row_r.at[here], r_s.at[k], r_r.at[k], line_dev(k))

    def row_start(k, carry):
        row_copy(k).start()
        return carry

    def row_recv(k, carry):
        row_copy(k).wait_recv()
        return carry

    def row_sent(k, carry):
        row_copy(k).wait_send()
        return carry

    lax.fori_loop(1, 2 * NZ, row_start, 0)
    row_r[here] = part[4:5]
    with jax.named_scope("t3wait"):
        t3_copy.wait_recv()
        lax.fori_loop(1, 2 * NZ, row_recv, 0)
    proj4 = part[0:4] + t3r[...]
    gram8 = jnp.concatenate([row_r[k] + row_r[NZ + k] for k in range(NZ)], axis=0)
    gram_sum = jnp.concatenate([gram8[:, 32 * q : 32 * q + 32] for q in range(4)], axis=0)
    proj_sum = jnp.concatenate([proj4[:, 32 * q : 32 * q + 32] for q in range(4)], axis=0)
    f = f_ref[...]
    bottom = jnp.dot(f, gram_sum, precision=exact_mode, preferred_element_type=F32) + EPSILON
    w_ref[...] = f * proj_sum / bottom

    for c in f_copies + [t3_copy]:
        c.wait_send()
    lax.fori_loop(1, PEERS, t_sent, 0)
    lax.fori_loop(1, 2 * NZ, row_sent, 0)

    @pl.when(m < 15)
    def _():
        to_right.wait_send()

    @pl.when(m > 0)
    def _():
        to_left.wait_send()

    g_half.wait_send()
    def hc_sent(pieces):
        part = hc.at[pl.ds(0, pieces)]
        rcopy(part, part, hc_s, hc_s, (inner, m)).wait_send()

    @pl.when(center)
    def _():
        hc_sent(NPZ * (NZ // 2))

    @pl.when(jnp.logical_not(center))
    def _():
        hc_sent(NPZ)

    for r in range(1, NY):
        rcopy(wg.at[:, r - 1], wg.at[:, r - 1], y_s.at[r - 1], y_s.at[r - 1], y_dev(r)).wait_send()
    rcopy(cout, cout, c_s, c_s, (inner, m)).wait_send()

    def h_sent(pieces):
        part = hbuf.at[pl.ds(0, pieces)]
        rcopy(part, part, h_s, h_s, (outer, m)).wait_send()

    @pl.when(center)
    def _():
        h_sent(NP)
        h_sent(2 * DIRECT)

    @pl.when(has_outer & jnp.logical_not(center))
    def _():
        h_sent(NP - DIRECT)


def body(spectra, shifts, fractions, pixel_factors, spectral_factors):
    vmem = pl.BlockSpec(memory_space=pltpu.VMEM)
    dma = pltpu.SemaphoreType.DMA
    return pl.pallas_call(
        kernel,
        out_shape=(
            jax.ShapeDtypeStruct((ROWS, RANK), F32),
            jax.ShapeDtypeStruct((RANK, OWN), F32),
        ),
        in_specs=[pl.BlockSpec(memory_space=pltpu.HBM)] * 5,
        out_specs=(vmem, vmem),
        scratch_shapes=[
            pltpu.VMEM((ROWS, SEGS), jnp.int32),
            pltpu.VMEM((ROWS, SEGS), F32),
            pltpu.VMEM((ROWS, RANK), F32),
            pltpu.VMEM((RANK, OWN), F32),
            pltpu.VMEM((ROWS, BINS + 256), F32),
            pltpu.VMEM((SEGS, ROWS, 128), jnp.int32),
            pltpu.VMEM((SEGS, ROWS, 128), F32),
            pltpu.VMEM((ROWS, BINS), F32),
            pltpu.VMEM((NP, NY - 1, ROWS, PW), F32),
            pltpu.VMEM((NP, 2 * GROUP, PW), BF16),
            pltpu.VMEM((2, NP, RANK, PW), F32),
            pltpu.VMEM((NP, RANK, PW), F32),
            pltpu.VMEM((NP, RANK, PW), F32),
            pltpu.VMEM((NP, RANK, PW), F32),
            pltpu.VMEM((NP, RANK, PW), F32),
            pltpu.VMEM((NY, ROWS, RANK), F32),
            pltpu.VMEM((RANK, 3 * GROUP), BF16),
            pltpu.VMEM((RANK, RANK), F32),
            pltpu.VMEM((NZ + 2, RANK, RANK), F32),
            pltpu.VMEM((2 * GROUP + 2 * RANK, 2 * RANK), F32),
            pltpu.VMEM((NZ, 128), F32),
            pltpu.VMEM((NY, 5, 128), F32),
            pltpu.VMEM((PEERS, 5, 128), F32),
            pltpu.VMEM((4, 128), F32),
            pltpu.VMEM((4, 128), F32),
            pltpu.VMEM((1, 128), F32),
            pltpu.VMEM((2 * NZ, 1, 128), F32),
            dma((7,)),
            dma((2,)),
            dma((2,)),
            dma((NY - 1,)),
            dma((NY - 1,)),
            dma(()),
            dma((NP,)),
            dma(()),
            dma((NZ + 1,)),
            dma((NY - 1,)),
            dma((NP, NY - 1)),
            dma(()),
            dma((2, NP, SUB)),
            dma(()),
            dma((NP, SUB)),
            dma((PEERS,)),
            dma((PEERS,)),
            dma(()),
            dma(()),
            dma((2 * NZ,)),
            dma((2 * NZ,)),
        ],
        compiler_params=pltpu.CompilerParams(
            collective_id=0, has_side_effects=True, vmem_limit_bytes=66_000_000
        ),
    )(spectra, shifts, fractions, pixel_factors, spectral_factors)


def solution(mesh):
    return jax.shard_map(
        body,
        mesh=mesh,
        in_specs=(
            P("pix", "mz"),
            P("pix", "mz"),
            P("pix", "mz"),
            P("pix", None),
            P(None, ("mz", "pix")),
        ),
        out_specs=(P("pix", None), P(None, ("mz", "pix"))),
        check_vma=False,
    )
```

```python
import jax
import jax.numpy as jnp
from jax import lax
from jax.experimental import pallas as pl
from jax.experimental.pallas import tpu as pltpu
from jax.sharding import PartitionSpec as P

SEG = 2048
RANK = 32
EPSILON = 1e-06
ROWS = 16
BINS = 24576
SEGS = BINS // SEG
NZ, NY = 8, 4
OWN = 768
PW = 256
NPZ = OWN // PW
NP = NZ * NPZ
GROUP = NY * ROWS
LAGS = (5, 12, 20, 24)
SUB = 2
SUB_ROWS = RANK // SUB
DIRECT = 2
CHUNK = 1024
GROUP_BINS = NY * OWN
EARLY = 6
CHIPS = 16
MESH = pl.DeviceIdType.MESH
F32 = jnp.float32
BF16 = jnp.bfloat16
exact_mode = lax.Precision.HIGHEST
NT = (((1,), (1,)), ((), ()))


def halves(v):
    hi = v.astype(BF16)
    return hi, (v - hi.astype(F32)).astype(BF16)


def kernel(
    x_hbm, sh_hbm, fr_hbm, f_hbm, hin_hbm, w_ref, hout_ref,
    sh_ref, fr_ref, f_ref, hin_ref,
    xp, shb, frb, ws, wg, wgb, cbuf, cout, hbuf, hc, rbuf, fbuf, lhs, gsend, gbuf, acc,
    f_all, t0s, t0r, t1s, t1r, t3s, t3r,
    xsem, halo_s, halo_r, f_s, f_r, hc_s, hc_r, g_s, g_r,
    y_s, y_r, c_s, c_r, h_s, h_r, t0_s, t0_r, t1_s, t1_r, t3_s, t3_r,
):
    p, m = lax.axis_index("pix"), lax.axis_index("mz")
    z, y = lax.div(p, NY), lax.rem(p, NY)
    mh, ml = lax.div(m, 8), lax.rem(m, 8)
    low_side = z < NZ // 2
    inner = jnp.where(low_side, p + NY, p - NY)
    outer = jnp.where(low_side, p - NY, p + NY)
    depth = jnp.where(low_side, NZ // 2 - 1 - z, z - NZ // 2)
    center = depth == 0
    slot = jnp.where(center, 1, 0)
    has_outer = depth < NZ // 2 - 1
    lag = jnp.where(
        depth == 0, LAGS[0], jnp.where(depth == 1, LAGS[1], jnp.where(depth == 2, LAGS[2], LAGS[3]))
    )

    def y_dev(r):
        return (z * NY + lax.rem(y + r, NY), m)

    def m_dev(r):
        return (p, mh * 8 + lax.rem(ml + r, 8))

    far = (p, lax.rem(m + 8, 16))

    def rcopy(src, dst, send, recv, dev):
        return pltpu.make_async_remote_copy(
            src_ref=src, dst_ref=dst, send_sem=send, recv_sem=recv, device_id=dev, device_id_type=MESH
        )

    small = [
        pltpu.make_async_copy(a, b, xsem.at[k])
        for k, (a, b) in enumerate(
            ((sh_hbm, sh_ref), (fr_hbm, fr_ref), (f_hbm, f_ref), (hin_hbm, hin_ref))
        )
    ]
    lo, hi = GROUP_BINS - 128, 2 * GROUP_BINS + 128
    parts = [
        pltpu.make_async_copy(
            x_hbm.at[:, pl.ds(a, b - a)], xp.at[:, pl.ds(128 + a, b - a)], xsem.at[4 + k]
        )
        for k, (a, b) in enumerate(((lo, hi), (hi, BINS), (0, lo)))
    ]
    for c in small[:2] + parts + small[2:]:
        c.start()

    barrier = pltpu.get_barrier_semaphore()

    def greet(dev):
        pl.semaphore_signal(barrier, inc=1, device_id=dev, device_id_type=MESH)

    core = lax.rem(ml, 2)
    partner = (p, m + 1 - 2 * core)

    def plane_dev(k):
        return (
            z * NY + lax.rem(y + lax.div(k, 4), NY),
            mh * 8 + lax.rem(ml + 2 * lax.rem(k, 4), 8),
        )

    for k in range(1, CHIPS):
        greet(plane_dev(k))
    greet(partner)
    greet(far)
    half = lax.div(z, NZ // 2) * (NZ // 2)
    for r in range(1, NZ // 2):
        greet(((half + lax.rem(z + r, NZ // 2)) * NY + y, m))

    @pl.when(center)
    def _():
        greet((inner, m))

    @pl.when((core == 0) & (m > 0))
    def _():
        greet((p, m - 1))

    @pl.when((core == 1) & (m < 15))
    def _():
        greet((p, m + 1))

    acc[...] = jnp.zeros_like(acc)

    @pl.when(m == 0)
    def _():
        xp[:, 0:128] = jnp.zeros((ROWS, 128), F32)

    @pl.when(m == 15)
    def _():
        xp[:, 128 + BINS :] = jnp.zeros((ROWS, 128), F32)

    small[0].wait()
    small[1].wait()
    for s in range(SEGS):
        shb[s] = jnp.broadcast_to(sh_ref[:, s : s + 1], (ROWS, 128))
        frb[s] = jnp.broadcast_to(fr_ref[:, s : s + 1], (ROWS, 128))

    def piece(i):
        return lax.rem(i + NPZ, NP)

    def own_bins(t):
        return first_bin(0, t)

    def first_bin(r, t):
        zq, j = lax.div(t, NPZ), lax.rem(t, NPZ)
        return pl.multiple_of(zq * GROUP_BINS + lax.rem(y + r, NY) * OWN + j * PW, 128)

    def warp(c):
        width = CHUNK + 256
        b = pl.multiple_of(c * CHUNK, 128)
        seg = lax.div(b, SEG)
        d, f = shb[seg], frb[seg]

        def wide(v, lanes):
            return jnp.concatenate([v] * (lanes // 128), axis=1)

        v = xp[:, pl.ds(b, width)]
        v = jnp.where(wide(d, width) < 0, pltpu.roll(v, 4, 1), v)
        shifted = [v] + [pltpu.roll(v, width - k, 1) for k in range(1, 5)]
        shifted = [u[:, 128 : 128 + CHUNK] for u in shifted]
        rest = wide(d & 3, CHUNK)
        high, odd = rest >= 2, (rest & 1) != 0

        def pick(k):
            return jnp.where(
                high,
                jnp.where(odd, shifted[k + 3], shifted[k + 2]),
                jnp.where(odd, shifted[k + 1], shifted[k]),
            )

        f = wide(f, CHUNK)
        ws[:, pl.ds(b, CHUNK)] = (1.0 - f) * pick(0) + f * pick(1)

    def warp_group(g):
        zq = lax.rem(g + 1, NZ)

        for k in range(GROUP_BINS // CHUNK):
            warp(zq * (GROUP_BINS // CHUNK) + k)

    def y_copy(r, t):
        src = ws.at[:, pl.ds(first_bin(r, t), PW)]
        return rcopy(src, wg.at[t, NY - r - 1], y_s.at[r - 1], y_r.at[t, NY - r - 1], y_dev(r))

    def send_group(g):
        zq = lax.rem(g + 1, NZ)
        for j in range(NPZ):
            for r in range(1, NY):
                y_copy(r, zq * NPZ + j).start()

    parts[0].wait()
    with jax.named_scope("warps"):
        warp_group(0)
    small[2].wait()
    f_all[...] = jnp.concatenate([f_ref[...], jnp.zeros((ROWS, 128 - RANK), F32)], axis=1)
    with jax.named_scope("barrier"):
        pl.semaphore_wait(
            barrier,
            CHIPS + 1 + NZ // 2 - 1 + jnp.where(center, 1, 0) + jnp.where((m == 0) | (m == 15), 0, 1),
        )

    f_copies = [
        rcopy(f_all, fbuf.at[NY - r - 1], f_s.at[r - 1], f_r.at[NY - r - 1], y_dev(r)) for r in range(1, NY)
    ]
    for c in f_copies:
        c.start()
    send_group(0)
    parts[1].wait()
    parts[2].wait()
    small[3].wait()

    to_right = rcopy(
        xp.at[:, pl.ds(BINS, 128)], xp.at[:, pl.ds(0, 128)], halo_s.at[0], halo_r.at[0], (p, m + 1)
    )
    to_left = rcopy(
        xp.at[:, pl.ds(128, 128)], xp.at[:, pl.ds(128 + BINS, 128)], halo_s.at[1], halo_r.at[1], (p, m - 1)
    )

    @pl.when(m < 15)
    def _():
        to_right.start()

    @pl.when(m > 0)
    def _():
        to_left.start()

    near = jnp.where(low_side, NZ // 2 - 1, NZ // 2)

    def h_part(j):
        t = z * NPZ + j
        dev = (jnp.where(center, inner, near * NY + y), m)
        return rcopy(hin_ref.at[:, pl.ds(j * PW, PW)], hc.at[t], hc_s, hc_r.at[t], dev)

    def h_relay(t):
        return rcopy(hc.at[t], hc.at[t], hc_s, hc_r.at[t], (inner, m))

    for j in range(NPZ):
        h_part(j).start()

    @pl.when(center)
    def _():
        for j in range(NPZ):
            hc[z * NPZ + j] = hin_ref[:, j * PW : (j + 1) * PW]

    def early(g, carry):
        warp_group(g)
        send_group(g)
        return carry

    with jax.named_scope("warps"):
        lax.fori_loop(1, EARLY, early, 0)

    with jax.named_scope("fwait"):
        for c in f_copies:
            c.wait_recv()
    fg = jnp.concatenate([f_all[...], fbuf[...].reshape(GROUP - ROWS, 128)], axis=0)[:, 0:RANK]
    gy = lax.dot_general(fg, fg, (((0,), (0,)), ((), ())), precision=exact_mode, preferred_element_type=F32)
    f_hi, f_lo = halves(fg.T)
    lhs[...] = jnp.concatenate([f_hi, f_hi, f_lo], axis=1)

    g_half = rcopy(gsend, gbuf.at[z], g_s, g_r.at[z], (near * NY + y, m))
    g_other = rcopy(gsend, gbuf.at[NZ], g_s, g_r.at[NZ], (inner, m))

    def outward(k):
        return jnp.where(low_side, NZ // 2 - 1 - k, NZ // 2 + k)

    @pl.when(jnp.logical_not(center))
    def _():
        gsend[...] = gy
        g_half.start()

    @pl.when(center)
    def _():
        total = gy
        for k in range(1, NZ // 2):
            zk = outward(k)
            rcopy(gsend, gbuf.at[zk], g_s, g_r.at[zk], (inner, m)).wait_recv()
            total = total + gbuf[zk]
        gsend[...] = total
        g_other.start()
        with jax.named_scope("relay"):
            for k in range(1, NZ // 2):
                for j in range(NPZ):
                    t = outward(k) * NPZ + j
                    h_relay(t).wait_recv()
                    h_relay(t).start()
        g_other.wait_recv()
        gbuf[NZ + 1] = total + gbuf[NZ]

    def rows_of(q):
        return pl.ds(q * SUB_ROWS, SUB_ROWS)

    def c_copy(t, q, s):
        return rcopy(
            cout.at[t, rows_of(q)], cbuf.at[s, t, rows_of(q)], c_s, c_r.at[s, t, q], (inner, m)
        )

    def h_copy(t, q, dev):
        part = hbuf.at[t, rows_of(q)]
        return rcopy(part, part, h_s, h_r.at[t, q], dev)

    def step(i, carry):
        @pl.when(i == 8)
        def _():
            @pl.when(m < 15)
            def _():
                to_left.wait_recv()

            warp_group(NZ - 2)
            send_group(NZ - 2)

        @pl.when(i == 11)
        def _():
            @pl.when(m > 0)
            def _():
                to_right.wait_recv()

            warp_group(NZ - 1)
            send_group(NZ - 1)

        @pl.when(i < NP)
        def _():
            t = piece(i)
            with jax.named_scope("ywait"):
                for r in range(1, NY):
                    y_copy(r, t).wait_recv()
            mine = ws[:, pl.ds(own_bins(t), PW)]
            w_hi, w_lo = halves(jnp.concatenate([mine, wg[t].reshape(GROUP - ROWS, PW)], axis=0))
            both = jnp.concatenate([w_hi, w_lo], axis=0)
            wgb[t] = both
            n = jnp.dot(lhs[...], jnp.concatenate([both, w_hi], axis=0), preferred_element_type=F32)

            @pl.when(has_outer)
            def _():
                for q in range(SUB):
                    with jax.named_scope("cwait"):
                        c_copy(t, q, 0).wait_recv()
                    part = n[q * SUB_ROWS : (q + 1) * SUB_ROWS]
                    cout[t, rows_of(q)] = part + cbuf[0, t, rows_of(q)]
                    c_copy(t, q, slot).start()

            @pl.when(jnp.logical_not(has_outer))
            def _():
                cout[t] = n
                for q in range(SUB):
                    c_copy(t, q, slot).start()

            @pl.when(center)
            def _():
                @pl.when(lax.div(t, NPZ * (NZ // 2)) != lax.div(z, NZ // 2))
                def _():
                    with jax.named_scope("hcwait"):
                        h_relay(t).wait_recv()

                own = hc[t]
                bottom = jnp.dot(gbuf[NZ + 1], own, precision=exact_mode, preferred_element_type=F32) + EPSILON
                rbuf[t] = own / bottom

        k = i - lag

        @pl.when((k >= 0) & (k < NP))
        def _():
            t = piece(k)

            @pl.when(center)
            def _():
                for q in range(SUB):
                    with jax.named_scope("xcwait"):
                        c_copy(t, q, 1).wait_recv()
                    r = rows_of(q)
                    hbuf[t, r] = rbuf[t, r] * (cout[t, r] + cbuf[1, t, r])
                    h_copy(t, q, (outer, m)).start()

                    @pl.when(k >= NP - DIRECT)
                    def _():
                        for far_out in (2, 3):
                            h_copy(t, q, (outward(far_out) * NY + y, m)).start()

            @pl.when(jnp.logical_not(center))
            def _():
                for q in range(SUB):
                    with jax.named_scope("hwait"):
                        h_copy(t, q, (outer, m)).wait_recv()

                    @pl.when(has_outer & (k < NP - DIRECT))
                    def _():
                        h_copy(t, q, (outer, m)).start()

            h = hbuf[t]
            h_hi, h_lo = halves(h)
            right = jnp.concatenate([h_hi, h_lo], axis=0)
            left = jnp.concatenate([wgb[t], right], axis=0)
            acc[...] += lax.dot_general(left, right, NT, preferred_element_type=F32)

            @pl.when(lax.div(t, NPZ) == z)
            def _():
                hout_ref[:, pl.ds(pl.multiple_of(lax.rem(t, NPZ) * PW, 128), PW)] = h

        return carry

    lax.fori_loop(0, NP + LAGS[-1], step, 0)

    both = acc[:, 0:RANK] + acc[:, RANK : 2 * RANK]
    proj = both[0:GROUP] + both[GROUP : 2 * GROUP]
    base = 2 * GROUP
    gram = both[base : base + RANK] + both[base + RANK : base + 2 * RANK]
    gram8 = jnp.concatenate([gram[8 * q : 8 * q + 8] for q in range(4)], axis=1)
    for k in range(NY):
        rows = proj[k * ROWS : (k + 1) * ROWS]
        t0s[k, 0:8] = gram8
        t0s[k, 8:12] = jnp.concatenate([rows[4 * q : 4 * q + 4] for q in range(4)], axis=1)
    t0_copy = rcopy(t0s, t0r, t0_s, t0_r, partner)
    t0_copy.start()
    with jax.named_scope("t0wait"):
        t0_copy.wait_recv()
    t1s[...] = t0s[...] + t0r[...]

    me = y * 4 + lax.div(ml, 2)

    def t_copy(k):
        return rcopy(t1s.at[lax.div(k, 4)], t1r.at[me], t1_s.at[k], t1_r.at[k], plane_dev(k))

    t1_copies = [t_copy(k) for k in range(1, CHIPS)]
    for c in t1_copies:
        c.start()
    t1r[me] = t1s[0]
    with jax.named_scope("t1wait"):
        for c in t1_copies:
            c.wait_recv()
    sums = [t1r[k] for k in range(CHIPS)]
    while len(sums) > 1:
        sums = [a + b for a, b in zip(sums[::2], sums[1::2])]
    t3s[...] = sums[0]
    t3_copy = rcopy(t3s, t3r, t3_s, t3_r, far)
    t3_copy.start()
    with jax.named_scope("t3wait"):
        t3_copy.wait_recv()
    total = sums[0] + t3r[...]
    gram_sum = jnp.concatenate([total[0:8, 32 * q : 32 * q + 32] for q in range(4)], axis=0)
    proj_sum = jnp.concatenate([total[8:12, 32 * q : 32 * q + 32] for q in range(4)], axis=0)
    f = f_ref[...]
    g_hi, g_lo = halves(gram_sum)
    own_hi, own_lo = halves(f)
    bottom = EPSILON + jnp.dot(
        jnp.concatenate([own_hi, own_hi, own_lo], axis=1),
        jnp.concatenate([g_hi, g_lo, g_hi], axis=0),
        preferred_element_type=F32,
    )
    w_ref[...] = f * proj_sum / bottom

    for c in f_copies + t1_copies + [t0_copy, t3_copy]:
        c.wait_send()

    @pl.when(m < 15)
    def _():
        to_right.wait_send()

    @pl.when(m > 0)
    def _():
        to_left.wait_send()

    g_half.wait_send()
    def hc_sent(pieces):
        part = hc.at[pl.ds(0, pieces)]
        rcopy(part, part, hc_s, hc_s, (inner, m)).wait_send()

    @pl.when(center)
    def _():
        hc_sent(NPZ * (NZ // 2))

    @pl.when(jnp.logical_not(center))
    def _():
        hc_sent(NPZ)

    for r in range(1, NY):
        rcopy(wg.at[:, r - 1], wg.at[:, r - 1], y_s.at[r - 1], y_s.at[r - 1], y_dev(r)).wait_send()
    rcopy(cout, cout, c_s, c_s, (inner, m)).wait_send()

    def h_sent(pieces):
        part = hbuf.at[pl.ds(0, pieces)]
        rcopy(part, part, h_s, h_s, (outer, m)).wait_send()

    @pl.when(center)
    def _():
        h_sent(NP)
        h_sent(2 * DIRECT)

    @pl.when(has_outer & jnp.logical_not(center))
    def _():
        h_sent(NP - DIRECT)


def body(spectra, shifts, fractions, pixel_factors, spectral_factors):
    vmem = pl.BlockSpec(memory_space=pltpu.VMEM)
    dma = pltpu.SemaphoreType.DMA
    return pl.pallas_call(
        kernel,
        out_shape=(
            jax.ShapeDtypeStruct((ROWS, RANK), F32),
            jax.ShapeDtypeStruct((RANK, OWN), F32),
        ),
        in_specs=[pl.BlockSpec(memory_space=pltpu.HBM)] * 5,
        out_specs=(vmem, vmem),
        scratch_shapes=[
            pltpu.VMEM((ROWS, SEGS), jnp.int32),
            pltpu.VMEM((ROWS, SEGS), F32),
            pltpu.VMEM((ROWS, RANK), F32),
            pltpu.VMEM((RANK, OWN), F32),
            pltpu.VMEM((ROWS, BINS + 256), F32),
            pltpu.VMEM((SEGS, ROWS, 128), jnp.int32),
            pltpu.VMEM((SEGS, ROWS, 128), F32),
            pltpu.VMEM((ROWS, BINS), F32),
            pltpu.VMEM((NP, NY - 1, ROWS, PW), F32),
            pltpu.VMEM((NP, 2 * GROUP, PW), BF16),
            pltpu.VMEM((2, NP, RANK, PW), F32),
            pltpu.VMEM((NP, RANK, PW), F32),
            pltpu.VMEM((NP, RANK, PW), F32),
            pltpu.VMEM((NP, RANK, PW), F32),
            pltpu.VMEM((NP, RANK, PW), F32),
            pltpu.VMEM((NY - 1, ROWS, 128), F32),
            pltpu.VMEM((RANK, 3 * GROUP), BF16),
            pltpu.VMEM((RANK, RANK), F32),
            pltpu.VMEM((NZ + 2, RANK, RANK), F32),
            pltpu.VMEM((2 * GROUP + 2 * RANK, 2 * RANK), F32),
            pltpu.VMEM((ROWS, 128), F32),
            pltpu.VMEM((NY, 12, 128), F32),
            pltpu.VMEM((NY, 12, 128), F32),
            pltpu.VMEM((NY, 12, 128), F32),
            pltpu.VMEM((CHIPS, 12, 128), F32),
            pltpu.VMEM((12, 128), F32),
            pltpu.VMEM((12, 128), F32),
            dma((7,)),
            dma((2,)),
            dma((2,)),
            dma((NY - 1,)),
            dma((NY - 1,)),
            dma(()),
            dma((NP,)),
            dma(()),
            dma((NZ + 1,)),
            dma((NY - 1,)),
            dma((NP, NY - 1)),
            dma(()),
            dma((2, NP, SUB)),
            dma(()),
            dma((NP, SUB)),
            dma(()),
            dma(()),
            dma((CHIPS,)),
            dma((CHIPS,)),
            dma(()),
            dma(()),
        ],
        compiler_params=pltpu.CompilerParams(
            collective_id=0, has_side_effects=True, vmem_limit_bytes=66_000_000
        ),
    )(spectra, shifts, fractions, pixel_factors, spectral_factors)


def solution(mesh):
    return jax.shard_map(
        body,
        mesh=mesh,
        in_specs=(
            P("pix", "mz"),
            P("pix", "mz"),
            P("pix", "mz"),
            P("pix", None),
            P(None, ("mz", "pix")),
        ),
        out_specs=(P("pix", None), P(None, ("mz", "pix"))),
        check_vma=False,
    )
```

```python
import jax
import jax.numpy as jnp
from jax import lax
from jax.experimental import pallas as pl
from jax.experimental.pallas import tpu as pltpu
from jax.sharding import PartitionSpec as P

SEG = 2048
RANK = 32
EPSILON = 1e-06
ROWS = 16
BINS = 24576
SEGS = BINS // SEG
NZ, NY = 8, 4
OWN = 768
PW = 256
NPZ = OWN // PW
NP = NZ * NPZ
GROUP = NY * ROWS
LAGS = (4, 13, 22, 24)
LATE_WARP = 6
SUB = 2
SUB_ROWS = RANK // SUB
DIRECT = 2
CHUNK = 1024
GROUP_BINS = NY * OWN
EARLY = 6
CHIPS = 16
MESH = pl.DeviceIdType.MESH
F32 = jnp.float32
BF16 = jnp.bfloat16
exact_mode = lax.Precision.HIGHEST
NT = (((1,), (1,)), ((), ()))


def halves(v):
    hi = v.astype(BF16)
    return hi, (v - hi.astype(F32)).astype(BF16)


def kernel(
    x_hbm, sh_hbm, fr_hbm, f_hbm, hin_hbm, w_ref, hout_ref,
    sh_ref, fr_ref, f_ref, hin_ref,
    xp, shb, frb, ws, wg, wgb, cbuf, cout, hbuf, hc, rbuf, fbuf, lhs, gsend, gbuf, acc,
    f_all, t0s, t0r, t1s, t1r, t3s, t3r,
    xsem, halo_s, halo_r, f_s, f_r, hc_s, hc_r, g_s, g_r,
    y_s, y_r, c_s, c_r, h_s, h_r, t0_s, t0_r, t1_s, t1_r, t3_s, t3_r,
):
    p, m = lax.axis_index("pix"), lax.axis_index("mz")
    z, y = lax.div(p, NY), lax.rem(p, NY)
    mh, ml = lax.div(m, 8), lax.rem(m, 8)
    low_side = z < NZ // 2
    inner = jnp.where(low_side, p + NY, p - NY)
    outer = jnp.where(low_side, p - NY, p + NY)
    depth = jnp.where(low_side, NZ // 2 - 1 - z, z - NZ // 2)
    center = depth == 0
    slot = jnp.where(center, 1, 0)
    has_outer = depth < NZ // 2 - 1
    lag = jnp.where(
        depth == 0, LAGS[0], jnp.where(depth == 1, LAGS[1], jnp.where(depth == 2, LAGS[2], LAGS[3]))
    )

    def y_dev(r):
        return (z * NY + lax.rem(y + r, NY), m)

    def m_dev(r):
        return (p, mh * 8 + lax.rem(ml + r, 8))

    far = (p, lax.rem(m + 8, 16))

    def rcopy(src, dst, send, recv, dev):
        return pltpu.make_async_remote_copy(
            src_ref=src, dst_ref=dst, send_sem=send, recv_sem=recv, device_id=dev, device_id_type=MESH
        )

    small = [
        pltpu.make_async_copy(a, b, xsem.at[k])
        for k, (a, b) in enumerate(
            ((sh_hbm, sh_ref), (fr_hbm, fr_ref), (f_hbm, f_ref), (hin_hbm, hin_ref))
        )
    ]
    lo, hi = GROUP_BINS - 128, 2 * GROUP_BINS + 128
    parts = [
        pltpu.make_async_copy(
            x_hbm.at[:, pl.ds(a, b - a)], xp.at[:, pl.ds(128 + a, b - a)], xsem.at[4 + k]
        )
        for k, (a, b) in enumerate(((lo, hi), (hi, BINS), (0, lo)))
    ]
    for c in small[:2] + parts + small[2:]:
        c.start()

    barrier = pltpu.get_barrier_semaphore()

    def greet(dev):
        pl.semaphore_signal(barrier, inc=1, device_id=dev, device_id_type=MESH)

    core = lax.rem(ml, 2)
    partner = (p, m + 1 - 2 * core)

    def plane_dev(k):
        return (
            z * NY + lax.rem(y + lax.div(k, 4), NY),
            mh * 8 + lax.rem(ml + 2 * lax.rem(k, 4), 8),
        )

    for k in range(1, CHIPS):
        greet(plane_dev(k))
    greet(partner)
    greet(far)
    half = lax.div(z, NZ // 2) * (NZ // 2)
    for r in range(1, NZ // 2):
        greet(((half + lax.rem(z + r, NZ // 2)) * NY + y, m))

    @pl.when(center)
    def _():
        greet((inner, m))

    @pl.when((core == 0) & (m > 0))
    def _():
        greet((p, m - 1))

    @pl.when((core == 1) & (m < 15))
    def _():
        greet((p, m + 1))

    acc[...] = jnp.zeros_like(acc)

    @pl.when(m == 0)
    def _():
        xp[:, 0:128] = jnp.zeros((ROWS, 128), F32)

    @pl.when(m == 15)
    def _():
        xp[:, 128 + BINS :] = jnp.zeros((ROWS, 128), F32)

    small[0].wait()
    small[1].wait()
    for s in range(SEGS):
        shb[s] = jnp.broadcast_to(sh_ref[:, s : s + 1], (ROWS, 128))
        frb[s] = jnp.broadcast_to(fr_ref[:, s : s + 1], (ROWS, 128))

    def piece(i):
        return lax.rem(i + NPZ, NP)

    def own_bins(t):
        return first_bin(0, t)

    def first_bin(r, t):
        zq, j = lax.div(t, NPZ), lax.rem(t, NPZ)
        return pl.multiple_of(zq * GROUP_BINS + lax.rem(y + r, NY) * OWN + j * PW, 128)

    def warp(c):
        width = CHUNK + 256
        b = pl.multiple_of(c * CHUNK, 128)
        seg = lax.div(b, SEG)
        d, f = shb[seg], frb[seg]

        def wide(v, lanes):
            return jnp.concatenate([v] * (lanes // 128), axis=1)

        v = xp[:, pl.ds(b, width)]
        v = jnp.where(wide(d, width) < 0, pltpu.roll(v, 4, 1), v)
        shifted = [v] + [pltpu.roll(v, width - k, 1) for k in range(1, 5)]
        shifted = [u[:, 128 : 128 + CHUNK] for u in shifted]
        rest = wide(d & 3, CHUNK)
        high, odd = rest >= 2, (rest & 1) != 0

        def pick(k):
            return jnp.where(
                high,
                jnp.where(odd, shifted[k + 3], shifted[k + 2]),
                jnp.where(odd, shifted[k + 1], shifted[k]),
            )

        f = wide(f, CHUNK)
        ws[:, pl.ds(b, CHUNK)] = (1.0 - f) * pick(0) + f * pick(1)

    def warp_group(g):
        zq = lax.rem(g + 1, NZ)

        for k in range(GROUP_BINS // CHUNK):
            warp(zq * (GROUP_BINS // CHUNK) + k)

    def y_copy(r, t):
        src = ws.at[:, pl.ds(first_bin(r, t), PW)]
        return rcopy(src, wg.at[t, NY - r - 1], y_s.at[r - 1], y_r.at[t, NY - r - 1], y_dev(r))

    def send_group(g):
        zq = lax.rem(g + 1, NZ)
        for j in range(NPZ):
            for r in range(1, NY):
                y_copy(r, zq * NPZ + j).start()

    parts[0].wait()
    with jax.named_scope("warps"):
        warp_group(0)
    small[2].wait()
    f_all[...] = jnp.concatenate([f_ref[...], jnp.zeros((ROWS, 128 - RANK), F32)], axis=1)
    with jax.named_scope("barrier"):
        pl.semaphore_wait(
            barrier,
            CHIPS + 1 + NZ // 2 - 1 + jnp.where(center, 1, 0) + jnp.where((m == 0) | (m == 15), 0, 1),
        )

    f_copies = [
        rcopy(f_all, fbuf.at[NY - r - 1], f_s.at[r - 1], f_r.at[NY - r - 1], y_dev(r)) for r in range(1, NY)
    ]
    for c in f_copies:
        c.start()
    send_group(0)
    parts[1].wait()
    parts[2].wait()
    small[3].wait()

    to_right = rcopy(
        xp.at[:, pl.ds(BINS, 128)], xp.at[:, pl.ds(0, 128)], halo_s.at[0], halo_r.at[0], (p, m + 1)
    )
    to_left = rcopy(
        xp.at[:, pl.ds(128, 128)], xp.at[:, pl.ds(128 + BINS, 128)], halo_s.at[1], halo_r.at[1], (p, m - 1)
    )

    @pl.when(m < 15)
    def _():
        to_right.start()

    @pl.when(m > 0)
    def _():
        to_left.start()

    near = jnp.where(low_side, NZ // 2 - 1, NZ // 2)

    def h_part(j):
        t = z * NPZ + j
        dev = (jnp.where(center, inner, near * NY + y), m)
        return rcopy(hin_ref.at[:, pl.ds(j * PW, PW)], hc.at[t], hc_s, hc_r.at[t], dev)

    def h_relay(t):
        return rcopy(hc.at[t], hc.at[t], hc_s, hc_r.at[t], (inner, m))

    for j in range(NPZ):
        h_part(j).start()

    @pl.when(center)
    def _():
        for j in range(NPZ):
            hc[z * NPZ + j] = hin_ref[:, j * PW : (j + 1) * PW]

    def early(g, carry):
        warp_group(g)
        send_group(g)
        return carry

    with jax.named_scope("warps"):
        lax.fori_loop(1, EARLY, early, 0)

    with jax.named_scope("fwait"):
        for c in f_copies:
            c.wait_recv()
    fg = jnp.concatenate([f_all[...], fbuf[...].reshape(GROUP - ROWS, 128)], axis=0)[:, 0:RANK]
    gy = lax.dot_general(fg, fg, (((0,), (0,)), ((), ())), precision=exact_mode, preferred_element_type=F32)
    f_hi, f_lo = halves(fg.T)
    lhs[...] = jnp.concatenate([f_hi, f_hi, f_lo], axis=1)

    g_half = rcopy(gsend, gbuf.at[z], g_s, g_r.at[z], (near * NY + y, m))
    g_other = rcopy(gsend, gbuf.at[NZ], g_s, g_r.at[NZ], (inner, m))

    def outward(k):
        return jnp.where(low_side, NZ // 2 - 1 - k, NZ // 2 + k)

    @pl.when(jnp.logical_not(center))
    def _():
        gsend[...] = gy
        g_half.start()

    @pl.when(center)
    def _():
        total = gy
        for k in range(1, NZ // 2):
            zk = outward(k)
            rcopy(gsend, gbuf.at[zk], g_s, g_r.at[zk], (inner, m)).wait_recv()
            total = total + gbuf[zk]
        gsend[...] = total
        g_other.start()
        with jax.named_scope("relay"):
            for k in range(1, NZ // 2):
                for j in range(NPZ):
                    t = outward(k) * NPZ + j
                    h_relay(t).wait_recv()
                    h_relay(t).start()
        g_other.wait_recv()
        gbuf[NZ + 1] = total + gbuf[NZ]

    def rows_of(q):
        return pl.ds(q * SUB_ROWS, SUB_ROWS)

    def c_copy(t, q, s):
        return rcopy(
            cout.at[t, rows_of(q)], cbuf.at[s, t, rows_of(q)], c_s, c_r.at[s, t, q], (inner, m)
        )

    def h_copy(t, q, dev):
        part = hbuf.at[t, rows_of(q)]
        return rcopy(part, part, h_s, h_r.at[t, q], dev)

    def step(i, carry):
        @pl.when(i < NP)
        def _():
            t = piece(i)
            with jax.named_scope("ywait"):
                for r in range(1, NY):
                    y_copy(r, t).wait_recv()
            mine = ws[:, pl.ds(own_bins(t), PW)]
            w_hi, w_lo = halves(jnp.concatenate([mine, wg[t].reshape(GROUP - ROWS, PW)], axis=0))
            both = jnp.concatenate([w_hi, w_lo], axis=0)
            wgb[t] = both
            n = jnp.dot(lhs[...], jnp.concatenate([both, w_hi], axis=0), preferred_element_type=F32)

            @pl.when(i == jnp.where(has_outer, 0, LATE_WARP))
            def _():
                @pl.when(m < 15)
                def _():
                    to_left.wait_recv()

                @pl.when(m > 0)
                def _():
                    to_right.wait_recv()

                def late(g, carry):
                    warp_group(g)
                    send_group(g)
                    return carry

                lax.fori_loop(EARLY, NZ, late, 0)

            @pl.when(has_outer)
            def _():
                for q in range(SUB):
                    with jax.named_scope("cwait"):
                        c_copy(t, q, 0).wait_recv()
                    part = n[q * SUB_ROWS : (q + 1) * SUB_ROWS]
                    cout[t, rows_of(q)] = part + cbuf[0, t, rows_of(q)]
                    c_copy(t, q, slot).start()

            @pl.when(jnp.logical_not(has_outer))
            def _():
                cout[t] = n
                for q in range(SUB):
                    c_copy(t, q, slot).start()

            @pl.when(center)
            def _():
                @pl.when(lax.div(t, NPZ * (NZ // 2)) != lax.div(z, NZ // 2))
                def _():
                    with jax.named_scope("hcwait"):
                        h_relay(t).wait_recv()

                own = hc[t]
                bottom = jnp.dot(gbuf[NZ + 1], own, precision=exact_mode, preferred_element_type=F32) + EPSILON
                rbuf[t] = own / bottom

        k = i - lag

        @pl.when((k >= 0) & (k < NP))
        def _():
            t = piece(k)

            @pl.when(center)
            def _():
                for q in range(SUB):
                    with jax.named_scope("xcwait"):
                        c_copy(t, q, 1).wait_recv()
                    r = rows_of(q)
                    hbuf[t, r] = rbuf[t, r] * (cout[t, r] + cbuf[1, t, r])
                    h_copy(t, q, (outer, m)).start()

                    @pl.when(k >= NP - DIRECT)
                    def _():
                        for far_out in (2, 3):
                            h_copy(t, q, (outward(far_out) * NY + y, m)).start()

            @pl.when(jnp.logical_not(center))
            def _():
                for q in range(SUB):
                    with jax.named_scope("hwait"):
                        h_copy(t, q, (outer, m)).wait_recv()

                    @pl.when(has_outer & (k < NP - DIRECT))
                    def _():
                        h_copy(t, q, (outer, m)).start()

            h = hbuf[t]
            h_hi, h_lo = halves(h)
            right = jnp.concatenate([h_hi, h_lo], axis=0)
            left = jnp.concatenate([wgb[t], right], axis=0)
            acc[...] += lax.dot_general(left, right, NT, preferred_element_type=F32)

            @pl.when(lax.div(t, NPZ) == z)
            def _():
                hout_ref[:, pl.ds(pl.multiple_of(lax.rem(t, NPZ) * PW, 128), PW)] = h

        return carry

    lax.fori_loop(0, NP + LAGS[-1], step, 0)

    both = acc[:, 0:RANK] + acc[:, RANK : 2 * RANK]
    proj = both[0:GROUP] + both[GROUP : 2 * GROUP]
    base = 2 * GROUP
    gram = both[base : base + RANK] + both[base + RANK : base + 2 * RANK]
    gram8 = jnp.concatenate([gram[8 * q : 8 * q + 8] for q in range(4)], axis=1)
    for k in range(NY):
        rows = proj[k * ROWS : (k + 1) * ROWS]
        t0s[k, 0:8] = gram8
        t0s[k, 8:12] = jnp.concatenate([rows[4 * q : 4 * q + 4] for q in range(4)], axis=1)
    t0_copy = rcopy(t0s, t0r, t0_s, t0_r, partner)
    t0_copy.start()
    with jax.named_scope("t0wait"):
        t0_copy.wait_recv()
    t1s[...] = t0s[...] + t0r[...]

    me = y * 4 + lax.div(ml, 2)

    def t_copy(k):
        return rcopy(t1s.at[lax.div(k, 4)], t1r.at[me], t1_s.at[k], t1_r.at[k], plane_dev(k))

    t1_copies = [t_copy(k) for k in range(1, CHIPS)]
    for c in t1_copies:
        c.start()
    t1r[me] = t1s[0]
    with jax.named_scope("t1wait"):
        for c in t1_copies:
            c.wait_recv()
    sums = [t1r[k] for k in range(CHIPS)]
    while len(sums) > 1:
        sums = [a + b for a, b in zip(sums[::2], sums[1::2])]
    t3s[...] = sums[0]
    t3_copy = rcopy(t3s, t3r, t3_s, t3_r, far)
    t3_copy.start()
    with jax.named_scope("t3wait"):
        t3_copy.wait_recv()
    total = sums[0] + t3r[...]
    gram_sum = jnp.concatenate([total[0:8, 32 * q : 32 * q + 32] for q in range(4)], axis=0)
    proj_sum = jnp.concatenate([total[8:12, 32 * q : 32 * q + 32] for q in range(4)], axis=0)
    f = f_ref[...]
    g_hi, g_lo = halves(gram_sum)
    own_hi, own_lo = halves(f)
    bottom = EPSILON + jnp.dot(
        jnp.concatenate([own_hi, own_hi, own_lo], axis=1),
        jnp.concatenate([g_hi, g_lo, g_hi], axis=0),
        preferred_element_type=F32,
    )
    w_ref[...] = f * proj_sum / bottom

    for c in f_copies + t1_copies + [t0_copy, t3_copy]:
        c.wait_send()

    @pl.when(m < 15)
    def _():
        to_right.wait_send()

    @pl.when(m > 0)
    def _():
        to_left.wait_send()

    g_half.wait_send()
    def hc_sent(pieces):
        part = hc.at[pl.ds(0, pieces)]
        rcopy(part, part, hc_s, hc_s, (inner, m)).wait_send()

    @pl.when(center)
    def _():
        hc_sent(NPZ * (NZ // 2))

    @pl.when(jnp.logical_not(center))
    def _():
        hc_sent(NPZ)

    for r in range(1, NY):
        rcopy(wg.at[:, r - 1], wg.at[:, r - 1], y_s.at[r - 1], y_s.at[r - 1], y_dev(r)).wait_send()
    rcopy(cout, cout, c_s, c_s, (inner, m)).wait_send()

    def h_sent(pieces):
        part = hbuf.at[pl.ds(0, pieces)]
        rcopy(part, part, h_s, h_s, (outer, m)).wait_send()

    @pl.when(center)
    def _():
        h_sent(NP)
        h_sent(2 * DIRECT)

    @pl.when(has_outer & jnp.logical_not(center))
    def _():
        h_sent(NP - DIRECT)


def body(spectra, shifts, fractions, pixel_factors, spectral_factors):
    vmem = pl.BlockSpec(memory_space=pltpu.VMEM)
    dma = pltpu.SemaphoreType.DMA
    return pl.pallas_call(
        kernel,
        out_shape=(
            pltpu.VMEM((ROWS, RANK), F32),
            pltpu.VMEM((RANK, OWN), F32),
        ),
        in_specs=[pl.BlockSpec(memory_space=pltpu.HBM)] * 5,
        out_specs=(vmem, vmem),
        scratch_shapes=[
            pltpu.VMEM((ROWS, SEGS), jnp.int32),
            pltpu.VMEM((ROWS, SEGS), F32),
            pltpu.VMEM((ROWS, RANK), F32),
            pltpu.VMEM((RANK, OWN), F32),
            pltpu.VMEM((ROWS, BINS + 256), F32),
            pltpu.VMEM((SEGS, ROWS, 128), jnp.int32),
            pltpu.VMEM((SEGS, ROWS, 128), F32),
            pltpu.VMEM((ROWS, BINS), F32),
            pltpu.VMEM((NP, NY - 1, ROWS, PW), F32),
            pltpu.VMEM((NP, 2 * GROUP, PW), BF16),
            pltpu.VMEM((2, NP, RANK, PW), F32),
            pltpu.VMEM((NP, RANK, PW), F32),
            pltpu.VMEM((NP, RANK, PW), F32),
            pltpu.VMEM((NP, RANK, PW), F32),
            pltpu.VMEM((NP, RANK, PW), F32),
            pltpu.VMEM((NY - 1, ROWS, 128), F32),
            pltpu.VMEM((RANK, 3 * GROUP), BF16),
            pltpu.VMEM((RANK, RANK), F32),
            pltpu.VMEM((NZ + 2, RANK, RANK), F32),
            pltpu.VMEM((2 * GROUP + 2 * RANK, 2 * RANK), F32),
            pltpu.VMEM((ROWS, 128), F32),
            pltpu.VMEM((NY, 12, 128), F32),
            pltpu.VMEM((NY, 12, 128), F32),
            pltpu.VMEM((NY, 12, 128), F32),
            pltpu.VMEM((CHIPS, 12, 128), F32),
            pltpu.VMEM((12, 128), F32),
            pltpu.VMEM((12, 128), F32),
            dma((7,)),
            dma((2,)),
            dma((2,)),
            dma((NY - 1,)),
            dma((NY - 1,)),
            dma(()),
            dma((NP,)),
            dma(()),
            dma((NZ + 1,)),
            dma((NY - 1,)),
            dma((NP, NY - 1)),
            dma(()),
            dma((2, NP, SUB)),
            dma(()),
            dma((NP, SUB)),
            dma(()),
            dma(()),
            dma((CHIPS,)),
            dma((CHIPS,)),
            dma(()),
            dma(()),
        ],
        compiler_params=pltpu.CompilerParams(
            collective_id=0, has_side_effects=True, vmem_limit_bytes=66_000_000
        ),
    )(spectra, shifts, fractions, pixel_factors, spectral_factors)


def solution(mesh):
    return jax.shard_map(
        body,
        mesh=mesh,
        in_specs=(
            P("pix", "mz"),
            P("pix", "mz"),
            P("pix", "mz"),
            P("pix", None),
            P(None, ("mz", "pix")),
        ),
        out_specs=(P("pix", None), P(None, ("mz", "pix"))),
        check_vma=False,
    )
```

```python
import jax
import jax.numpy as jnp
from jax import lax
from jax.experimental import pallas as pl
from jax.experimental.pallas import tpu as pltpu
from jax.sharding import PartitionSpec as P

SEG = 2048
RANK = 32
EPSILON = 1e-06
ROWS = 16
BINS = 24576
SEGS = BINS // SEG
NZ, NY = 8, 4
OWN = 768
PW = 256
NPZ = OWN // PW
NP = NZ * NPZ
GROUP = NY * ROWS
LAGS = (6, 14, 22, 24)
LATE_OUT, LATE_FAR = 6, 8
SUB = 2
SUB_ROWS = RANK // SUB
DIRECT = 2
CHUNK = 1024
GROUP_BINS = NY * OWN
EARLY = 6
CHIPS = 16
MESH = pl.DeviceIdType.MESH
F32 = jnp.float32
BF16 = jnp.bfloat16
exact_mode = lax.Precision.HIGHEST
NT = (((1,), (1,)), ((), ()))


def halves(v):
    hi = v.astype(BF16)
    return hi, (v - hi.astype(F32)).astype(BF16)


def kernel(
    x_hbm, sh_hbm, fr_hbm, f_hbm, hin_hbm, w_ref, hout_ref,
    sh_ref, fr_ref, f_ref, hin_ref,
    xp, shb, frb, ws, wg, wgb, cbuf, cout, hbuf, hc, rbuf, fbuf, lhs, gsend, gbuf, acc,
    f_all, t0s, t0r, t1s, t1r, t3s, t3r,
    xsem, halo_s, halo_r, f_s, f_r, hc_s, hc_r, g_s, g_r,
    y_s, y_r, c_s, c_r, h_s, x_r, t0_s, t0_r, t1_s, t1_r, t3_s, t3_r,
):
    p, m = lax.axis_index("pix"), lax.axis_index("mz")
    z, y = lax.div(p, NY), lax.rem(p, NY)
    mh, ml = lax.div(m, 8), lax.rem(m, 8)
    low_side = z < NZ // 2
    inner = jnp.where(low_side, p + NY, p - NY)
    outer = jnp.where(low_side, p - NY, p + NY)
    depth = jnp.where(low_side, NZ // 2 - 1 - z, z - NZ // 2)
    center = depth == 0
    has_outer = depth < NZ // 2 - 1
    lag = jnp.where(
        depth == 0, LAGS[0], jnp.where(depth == 1, LAGS[1], jnp.where(depth == 2, LAGS[2], LAGS[3]))
    )

    def y_dev(r):
        return (z * NY + lax.rem(y + r, NY), m)

    def m_dev(r):
        return (p, mh * 8 + lax.rem(ml + r, 8))

    far = (p, lax.rem(m + 8, 16))

    def rcopy(src, dst, send, recv, dev):
        return pltpu.make_async_remote_copy(
            src_ref=src, dst_ref=dst, send_sem=send, recv_sem=recv, device_id=dev, device_id_type=MESH
        )

    small = [
        pltpu.make_async_copy(a, b, xsem.at[k])
        for k, (a, b) in enumerate(
            ((sh_hbm, sh_ref), (fr_hbm, fr_ref), (f_hbm, f_ref), (hin_hbm, hin_ref))
        )
    ]
    lo, hi = GROUP_BINS - 128, 2 * GROUP_BINS + 128
    parts = [
        pltpu.make_async_copy(
            x_hbm.at[:, pl.ds(a, b - a)], xp.at[:, pl.ds(128 + a, b - a)], xsem.at[4 + k]
        )
        for k, (a, b) in enumerate(((lo, hi), (hi, BINS), (0, lo)))
    ]
    for c in small[:2] + parts + small[2:]:
        c.start()

    barrier = pltpu.get_barrier_semaphore()

    def greet(dev):
        pl.semaphore_signal(barrier, inc=1, device_id=dev, device_id_type=MESH)

    core = lax.rem(ml, 2)
    partner = (p, m + 1 - 2 * core)

    def plane_dev(k):
        return (
            z * NY + lax.rem(y + lax.div(k, 4), NY),
            mh * 8 + lax.rem(ml + 2 * lax.rem(k, 4), 8),
        )

    for k in range(1, CHIPS):
        greet(plane_dev(k))
    greet(partner)
    greet(far)
    half = lax.div(z, NZ // 2) * (NZ // 2)
    for r in range(1, NZ // 2):
        greet(((half + lax.rem(z + r, NZ // 2)) * NY + y, m))

    @pl.when(center)
    def _():
        greet((inner, m))

    @pl.when((core == 0) & (m > 0))
    def _():
        greet((p, m - 1))

    @pl.when((core == 1) & (m < 15))
    def _():
        greet((p, m + 1))

    acc[...] = jnp.zeros_like(acc)

    @pl.when(m == 0)
    def _():
        xp[:, 0:128] = jnp.zeros((ROWS, 128), F32)

    @pl.when(m == 15)
    def _():
        xp[:, 128 + BINS :] = jnp.zeros((ROWS, 128), F32)

    small[0].wait()
    small[1].wait()
    for s in range(SEGS):
        shb[s] = jnp.broadcast_to(sh_ref[:, s : s + 1], (ROWS, 128))
        frb[s] = jnp.broadcast_to(fr_ref[:, s : s + 1], (ROWS, 128))

    def piece(i):
        return lax.rem(i + NPZ, NP)

    def own_bins(t):
        return first_bin(0, t)

    def first_bin(r, t):
        zq, j = lax.div(t, NPZ), lax.rem(t, NPZ)
        return pl.multiple_of(zq * GROUP_BINS + lax.rem(y + r, NY) * OWN + j * PW, 128)

    def warp(c):
        width = CHUNK + 256
        b = pl.multiple_of(c * CHUNK, 128)
        seg = lax.div(b, SEG)
        d, f = shb[seg], frb[seg]

        def wide(v, lanes):
            return jnp.concatenate([v] * (lanes // 128), axis=1)

        v = xp[:, pl.ds(b, width)]
        v = jnp.where(wide(d, width) < 0, pltpu.roll(v, 4, 1), v)
        shifted = [v] + [pltpu.roll(v, width - k, 1) for k in range(1, 5)]
        shifted = [u[:, 128 : 128 + CHUNK] for u in shifted]
        rest = wide(d & 3, CHUNK)
        high, odd = rest >= 2, (rest & 1) != 0

        def pick(k):
            return jnp.where(
                high,
                jnp.where(odd, shifted[k + 3], shifted[k + 2]),
                jnp.where(odd, shifted[k + 1], shifted[k]),
            )

        f = wide(f, CHUNK)
        ws[:, pl.ds(b, CHUNK)] = (1.0 - f) * pick(0) + f * pick(1)

    def warp_group(g):
        zq = lax.rem(g + 1, NZ)

        for k in range(GROUP_BINS // CHUNK):
            warp(zq * (GROUP_BINS // CHUNK) + k)

    def y_copy(r, t):
        src = ws.at[:, pl.ds(first_bin(r, t), PW)]
        return rcopy(src, wg.at[t, NY - r - 1], y_s.at[r - 1], y_r.at[t], y_dev(r))

    def send_group(g):
        zq = lax.rem(g + 1, NZ)
        for j in range(NPZ):
            for r in range(1, NY):
                y_copy(r, zq * NPZ + j).start()

    parts[0].wait()
    with jax.named_scope("warps"):
        warp_group(0)
    small[2].wait()
    f_all[...] = jnp.concatenate([f_ref[...], jnp.zeros((ROWS, 128 - RANK), F32)], axis=1)
    with jax.named_scope("barrier"):
        pl.semaphore_wait(
            barrier,
            CHIPS + 1 + NZ // 2 - 1 + jnp.where(center, 1, 0) + jnp.where((m == 0) | (m == 15), 0, 1),
        )

    f_copies = [
        rcopy(f_all, fbuf.at[NY - r - 1], f_s, f_r, y_dev(r)) for r in range(1, NY)
    ]
    for c in f_copies:
        c.start()
    send_group(0)
    parts[1].wait()
    parts[2].wait()
    small[3].wait()

    to_right = rcopy(
        xp.at[:, pl.ds(BINS, 128)], xp.at[:, pl.ds(0, 128)], halo_s.at[0], halo_r.at[0], (p, m + 1)
    )
    to_left = rcopy(
        xp.at[:, pl.ds(128, 128)], xp.at[:, pl.ds(128 + BINS, 128)], halo_s.at[1], halo_r.at[1], (p, m - 1)
    )

    @pl.when(m < 15)
    def _():
        to_right.start()

    @pl.when(m > 0)
    def _():
        to_left.start()

    near = jnp.where(low_side, NZ // 2 - 1, NZ // 2)

    h_part = rcopy(hin_ref, hc.at[z], hc_s, hc_r.at[z], (jnp.where(center, inner, near * NY + y), m))

    def h_relay(zk):
        return rcopy(hc.at[zk], hc.at[zk], hc_s, hc_r.at[zk], (inner, m))

    h_part.start()

    @pl.when(center)
    def _():
        hc[z] = hin_ref[...]

    def early(g, carry):
        warp_group(g)
        send_group(g)
        return carry

    with jax.named_scope("warps"):
        lax.fori_loop(1, EARLY, early, 0)

    with jax.named_scope("fwait"):
        rcopy(fbuf, fbuf, f_s, f_r, y_dev(1)).wait_recv()
    fg = jnp.concatenate([f_all[...], fbuf[...].reshape(GROUP - ROWS, 128)], axis=0)[:, 0:RANK]
    gy = lax.dot_general(fg, fg, (((0,), (0,)), ((), ())), precision=exact_mode, preferred_element_type=F32)
    f_hi, f_lo = halves(fg.T)
    lhs[...] = jnp.concatenate([f_hi, f_hi, f_lo], axis=1)

    g_half = rcopy(gsend, gbuf.at[depth], g_s, g_r.at[depth], (near * NY + y, m))
    g_other = rcopy(gsend, gbuf.at[0], g_s, g_r.at[0], (inner, m))

    def outward(k):
        return jnp.where(low_side, NZ // 2 - 1 - k, NZ // 2 + k)

    def warp_late():
        @pl.when(m < 15)
        def _():
            to_left.wait_recv()

        @pl.when(m > 0)
        def _():
            to_right.wait_recv()

        lax.fori_loop(EARLY, NZ, early, 0)

    @pl.when(jnp.logical_not(center))
    def _():
        gsend[...] = gy
        g_half.start()

    @pl.when(center)
    def _():
        total = gy
        for k in range(1, NZ // 2):
            rcopy(gsend, gbuf.at[k], g_s, g_r.at[k], (inner, m)).wait_recv()
            total = total + gbuf[k]
        gsend[...] = total
        g_other.start()
        warp_late()
        with jax.named_scope("relay"):
            for k in range(1, NZ // 2):
                h_relay(outward(k)).wait_recv()
                h_relay(outward(k)).start()
        g_other.wait_recv()
        gbuf[NZ // 2] = total + gbuf[0]

    across = (m == 7) | (m == 8)
    late_step = jnp.where(has_outer, jnp.where(center, -1, jnp.where(across, LATE_FAR, 0)), LATE_OUT)

    def rows_of(q):
        return pl.ds(q * SUB_ROWS, SUB_ROWS)

    def c_copy(t, q):
        dst = cbuf.at[0, t, rows_of(q)]
        return rcopy(cout.at[t, rows_of(q)], dst, c_s, c_r.at[t, q], (inner, m))

    def cx_copy(t, q):
        dst = cbuf.at[1, t, rows_of(q)]
        return rcopy(cout.at[t, rows_of(q)], dst, c_s, x_r.at[t, q], (inner, m))

    def c_send(t, q):
        @pl.when(center)
        def _():
            cx_copy(t, q).start()

        @pl.when(jnp.logical_not(center))
        def _():
            c_copy(t, q).start()

    def h_copy(t, q, dev):
        part = hbuf.at[t, rows_of(q)]
        return rcopy(part, part, h_s, x_r.at[t, q], dev)

    def step(i, carry):
        @pl.when(i < NP)
        def _():
            t = piece(i)
            with jax.named_scope("ywait"):
                rcopy(wg.at[t], wg.at[t], y_s.at[0], y_r.at[t], y_dev(1)).wait_recv()
            mine = ws[:, pl.ds(own_bins(t), PW)]
            w_hi, w_lo = halves(jnp.concatenate([mine, wg[t].reshape(GROUP - ROWS, PW)], axis=0))
            both = jnp.concatenate([w_hi, w_lo], axis=0)
            wgb[t] = both
            n = jnp.dot(lhs[...], jnp.concatenate([both, w_hi], axis=0), preferred_element_type=F32)

            @pl.when(i == late_step)
            def _():
                warp_late()

            @pl.when(has_outer)
            def _():
                for q in range(SUB):
                    with jax.named_scope("cwait"):
                        c_copy(t, q).wait_recv()
                    part = n[q * SUB_ROWS : (q + 1) * SUB_ROWS]
                    cout[t, rows_of(q)] = part + cbuf[0, t, rows_of(q)]
                    c_send(t, q)

            @pl.when(jnp.logical_not(has_outer))
            def _():
                cout[t] = n
                for q in range(SUB):
                    c_send(t, q)

            @pl.when(center)
            def _():
                zq, j = lax.div(t, NPZ), lax.rem(t, NPZ)

                @pl.when((j == 0) & (lax.div(zq, NZ // 2) != lax.div(z, NZ // 2)))
                def _():
                    with jax.named_scope("hcwait"):
                        h_relay(zq).wait_recv()

                own = hc[zq, :, pl.ds(pl.multiple_of(j * PW, 128), PW)]
                bottom = jnp.dot(gbuf[NZ // 2], own, precision=exact_mode, preferred_element_type=F32) + EPSILON
                rbuf[t] = own / bottom

        k = i - lag

        @pl.when((k >= 0) & (k < NP))
        def _():
            t = piece(k)

            @pl.when(center)
            def _():
                for q in range(SUB):
                    with jax.named_scope("xcwait"):
                        cx_copy(t, q).wait_recv()
                    r = rows_of(q)
                    hbuf[t, r] = rbuf[t, r] * (cout[t, r] + cbuf[1, t, r])
                    h_copy(t, q, (outer, m)).start()

                    @pl.when(k >= NP - DIRECT)
                    def _():
                        for far_out in (2, 3):
                            h_copy(t, q, (outward(far_out) * NY + y, m)).start()

            @pl.when(jnp.logical_not(center))
            def _():
                for q in range(SUB):
                    with jax.named_scope("hwait"):
                        h_copy(t, q, (outer, m)).wait_recv()

                    @pl.when(has_outer & (k < NP - DIRECT))
                    def _():
                        h_copy(t, q, (outer, m)).start()

            h = hbuf[t]
            h_hi, h_lo = halves(h)
            right = jnp.concatenate([h_hi, h_lo], axis=0)
            left = jnp.concatenate([wgb[t], right], axis=0)
            acc[...] += lax.dot_general(left, right, NT, preferred_element_type=F32)

            @pl.when(lax.div(t, NPZ) == z)
            def _():
                hout_ref[:, pl.ds(pl.multiple_of(lax.rem(t, NPZ) * PW, 128), PW)] = h

        return carry

    lax.fori_loop(0, NP + LAGS[-1], step, 0)

    both = acc[:, 0:RANK] + acc[:, RANK : 2 * RANK]
    proj = both[0:GROUP] + both[GROUP : 2 * GROUP]
    base = 2 * GROUP
    gram = both[base : base + RANK] + both[base + RANK : base + 2 * RANK]
    gram8 = jnp.concatenate([gram[8 * q : 8 * q + 8] for q in range(4)], axis=1)
    for k in range(NY):
        rows = proj[k * ROWS : (k + 1) * ROWS]
        t0s[k, 0:8] = gram8
        t0s[k, 8:12] = jnp.concatenate([rows[4 * q : 4 * q + 4] for q in range(4)], axis=1)
    t0_copy = rcopy(t0s, t0r, t0_s, t0_r, partner)
    t0_copy.start()
    with jax.named_scope("t0wait"):
        t0_copy.wait_recv()
    t1s[...] = t0s[...] + t0r[...]

    me = y * 4 + lax.div(ml, 2)

    def t_copy(k):
        return rcopy(t1s.at[lax.div(k, 4)], t1r.at[me], t1_s.at[k], t1_r.at[k], plane_dev(k))

    t1_copies = [t_copy(k) for k in range(1, CHIPS)]
    for c in t1_copies:
        c.start()
    t1r[me] = t1s[0]
    with jax.named_scope("t1wait"):
        for c in t1_copies:
            c.wait_recv()
    sums = [t1r[k] for k in range(CHIPS)]
    while len(sums) > 1:
        sums = [a + b for a, b in zip(sums[::2], sums[1::2])]
    t3s[...] = sums[0]
    t3_copy = rcopy(t3s, t3r, t3_s, t3_r, far)
    t3_copy.start()
    with jax.named_scope("t3wait"):
        t3_copy.wait_recv()
    total = sums[0] + t3r[...]
    gram_sum = jnp.concatenate([total[0:8, 32 * q : 32 * q + 32] for q in range(4)], axis=0)
    proj_sum = jnp.concatenate([total[8:12, 32 * q : 32 * q + 32] for q in range(4)], axis=0)
    f = f_ref[...]
    g_hi, g_lo = halves(gram_sum)
    own_hi, own_lo = halves(f)
    bottom = EPSILON + jnp.dot(
        jnp.concatenate([own_hi, own_hi, own_lo], axis=1),
        jnp.concatenate([g_hi, g_lo, g_hi], axis=0),
        preferred_element_type=F32,
    )
    w_ref[...] = f * proj_sum / bottom

    rcopy(fbuf, fbuf, f_s, f_r, y_dev(1)).wait_send()
    for c in t1_copies + [t0_copy, t3_copy]:
        c.wait_send()

    @pl.when(m < 15)
    def _():
        to_right.wait_send()

    @pl.when(m > 0)
    def _():
        to_left.wait_send()

    g_half.wait_send()
    h_part.wait_send()

    @pl.when(center)
    def _():
        part = hc.at[pl.ds(0, NZ // 2 - 1)]
        rcopy(part, part, hc_s, hc_s, (inner, m)).wait_send()

    for r in range(1, NY):
        rcopy(wg.at[:, r - 1], wg.at[:, r - 1], y_s.at[r - 1], y_s.at[r - 1], y_dev(r)).wait_send()
    rcopy(cout, cout, c_s, c_s, (inner, m)).wait_send()

    def h_sent(pieces):
        part = hbuf.at[pl.ds(0, pieces)]
        rcopy(part, part, h_s, h_s, (outer, m)).wait_send()

    @pl.when(center)
    def _():
        h_sent(NP)
        h_sent(2 * DIRECT)

    @pl.when(has_outer & jnp.logical_not(center))
    def _():
        h_sent(NP - DIRECT)


def body(spectra, shifts, fractions, pixel_factors, spectral_factors):
    vmem = pl.BlockSpec(memory_space=pltpu.VMEM)
    dma = pltpu.SemaphoreType.DMA
    return pl.pallas_call(
        kernel,
        out_shape=(
            pltpu.VMEM((ROWS, RANK), F32),
            pltpu.VMEM((RANK, OWN), F32),
        ),
        in_specs=[pl.BlockSpec(memory_space=pltpu.HBM)] * 5,
        out_specs=(vmem, vmem),
        scratch_shapes=[
            pltpu.VMEM((ROWS, SEGS), jnp.int32),
            pltpu.VMEM((ROWS, SEGS), F32),
            pltpu.VMEM((ROWS, RANK), F32),
            pltpu.VMEM((RANK, OWN), F32),
            pltpu.VMEM((ROWS, BINS + 256), F32),
            pltpu.VMEM((SEGS, ROWS, 128), jnp.int32),
            pltpu.VMEM((SEGS, ROWS, 128), F32),
            pltpu.VMEM((ROWS, BINS), F32),
            pltpu.VMEM((NP, NY - 1, ROWS, PW), F32),
            pltpu.VMEM((NP, 2 * GROUP, PW), BF16),
            pltpu.VMEM((2, NP, RANK, PW), F32),
            pltpu.VMEM((NP, RANK, PW), F32),
            pltpu.VMEM((NP, RANK, PW), F32),
            pltpu.VMEM((NZ, RANK, OWN), F32),
            pltpu.VMEM((NP, RANK, PW), F32),
            pltpu.VMEM((NY - 1, ROWS, 128), F32),
            pltpu.VMEM((RANK, 3 * GROUP), BF16),
            pltpu.VMEM((RANK, RANK), F32),
            pltpu.VMEM((NZ // 2 + 1, RANK, RANK), F32),
            pltpu.VMEM((2 * GROUP + 2 * RANK, 2 * RANK), F32),
            pltpu.VMEM((ROWS, 128), F32),
            pltpu.VMEM((NY, 12, 128), F32),
            pltpu.VMEM((NY, 12, 128), F32),
            pltpu.VMEM((NY, 12, 128), F32),
            pltpu.VMEM((CHIPS, 12, 128), F32),
            pltpu.VMEM((12, 128), F32),
            pltpu.VMEM((12, 128), F32),
            dma((7,)),
            dma((2,)),
            dma((2,)),
            dma(()),
            dma(()),
            dma(()),
            dma((NZ,)),
            dma(()),
            dma((NZ // 2,)),
            dma((NY - 1,)),
            dma((NP,)),
            dma(()),
            dma((NP, SUB)),
            dma(()),
            dma((NP, SUB)),
            dma(()),
            dma(()),
            dma((CHIPS,)),
            dma((CHIPS,)),
            dma(()),
            dma(()),
        ],
        compiler_params=pltpu.CompilerParams(
            collective_id=0, has_side_effects=True, vmem_limit_bytes=66_000_000
        ),
    )(spectra, shifts, fractions, pixel_factors, spectral_factors)


def solution(mesh):
    return jax.shard_map(
        body,
        mesh=mesh,
        in_specs=(
            P("pix", "mz"),
            P("pix", "mz"),
            P("pix", "mz"),
            P("pix", None),
            P(None, ("mz", "pix")),
        ),
        out_specs=(P("pix", None), P(None, ("mz", "pix"))),
        check_vma=False,
    )
```

```python
import jax
import jax.numpy as jnp
from jax import lax
from jax.experimental import pallas as pl
from jax.experimental.pallas import tpu as pltpu
from jax.sharding import PartitionSpec as P

SEG = 2048
RANK = 32
EPSILON = 1e-06
ROWS = 16
BINS = 24576
SEGS = BINS // SEG
NZ, NY = 8, 4
OWN = 768
PW = 256
NPZ = OWN // PW
NP = NZ * NPZ
GROUP = NY * ROWS
LAGS = (5, 13, 21, 24)
LATE, LATE_FAR = 3, 7
SUB = 2
SUB_ROWS = RANK // SUB
DIRECT = 3
CHUNK = 1024
GROUP_BINS = NY * OWN
EARLY = 6
LATE_CHUNKS = (NZ - EARLY) * (GROUP_BINS // CHUNK)
CHIPS = 16
MESH = pl.DeviceIdType.MESH
F32 = jnp.float32
BF16 = jnp.bfloat16
exact_mode = lax.Precision.HIGHEST
NT = (((1,), (1,)), ((), ()))


def halves(v):
    hi = v.astype(BF16)
    return hi, (v - hi.astype(F32)).astype(BF16)


def kernel(
    x_hbm, sh_hbm, fr_hbm, f_hbm, hin_hbm, w_ref, hout_ref,
    sh_ref, fr_ref, f_ref, hin_ref,
    xp, shb, frb, ws, wg, wgb, cbuf, cout, hbuf, hc, fbuf, lhs, gsend, gbuf, acc,
    f_all, t0s, t0r, t1s, t1r, t3s, t3r,
    xsem, halo_s, halo_r, f_s, f_r, hc_s, hc_r, g_s, g_r,
    y_s, y_r, c_s, c_r, h_s, x_r, t0_s, t0_r, t1_s, t1_r, t3_s, t3_r,
):
    p, m = lax.axis_index("pix"), lax.axis_index("mz")
    z, y = lax.div(p, NY), lax.rem(p, NY)
    mh, ml = lax.div(m, 8), lax.rem(m, 8)
    low_side = z < NZ // 2
    inner = jnp.where(low_side, p + NY, p - NY)
    outer = jnp.where(low_side, p - NY, p + NY)
    depth = jnp.where(low_side, NZ // 2 - 1 - z, z - NZ // 2)
    center = depth == 0
    has_outer = depth < NZ // 2 - 1
    lag = jnp.where(
        depth == 0, LAGS[0], jnp.where(depth == 1, LAGS[1], jnp.where(depth == 2, LAGS[2], LAGS[3]))
    )

    def y_dev(r):
        return (z * NY + lax.rem(y + r, NY), m)

    def m_dev(r):
        return (p, mh * 8 + lax.rem(ml + r, 8))

    far = (p, lax.rem(m + 8, 16))

    def rcopy(src, dst, send, recv, dev):
        return pltpu.make_async_remote_copy(
            src_ref=src, dst_ref=dst, send_sem=send, recv_sem=recv, device_id=dev, device_id_type=MESH
        )

    small = [
        pltpu.make_async_copy(a, b, xsem.at[k])
        for k, (a, b) in enumerate(
            ((sh_hbm, sh_ref), (fr_hbm, fr_ref), (f_hbm, f_ref), (hin_hbm, hin_ref))
        )
    ]
    lo, hi = 3 * GROUP_BINS - 128, 4 * GROUP_BINS + 128
    parts = [
        pltpu.make_async_copy(
            x_hbm.at[:, pl.ds(a, b - a)], xp.at[:, pl.ds(128 + a, b - a)], xsem.at[4 + k]
        )
        for k, (a, b) in enumerate(((lo, hi), (hi, BINS), (0, lo)))
    ]
    for c in small[:2] + parts + small[2:]:
        c.start()

    barrier = pltpu.get_barrier_semaphore()

    def greet(dev):
        pl.semaphore_signal(barrier, inc=1, device_id=dev, device_id_type=MESH)

    core = lax.rem(ml, 2)
    partner = (p, m + 1 - 2 * core)

    def plane_dev(k):
        return (
            z * NY + lax.rem(y + lax.div(k, 4), NY),
            mh * 8 + lax.rem(ml + 2 * lax.rem(k, 4), 8),
        )

    for k in range(1, CHIPS):
        greet(plane_dev(k))
    greet(partner)
    greet(far)
    half = lax.div(z, NZ // 2) * (NZ // 2)
    for r in range(1, NZ // 2):
        greet(((half + lax.rem(z + r, NZ // 2)) * NY + y, m))

    @pl.when(center)
    def _():
        greet((inner, m))

    @pl.when((core == 0) & (m > 0))
    def _():
        greet((p, m - 1))

    @pl.when((core == 1) & (m < 15))
    def _():
        greet((p, m + 1))

    acc[...] = jnp.zeros_like(acc)

    @pl.when(m == 0)
    def _():
        xp[:, 0:128] = jnp.zeros((ROWS, 128), F32)

    @pl.when(m == 15)
    def _():
        xp[:, 128 + BINS :] = jnp.zeros((ROWS, 128), F32)

    small[0].wait()
    small[1].wait()
    for s in range(SEGS):
        shb[s] = jnp.broadcast_to(sh_ref[:, s : s + 1], (ROWS, 128))
        frb[s] = jnp.broadcast_to(fr_ref[:, s : s + 1], (ROWS, 128))

    def group_z(g):
        step = lax.div(g, 2)
        return jnp.where(lax.rem(g, 2) == 0, NZ // 2 - 1 - step, NZ // 2 + step)

    def piece(i):
        return group_z(lax.div(i, NPZ)) * NPZ + lax.rem(i, NPZ)

    def own_bins(t):
        return first_bin(0, t)

    def first_bin(r, t):
        zq, j = lax.div(t, NPZ), lax.rem(t, NPZ)
        return pl.multiple_of(zq * GROUP_BINS + lax.rem(y + r, NY) * OWN + j * PW, 128)

    def warp(c):
        width = CHUNK + 256
        b = pl.multiple_of(c * CHUNK, 128)
        seg = lax.div(b, SEG)
        d, f = shb[seg], frb[seg]

        def wide(v, lanes):
            return jnp.concatenate([v] * (lanes // 128), axis=1)

        v = xp[:, pl.ds(b, width)]
        v = jnp.where(wide(d, width) < 0, pltpu.roll(v, 4, 1), v)
        shifted = [v] + [pltpu.roll(v, width - k, 1) for k in range(1, 5)]
        shifted = [u[:, 128 : 128 + CHUNK] for u in shifted]
        rest = wide(d & 3, CHUNK)
        high, odd = rest >= 2, (rest & 1) != 0

        def pick(k):
            return jnp.where(
                high,
                jnp.where(odd, shifted[k + 3], shifted[k + 2]),
                jnp.where(odd, shifted[k + 1], shifted[k]),
            )

        f = wide(f, CHUNK)
        ws[:, pl.ds(b, CHUNK)] = (1.0 - f) * pick(0) + f * pick(1)

    def warp_group(g):
        zq = group_z(g)

        for k in range(GROUP_BINS // CHUNK):
            warp(zq * (GROUP_BINS // CHUNK) + k)

    def y_copy(r, t):
        src = ws.at[:, pl.ds(first_bin(r, t), PW)]
        return rcopy(src, wg.at[t, NY - r - 1], y_s.at[r - 1], y_r.at[t], y_dev(r))

    def send_group(g):
        zq = group_z(g)
        for j in range(NPZ):
            for r in range(1, NY):
                y_copy(r, zq * NPZ + j).start()

    parts[0].wait()
    with jax.named_scope("warps"):
        warp_group(0)
    small[2].wait()
    f_all[...] = jnp.concatenate([f_ref[...], jnp.zeros((ROWS, 128 - RANK), F32)], axis=1)
    with jax.named_scope("barrier"):
        pl.semaphore_wait(
            barrier,
            CHIPS + 1 + NZ // 2 - 1 + jnp.where(center, 1, 0) + jnp.where((m == 0) | (m == 15), 0, 1),
        )

    f_copies = [
        rcopy(f_all, fbuf.at[NY - r - 1], f_s, f_r, y_dev(r)) for r in range(1, NY)
    ]
    for c in f_copies:
        c.start()
    send_group(0)
    parts[1].wait()
    parts[2].wait()
    small[3].wait()

    to_right = rcopy(
        xp.at[:, pl.ds(BINS, 128)], xp.at[:, pl.ds(0, 128)], halo_s.at[0], halo_r.at[0], (p, m + 1)
    )
    to_left = rcopy(
        xp.at[:, pl.ds(128, 128)], xp.at[:, pl.ds(128 + BINS, 128)], halo_s.at[1], halo_r.at[1], (p, m - 1)
    )

    @pl.when(m < 15)
    def _():
        to_right.start()

    @pl.when(m > 0)
    def _():
        to_left.start()

    near = jnp.where(low_side, NZ // 2 - 1, NZ // 2)

    h_part = rcopy(hin_ref, hc.at[z], hc_s, hc_r.at[z], (jnp.where(center, inner, near * NY + y), m))

    def h_relay(zk):
        return rcopy(hc.at[zk], hc.at[zk], hc_s, hc_r.at[zk], (inner, m))

    h_part.start()

    @pl.when(center)
    def _():
        hc[z] = hin_ref[...]

    def early(g, carry):
        warp_group(g)
        send_group(g)
        return carry

    with jax.named_scope("warps"):
        lax.fori_loop(1, EARLY, early, 0)

    with jax.named_scope("fwait"):
        rcopy(fbuf, fbuf, f_s, f_r, y_dev(1)).wait_recv()
    fg = jnp.concatenate([f_all[...], fbuf[...].reshape(GROUP - ROWS, 128)], axis=0)[:, 0:RANK]
    gy = lax.dot_general(fg, fg, (((0,), (0,)), ((), ())), precision=exact_mode, preferred_element_type=F32)
    f_hi, f_lo = halves(fg.T)
    lhs[...] = jnp.concatenate([f_hi, f_hi, f_lo], axis=1)

    g_half = rcopy(gsend, gbuf.at[depth], g_s, g_r.at[depth], (near * NY + y, m))
    g_other = rcopy(gsend, gbuf.at[0], g_s, g_r.at[0], (inner, m))

    def outward(k):
        return jnp.where(low_side, NZ // 2 - 1 - k, NZ // 2 + k)

    def warp_late(e):
        chunks = GROUP_BINS // CHUNK
        g = EARLY + lax.div(e, chunks)

        @pl.when((e == 0) & (m > 0))
        def _():
            to_right.wait_recv()

        @pl.when((e == 2 * chunks - 1) & (m < 15))
        def _():
            to_left.wait_recv()

        warp(group_z(g) * chunks + lax.rem(e, chunks))

        @pl.when(lax.rem(e, chunks) == chunks - 1)
        def _():
            send_group(g)

    @pl.when(jnp.logical_not(center))
    def _():
        gsend[...] = gy
        g_half.start()

    @pl.when(center)
    def _():
        total = gy
        for k in range(1, NZ // 2):
            rcopy(gsend, gbuf.at[k], g_s, g_r.at[k], (inner, m)).wait_recv()
            total = total + gbuf[k]
        gsend[...] = total
        g_other.start()
        def late(e, carry):
            warp_late(e)
            return carry

        lax.fori_loop(0, LATE_CHUNKS, late, 0)
        with jax.named_scope("relay"):
            for k in range(1, NZ // 2):
                h_relay(outward(k)).wait_recv()
                h_relay(outward(k)).start()
        g_other.wait_recv()
        gbuf[NZ // 2] = total + gbuf[0]

    across = (m == 7) | (m == 8)
    late_from = jnp.where(center, -LATE_CHUNKS, jnp.where(across, LATE_FAR, LATE))

    def rows_of(q):
        return pl.ds(q * SUB_ROWS, SUB_ROWS)

    def c_copy(t, q):
        dst = cbuf.at[0, t, rows_of(q)]
        return rcopy(cout.at[t, rows_of(q)], dst, c_s, c_r.at[t, q], (inner, m))

    def cx_copy(t, q):
        dst = cbuf.at[1, t, rows_of(q)]
        return rcopy(cout.at[t, rows_of(q)], dst, c_s, x_r.at[t, q], (inner, m))

    def c_send(t, q):
        @pl.when(center)
        def _():
            cx_copy(t, q).start()

        @pl.when(jnp.logical_not(center))
        def _():
            c_copy(t, q).start()

    def h_copy(t, q, dev):
        part = hbuf.at[t, rows_of(q)]
        return rcopy(part, part, h_s, x_r.at[t, q], dev)

    def step(i, carry):
        @pl.when(i < NP)
        def _():
            t = piece(i)
            with jax.named_scope("ywait"):
                rcopy(wg.at[t], wg.at[t], y_s.at[0], y_r.at[t], y_dev(1)).wait_recv()
            mine = ws[:, pl.ds(own_bins(t), PW)]
            w_hi, w_lo = halves(jnp.concatenate([mine, wg[t].reshape(GROUP - ROWS, PW)], axis=0))
            both = jnp.concatenate([w_hi, w_lo], axis=0)
            wgb[t] = both
            n = jnp.dot(lhs[...], jnp.concatenate([both, w_hi], axis=0), preferred_element_type=F32)

            @pl.when(has_outer)
            def _():
                for q in range(SUB):
                    with jax.named_scope("cwait"):
                        c_copy(t, q).wait_recv()
                    part = n[q * SUB_ROWS : (q + 1) * SUB_ROWS]
                    cout[t, rows_of(q)] = part + cbuf[0, t, rows_of(q)]
                    c_send(t, q)

            @pl.when(jnp.logical_not(has_outer))
            def _():
                cout[t] = n
                for q in range(SUB):
                    c_send(t, q)

            late = i - late_from

            @pl.when((late >= 0) & (late < LATE_CHUNKS))
            def _():
                warp_late(late)

        k = i - lag

        @pl.when((k >= 0) & (k < NP))
        def _():
            t = piece(k)

            @pl.when(center)
            def _():
                zq, j = lax.div(t, NPZ), lax.rem(t, NPZ)

                @pl.when((j == 0) & (lax.div(zq, NZ // 2) != lax.div(z, NZ // 2)))
                def _():
                    with jax.named_scope("hcwait"):
                        h_relay(zq).wait_recv()

                own = hc[zq, :, pl.ds(pl.multiple_of(j * PW, 128), PW)]
                bottom = jnp.dot(gbuf[NZ // 2], own, precision=exact_mode, preferred_element_type=F32) + EPSILON
                ratio = own / bottom
                for q in range(SUB):
                    with jax.named_scope("xcwait"):
                        cx_copy(t, q).wait_recv()
                    r = rows_of(q)
                    hbuf[t, r] = ratio[q * SUB_ROWS : (q + 1) * SUB_ROWS] * (cout[t, r] + cbuf[1, t, r])

                    @pl.when(k >= NP - DIRECT)
                    def _():
                        for far_out in (3, 2):
                            h_copy(t, q, (outward(far_out) * NY + y, m)).start()

                    h_copy(t, q, (outer, m)).start()

            @pl.when(jnp.logical_not(center))
            def _():
                for q in range(SUB):
                    with jax.named_scope("hwait"):
                        h_copy(t, q, (outer, m)).wait_recv()

                    @pl.when(has_outer & (k < NP - DIRECT))
                    def _():
                        h_copy(t, q, (outer, m)).start()

            h = hbuf[t]
            h_hi, h_lo = halves(h)
            right = jnp.concatenate([h_hi, h_lo], axis=0)
            left = jnp.concatenate([wgb[t], right], axis=0)
            acc[...] += lax.dot_general(left, right, NT, preferred_element_type=F32)

            @pl.when(lax.div(t, NPZ) == z)
            def _():
                hout_ref[:, pl.ds(pl.multiple_of(lax.rem(t, NPZ) * PW, 128), PW)] = h

        return carry

    lax.fori_loop(0, NP + LAGS[-1], step, 0)

    both = acc[:, 0:RANK] + acc[:, RANK : 2 * RANK]
    proj = both[0:GROUP] + both[GROUP : 2 * GROUP]
    base = 2 * GROUP
    gram = both[base : base + RANK] + both[base + RANK : base + 2 * RANK]
    gram8 = jnp.concatenate([gram[8 * q : 8 * q + 8] for q in range(4)], axis=1)
    for k in range(NY):
        rows = proj[k * ROWS : (k + 1) * ROWS]
        t0s[k, 0:8] = gram8
        t0s[k, 8:12] = jnp.concatenate([rows[4 * q : 4 * q + 4] for q in range(4)], axis=1)
    t0_copy = rcopy(t0s, t0r, t0_s, t0_r, partner)
    t0_copy.start()
    with jax.named_scope("t0wait"):
        t0_copy.wait_recv()
    t1s[...] = t0s[...] + t0r[...]

    me = y * 4 + lax.div(ml, 2)

    def t_copy(k):
        return rcopy(t1s.at[lax.div(k, 4)], t1r.at[me], t1_s.at[k], t1_r.at[k], plane_dev(k))

    t1_copies = [t_copy(k) for k in range(1, CHIPS)]
    for c in t1_copies:
        c.start()
    t1r[me] = t1s[0]
    with jax.named_scope("t1wait"):
        for c in t1_copies:
            c.wait_recv()
    sums = [t1r[k] for k in range(CHIPS)]
    while len(sums) > 1:
        sums = [a + b for a, b in zip(sums[::2], sums[1::2])]
    t3s[...] = sums[0]
    t3_copy = rcopy(t3s, t3r, t3_s, t3_r, far)
    t3_copy.start()
    with jax.named_scope("t3wait"):
        t3_copy.wait_recv()
    total = sums[0] + t3r[...]
    gram_sum = jnp.concatenate([total[0:8, 32 * q : 32 * q + 32] for q in range(4)], axis=0)
    proj_sum = jnp.concatenate([total[8:12, 32 * q : 32 * q + 32] for q in range(4)], axis=0)
    f = f_ref[...]
    g_hi, g_lo = halves(gram_sum)
    own_hi, own_lo = halves(f)
    bottom = EPSILON + jnp.dot(
        jnp.concatenate([own_hi, own_hi, own_lo], axis=1),
        jnp.concatenate([g_hi, g_lo, g_hi], axis=0),
        preferred_element_type=F32,
    )
    w_ref[...] = f * proj_sum / bottom

    rcopy(fbuf, fbuf, f_s, f_r, y_dev(1)).wait_send()
    for c in t1_copies + [t0_copy, t3_copy]:
        c.wait_send()

    @pl.when(m < 15)
    def _():
        to_right.wait_send()

    @pl.when(m > 0)
    def _():
        to_left.wait_send()

    g_half.wait_send()
    h_part.wait_send()

    @pl.when(center)
    def _():
        part = hc.at[pl.ds(0, NZ // 2 - 1)]
        rcopy(part, part, hc_s, hc_s, (inner, m)).wait_send()

    for r in range(1, NY):
        rcopy(wg.at[:, r - 1], wg.at[:, r - 1], y_s.at[r - 1], y_s.at[r - 1], y_dev(r)).wait_send()
    rcopy(cout, cout, c_s, c_s, (inner, m)).wait_send()

    def h_sent(pieces):
        part = hbuf.at[pl.ds(0, pieces)]
        rcopy(part, part, h_s, h_s, (outer, m)).wait_send()

    @pl.when(center)
    def _():
        h_sent(NP)
        h_sent(2 * DIRECT)

    @pl.when(has_outer & jnp.logical_not(center))
    def _():
        h_sent(NP - DIRECT)


def body(spectra, shifts, fractions, pixel_factors, spectral_factors):
    vmem = pl.BlockSpec(memory_space=pltpu.VMEM)
    dma = pltpu.SemaphoreType.DMA
    return pl.pallas_call(
        kernel,
        out_shape=(
            pltpu.VMEM((ROWS, RANK), F32),
            pltpu.VMEM((RANK, OWN), F32),
        ),
        in_specs=[pl.BlockSpec(memory_space=pltpu.HBM)] * 5,
        out_specs=(vmem, vmem),
        scratch_shapes=[
            pltpu.VMEM((ROWS, SEGS), jnp.int32),
            pltpu.VMEM((ROWS, SEGS), F32),
            pltpu.VMEM((ROWS, RANK), F32),
            pltpu.VMEM((RANK, OWN), F32),
            pltpu.VMEM((ROWS, BINS + 256), F32),
            pltpu.VMEM((SEGS, ROWS, 128), jnp.int32),
            pltpu.VMEM((SEGS, ROWS, 128), F32),
            pltpu.VMEM((ROWS, BINS), F32),
            pltpu.VMEM((NP, NY - 1, ROWS, PW), F32),
            pltpu.VMEM((NP, 2 * GROUP, PW), BF16),
            pltpu.VMEM((2, NP, RANK, PW), F32),
            pltpu.VMEM((NP, RANK, PW), F32),
            pltpu.VMEM((NP, RANK, PW), F32),
            pltpu.VMEM((NZ, RANK, OWN), F32),
            pltpu.VMEM((NY - 1, ROWS, 128), F32),
            pltpu.VMEM((RANK, 3 * GROUP), BF16),
            pltpu.VMEM((RANK, RANK), F32),
            pltpu.VMEM((NZ // 2 + 1, RANK, RANK), F32),
            pltpu.VMEM((2 * GROUP + 2 * RANK, 2 * RANK), F32),
            pltpu.VMEM((ROWS, 128), F32),
            pltpu.VMEM((NY, 12, 128), F32),
            pltpu.VMEM((NY, 12, 128), F32),
            pltpu.VMEM((NY, 12, 128), F32),
            pltpu.VMEM((CHIPS, 12, 128), F32),
            pltpu.VMEM((12, 128), F32),
            pltpu.VMEM((12, 128), F32),
            dma((7,)),
            dma((2,)),
            dma((2,)),
            dma(()),
            dma(()),
            dma(()),
            dma((NZ,)),
            dma(()),
            dma((NZ // 2,)),
            dma((NY - 1,)),
            dma((NP,)),
            dma(()),
            dma((NP, SUB)),
            dma(()),
            dma((NP, SUB)),
            dma(()),
            dma(()),
            dma((CHIPS,)),
            dma((CHIPS,)),
            dma(()),
            dma(()),
        ],
        compiler_params=pltpu.CompilerParams(
            collective_id=0, has_side_effects=True, vmem_limit_bytes=66_000_000
        ),
    )(spectra, shifts, fractions, pixel_factors, spectral_factors)


def solution(mesh):
    return jax.shard_map(
        body,
        mesh=mesh,
        in_specs=(
            P("pix", "mz"),
            P("pix", "mz"),
            P("pix", "mz"),
            P("pix", None),
            P(None, ("mz", "pix")),
        ),
        out_specs=(P("pix", None), P(None, ("mz", "pix"))),
        check_vma=False,
    )
```

```python
import jax
import jax.numpy as jnp
from jax import lax
from jax.experimental import pallas as pl
from jax.experimental.pallas import tpu as pltpu
from jax.sharding import PartitionSpec as P

SEG = 2048
RANK = 32
EPSILON = 1e-06
ROWS = 16
BINS = 24576
SEGS = BINS // SEG
NZ, NY = 8, 4
OWN = 768
PW = 256
NPZ = OWN // PW
NP = NZ * NPZ
GROUP = NY * ROWS
LAGS = (5, 13, 21, 24)
LATE, LATE_FAR = 3, 7
SUB = 2
SUB_ROWS = RANK // SUB
DIRECT = 2
CHUNK = 1024
GROUP_BINS = NY * OWN
EARLY = 6
LATE_CHUNKS = (NZ - EARLY) * (GROUP_BINS // CHUNK)
CHIPS = 16
MESH = pl.DeviceIdType.MESH
F32 = jnp.float32
BF16 = jnp.bfloat16
exact_mode = lax.Precision.HIGHEST
NT = (((1,), (1,)), ((), ()))


def halves(v):
    hi = v.astype(BF16)
    return hi, (v - hi.astype(F32)).astype(BF16)


def kernel(
    x_hbm, sh_hbm, fr_hbm, f_hbm, hin_hbm, w_ref, hout_ref,
    sh_ref, fr_ref, f_ref, hin_ref,
    xp, shb, frb, ws, wg, wgb, cbuf, cout, hbuf, hc, fbuf, lhs, gsend, gbuf, acc,
    f_all, t0s, t0r, t1s, t1r, t3s, t3r,
    xsem, halo_s, halo_r, f_s, f_r, hc_s, hc_r, g_s, g_r,
    y_s, y_r, c_s, c_r, h_s, x_r, t0_s, t0_r, t1_s, t1_r, t3_s, t3_r,
):
    p, m = lax.axis_index("pix"), lax.axis_index("mz")
    z, y = lax.div(p, NY), lax.rem(p, NY)
    mh, ml = lax.div(m, 8), lax.rem(m, 8)
    low_side = z < NZ // 2
    inner = jnp.where(low_side, p + NY, p - NY)
    outer = jnp.where(low_side, p - NY, p + NY)
    depth = jnp.where(low_side, NZ // 2 - 1 - z, z - NZ // 2)
    center = depth == 0
    has_outer = depth < NZ // 2 - 1
    lag = jnp.where(
        depth == 0, LAGS[0], jnp.where(depth == 1, LAGS[1], jnp.where(depth == 2, LAGS[2], LAGS[3]))
    )

    def y_dev(r):
        return (z * NY + lax.rem(y + r, NY), m)

    def m_dev(r):
        return (p, mh * 8 + lax.rem(ml + r, 8))

    far = (p, lax.rem(m + 8, 16))

    def rcopy(src, dst, send, recv, dev):
        return pltpu.make_async_remote_copy(
            src_ref=src, dst_ref=dst, send_sem=send, recv_sem=recv, device_id=dev, device_id_type=MESH
        )

    small = [
        pltpu.make_async_copy(a, b, xsem.at[k])
        for k, (a, b) in enumerate(
            ((sh_hbm, sh_ref), (fr_hbm, fr_ref), (f_hbm, f_ref), (hin_hbm, hin_ref))
        )
    ]
    lo, hi = 3 * GROUP_BINS - 128, 4 * GROUP_BINS + 128
    parts = [
        pltpu.make_async_copy(
            x_hbm.at[:, pl.ds(a, b - a)], xp.at[:, pl.ds(128 + a, b - a)], xsem.at[4 + k]
        )
        for k, (a, b) in enumerate(((lo, hi), (hi, BINS), (0, lo)))
    ]
    for c in small[:2] + parts + small[2:]:
        c.start()

    barrier = pltpu.get_barrier_semaphore()

    def greet(dev):
        pl.semaphore_signal(barrier, inc=1, device_id=dev, device_id_type=MESH)

    core = lax.rem(ml, 2)
    partner = (p, m + 1 - 2 * core)

    def plane_dev(k):
        return (
            z * NY + lax.rem(y + lax.div(k, 4), NY),
            mh * 8 + lax.rem(ml + 2 * lax.rem(k, 4), 8),
        )

    for k in range(1, CHIPS):
        greet(plane_dev(k))
    greet(partner)
    greet(far)
    half = lax.div(z, NZ // 2) * (NZ // 2)
    for r in range(1, NZ // 2):
        greet(((half + lax.rem(z + r, NZ // 2)) * NY + y, m))

    @pl.when(center)
    def _():
        greet((inner, m))

    @pl.when((core == 0) & (m > 0))
    def _():
        greet((p, m - 1))

    @pl.when((core == 1) & (m < 15))
    def _():
        greet((p, m + 1))

    acc[...] = jnp.zeros_like(acc)

    @pl.when(m == 0)
    def _():
        xp[:, 0:128] = jnp.zeros((ROWS, 128), F32)

    @pl.when(m == 15)
    def _():
        xp[:, 128 + BINS :] = jnp.zeros((ROWS, 128), F32)

    small[0].wait()
    small[1].wait()
    for s in range(SEGS):
        shb[s] = jnp.broadcast_to(sh_ref[:, s : s + 1], (ROWS, 128))
        frb[s] = jnp.broadcast_to(fr_ref[:, s : s + 1], (ROWS, 128))

    def group_z(g):
        step = lax.div(g, 2)
        return jnp.where(lax.rem(g, 2) == 0, NZ // 2 - 1 - step, NZ // 2 + step)

    def piece(i):
        return group_z(lax.div(i, NPZ)) * NPZ + lax.rem(i, NPZ)

    def own_bins(t):
        return first_bin(0, t)

    def first_bin(r, t):
        zq, j = lax.div(t, NPZ), lax.rem(t, NPZ)
        return pl.multiple_of(zq * GROUP_BINS + lax.rem(y + r, NY) * OWN + j * PW, 128)

    def warp(c):
        width = CHUNK + 256
        b = pl.multiple_of(c * CHUNK, 128)
        seg = lax.div(b, SEG)
        d, f = shb[seg], frb[seg]

        def wide(v, lanes):
            return jnp.concatenate([v] * (lanes // 128), axis=1)

        v = xp[:, pl.ds(b, width)]
        v = jnp.where(wide(d, width) < 0, pltpu.roll(v, 4, 1), v)
        shifted = [v] + [pltpu.roll(v, width - k, 1) for k in range(1, 5)]
        shifted = [u[:, 128 : 128 + CHUNK] for u in shifted]
        rest = wide(d & 3, CHUNK)
        high, odd = rest >= 2, (rest & 1) != 0

        def pick(k):
            return jnp.where(
                high,
                jnp.where(odd, shifted[k + 3], shifted[k + 2]),
                jnp.where(odd, shifted[k + 1], shifted[k]),
            )

        f = wide(f, CHUNK)
        ws[:, pl.ds(b, CHUNK)] = (1.0 - f) * pick(0) + f * pick(1)

    def warp_group(g):
        zq = group_z(g)

        for k in range(GROUP_BINS // CHUNK):
            warp(zq * (GROUP_BINS // CHUNK) + k)

    def y_copy(r, t):
        src = ws.at[:, pl.ds(first_bin(r, t), PW)]
        return rcopy(src, wg.at[t, NY - r - 1], y_s.at[r - 1], y_r.at[t], y_dev(r))

    def send_group(g):
        zq = group_z(g)
        for j in range(NPZ):
            for r in range(1, NY):
                y_copy(r, zq * NPZ + j).start()

    parts[0].wait()
    with jax.named_scope("warps"):
        warp_group(0)
    small[2].wait()
    f_all[...] = jnp.concatenate([f_ref[...], jnp.zeros((ROWS, 128 - RANK), F32)], axis=1)
    with jax.named_scope("barrier"):
        pl.semaphore_wait(
            barrier,
            CHIPS + 1 + NZ // 2 - 1 + jnp.where(center, 1, 0) + jnp.where((m == 0) | (m == 15), 0, 1),
        )

    f_copies = [
        rcopy(f_all, fbuf.at[NY - r - 1], f_s, f_r, y_dev(r)) for r in range(1, NY)
    ]
    for c in f_copies:
        c.start()
    send_group(0)
    parts[1].wait()
    parts[2].wait()
    small[3].wait()

    to_right = rcopy(
        xp.at[:, pl.ds(BINS, 128)], xp.at[:, pl.ds(0, 128)], halo_s.at[0], halo_r.at[0], (p, m + 1)
    )
    to_left = rcopy(
        xp.at[:, pl.ds(128, 128)], xp.at[:, pl.ds(128 + BINS, 128)], halo_s.at[1], halo_r.at[1], (p, m - 1)
    )

    @pl.when(m < 15)
    def _():
        to_right.start()

    @pl.when(m > 0)
    def _():
        to_left.start()

    near = jnp.where(low_side, NZ // 2 - 1, NZ // 2)

    h_part = rcopy(hin_ref, hc.at[z], hc_s, hc_r.at[z], (jnp.where(center, inner, near * NY + y), m))

    def h_relay(zk):
        return rcopy(hc.at[zk], hc.at[zk], hc_s, hc_r.at[zk], (inner, m))

    @pl.when(depth <= 1)
    def _():
        h_part.start()

    @pl.when(center)
    def _():
        hc[z] = hin_ref[...]

    def early(g, carry):
        warp_group(g)
        send_group(g)
        return carry

    with jax.named_scope("warps"):
        lax.fori_loop(1, EARLY // 2, early, 0)

        @pl.when(depth == 2)
        def _():
            h_part.start()

        lax.fori_loop(EARLY // 2, EARLY, early, 0)

        @pl.when(depth == 3)
        def _():
            h_part.start()

    with jax.named_scope("fwait"):
        rcopy(fbuf, fbuf, f_s, f_r, y_dev(1)).wait_recv()
    fg = jnp.concatenate([f_all[...], fbuf[...].reshape(GROUP - ROWS, 128)], axis=0)[:, 0:RANK]
    gy = lax.dot_general(fg, fg, (((0,), (0,)), ((), ())), precision=exact_mode, preferred_element_type=F32)
    f_hi, f_lo = halves(fg.T)
    lhs[...] = jnp.concatenate([f_hi, f_hi, f_lo], axis=1)

    g_half = rcopy(gsend, gbuf.at[depth], g_s, g_r.at[depth], (near * NY + y, m))
    g_other = rcopy(gsend, gbuf.at[0], g_s, g_r.at[0], (inner, m))

    def outward(k):
        return jnp.where(low_side, NZ // 2 - 1 - k, NZ // 2 + k)

    def warp_late(e):
        chunks = GROUP_BINS // CHUNK
        g = EARLY + lax.div(e, chunks)

        @pl.when((e == 0) & (m > 0))
        def _():
            to_right.wait_recv()

        @pl.when((e == 2 * chunks - 1) & (m < 15))
        def _():
            to_left.wait_recv()

        warp(group_z(g) * chunks + lax.rem(e, chunks))

        @pl.when(lax.rem(e, chunks) == chunks - 1)
        def _():
            send_group(g)

    @pl.when(jnp.logical_not(center))
    def _():
        gsend[...] = gy
        g_half.start()

    def relay(k):
        h_relay(outward(k)).wait_recv()
        h_relay(outward(k)).start()

    @pl.when(center)
    def _():
        with jax.named_scope("relay"):
            relay(1)
            relay(2)
            total = gy
            for k in range(1, NZ // 2):
                rcopy(gsend, gbuf.at[k], g_s, g_r.at[k], (inner, m)).wait_recv()
                total = total + gbuf[k]
            gsend[...] = total
            gbuf[NZ // 2] = total
            g_other.start()
            relay(3)

        def late(e, carry):
            warp_late(e)
            return carry

        lax.fori_loop(0, LATE_CHUNKS, late, 0)

    across = (m == 7) | (m == 8)
    late_from = jnp.where(center, -LATE_CHUNKS, jnp.where(across, LATE_FAR, LATE))

    def rows_of(q):
        return pl.ds(q * SUB_ROWS, SUB_ROWS)

    def c_copy(t, q):
        dst = cbuf.at[0, t, rows_of(q)]
        return rcopy(cout.at[t, rows_of(q)], dst, c_s, c_r.at[t, q], (inner, m))

    def cx_copy(t, q):
        dst = cbuf.at[1, t, rows_of(q)]
        return rcopy(cout.at[t, rows_of(q)], dst, c_s, x_r.at[t, q], (inner, m))

    def c_send(t, q):
        @pl.when(center)
        def _():
            cx_copy(t, q).start()

        @pl.when(jnp.logical_not(center))
        def _():
            c_copy(t, q).start()

    def h_copy(t, q, dev):
        part = hbuf.at[t, rows_of(q)]
        return rcopy(part, part, h_s, x_r.at[t, q], dev)

    def step(i, carry):
        @pl.when(i < NP)
        def _():
            t = piece(i)
            with jax.named_scope("ywait"):
                rcopy(wg.at[t], wg.at[t], y_s.at[0], y_r.at[t], y_dev(1)).wait_recv()
            mine = ws[:, pl.ds(own_bins(t), PW)]
            w_hi, w_lo = halves(jnp.concatenate([mine, wg[t].reshape(GROUP - ROWS, PW)], axis=0))
            both = jnp.concatenate([w_hi, w_lo], axis=0)
            wgb[t] = both
            n = jnp.dot(lhs[...], jnp.concatenate([both, w_hi], axis=0), preferred_element_type=F32)

            @pl.when(has_outer)
            def _():
                for q in range(SUB):
                    with jax.named_scope("cwait"):
                        c_copy(t, q).wait_recv()
                    part = n[q * SUB_ROWS : (q + 1) * SUB_ROWS]
                    cout[t, rows_of(q)] = part + cbuf[0, t, rows_of(q)]
                    c_send(t, q)

            @pl.when(jnp.logical_not(has_outer))
            def _():
                cout[t] = n
                for q in range(SUB):
                    c_send(t, q)

            late = i - late_from

            @pl.when((late >= 0) & (late < LATE_CHUNKS))
            def _():
                warp_late(late)

        k = i - lag

        @pl.when((k >= 0) & (k < NP))
        def _():
            t = piece(k)

            @pl.when(center)
            def _():
                zq, j = lax.div(t, NPZ), lax.rem(t, NPZ)

                @pl.when(k == 0)
                def _():
                    g_other.wait_recv()
                    gbuf[NZ // 2] = gbuf[NZ // 2] + gbuf[0]

                @pl.when((j == 0) & (lax.div(zq, NZ // 2) != lax.div(z, NZ // 2)))
                def _():
                    with jax.named_scope("hcwait"):
                        h_relay(zq).wait_recv()

                own = hc[zq, :, pl.ds(pl.multiple_of(j * PW, 128), PW)]
                bottom = jnp.dot(gbuf[NZ // 2], own, precision=exact_mode, preferred_element_type=F32) + EPSILON
                ratio = own / bottom
                for q in range(SUB):
                    with jax.named_scope("xcwait"):
                        cx_copy(t, q).wait_recv()
                    r = rows_of(q)
                    hbuf[t, r] = ratio[q * SUB_ROWS : (q + 1) * SUB_ROWS] * (cout[t, r] + cbuf[1, t, r])

                    @pl.when(k >= NP - DIRECT)
                    def _():
                        for far_out in (3, 2):
                            h_copy(t, q, (outward(far_out) * NY + y, m)).start()

                    h_copy(t, q, (outer, m)).start()

            @pl.when(jnp.logical_not(center))
            def _():
                for q in range(SUB):
                    with jax.named_scope("hwait"):
                        h_copy(t, q, (outer, m)).wait_recv()

                    @pl.when(has_outer & (k < NP - DIRECT))
                    def _():
                        h_copy(t, q, (outer, m)).start()

            h = hbuf[t]
            h_hi, h_lo = halves(h)
            right = jnp.concatenate([h_hi, h_lo], axis=0)
            left = jnp.concatenate([wgb[t], right], axis=0)
            acc[...] += lax.dot_general(left, right, NT, preferred_element_type=F32)

            @pl.when(lax.div(t, NPZ) == z)
            def _():
                hout_ref[:, pl.ds(pl.multiple_of(lax.rem(t, NPZ) * PW, 128), PW)] = h

        return carry

    lax.fori_loop(0, NP + LAGS[-1], step, 0)

    both = acc[:, 0:RANK] + acc[:, RANK : 2 * RANK]
    proj = both[0:GROUP] + both[GROUP : 2 * GROUP]
    base = 2 * GROUP
    gram = both[base : base + RANK] + both[base + RANK : base + 2 * RANK]
    gram8 = jnp.concatenate([gram[8 * q : 8 * q + 8] for q in range(4)], axis=1)
    for k in range(NY):
        rows = proj[k * ROWS : (k + 1) * ROWS]
        t0s[k, 0:8] = gram8
        t0s[k, 8:12] = jnp.concatenate([rows[4 * q : 4 * q + 4] for q in range(4)], axis=1)
    t0_copy = rcopy(t0s, t0r, t0_s, t0_r, partner)
    t0_copy.start()
    with jax.named_scope("t0wait"):
        t0_copy.wait_recv()
    t1s[...] = t0s[...] + t0r[...]

    me = y * 4 + lax.div(ml, 2)

    def t_copy(k):
        return rcopy(t1s.at[lax.div(k, 4)], t1r.at[me], t1_s.at[k], t1_r.at[k], plane_dev(k))

    t1_copies = [t_copy(k) for k in range(1, CHIPS)]
    for c in t1_copies:
        c.start()
    t1r[me] = t1s[0]
    with jax.named_scope("t1wait"):
        for c in t1_copies:
            c.wait_recv()
    sums = [t1r[k] for k in range(CHIPS)]
    while len(sums) > 1:
        sums = [a + b for a, b in zip(sums[::2], sums[1::2])]
    t3s[...] = sums[0]
    t3_copy = rcopy(t3s, t3r, t3_s, t3_r, far)
    t3_copy.start()
    with jax.named_scope("t3wait"):
        t3_copy.wait_recv()
    total = sums[0] + t3r[...]
    gram_sum = jnp.concatenate([total[0:8, 32 * q : 32 * q + 32] for q in range(4)], axis=0)
    proj_sum = jnp.concatenate([total[8:12, 32 * q : 32 * q + 32] for q in range(4)], axis=0)
    f = f_ref[...]
    g_hi, g_lo = halves(gram_sum)
    own_hi, own_lo = halves(f)
    bottom = EPSILON + jnp.dot(
        jnp.concatenate([own_hi, own_hi, own_lo], axis=1),
        jnp.concatenate([g_hi, g_lo, g_hi], axis=0),
        preferred_element_type=F32,
    )
    w_ref[...] = f * proj_sum / bottom

    rcopy(fbuf, fbuf, f_s, f_r, y_dev(1)).wait_send()
    for c in t1_copies + [t0_copy, t3_copy]:
        c.wait_send()

    @pl.when(m < 15)
    def _():
        to_right.wait_send()

    @pl.when(m > 0)
    def _():
        to_left.wait_send()

    g_half.wait_send()
    h_part.wait_send()

    @pl.when(center)
    def _():
        part = hc.at[pl.ds(0, NZ // 2 - 1)]
        rcopy(part, part, hc_s, hc_s, (inner, m)).wait_send()

    for r in range(1, NY):
        rcopy(wg.at[:, r - 1], wg.at[:, r - 1], y_s.at[r - 1], y_s.at[r - 1], y_dev(r)).wait_send()
    rcopy(cout, cout, c_s, c_s, (inner, m)).wait_send()

    def h_sent(pieces):
        part = hbuf.at[pl.ds(0, pieces)]
        rcopy(part, part, h_s, h_s, (outer, m)).wait_send()

    @pl.when(center)
    def _():
        h_sent(NP)
        h_sent(2 * DIRECT)

    @pl.when(has_outer & jnp.logical_not(center))
    def _():
        h_sent(NP - DIRECT)


def body(spectra, shifts, fractions, pixel_factors, spectral_factors):
    vmem = pl.BlockSpec(memory_space=pltpu.VMEM)
    dma = pltpu.SemaphoreType.DMA
    return pl.pallas_call(
        kernel,
        out_shape=(
            pltpu.VMEM((ROWS, RANK), F32),
            pltpu.VMEM((RANK, OWN), F32),
        ),
        in_specs=[pl.BlockSpec(memory_space=pltpu.HBM)] * 5,
        out_specs=(vmem, vmem),
        scratch_shapes=[
            pltpu.VMEM((ROWS, SEGS), jnp.int32),
            pltpu.VMEM((ROWS, SEGS), F32),
            pltpu.VMEM((ROWS, RANK), F32),
            pltpu.VMEM((RANK, OWN), F32),
            pltpu.VMEM((ROWS, BINS + 256), F32),
            pltpu.VMEM((SEGS, ROWS, 128), jnp.int32),
            pltpu.VMEM((SEGS, ROWS, 128), F32),
            pltpu.VMEM((ROWS, BINS), F32),
            pltpu.VMEM((NP, NY - 1, ROWS, PW), F32),
            pltpu.VMEM((NP, 2 * GROUP, PW), BF16),
            pltpu.VMEM((2, NP, RANK, PW), F32),
            pltpu.VMEM((NP, RANK, PW), F32),
            pltpu.VMEM((NP, RANK, PW), F32),
            pltpu.VMEM((NZ, RANK, OWN), F32),
            pltpu.VMEM((NY - 1, ROWS, 128), F32),
            pltpu.VMEM((RANK, 3 * GROUP), BF16),
            pltpu.VMEM((RANK, RANK), F32),
            pltpu.VMEM((NZ // 2 + 1, RANK, RANK), F32),
            pltpu.VMEM((2 * GROUP + 2 * RANK, 2 * RANK), F32),
            pltpu.VMEM((ROWS, 128), F32),
            pltpu.VMEM((NY, 12, 128), F32),
            pltpu.VMEM((NY, 12, 128), F32),
            pltpu.VMEM((NY, 12, 128), F32),
            pltpu.VMEM((CHIPS, 12, 128), F32),
            pltpu.VMEM((12, 128), F32),
            pltpu.VMEM((12, 128), F32),
            dma((7,)),
            dma((2,)),
            dma((2,)),
            dma(()),
            dma(()),
            dma(()),
            dma((NZ,)),
            dma(()),
            dma((NZ // 2,)),
            dma((NY - 1,)),
            dma((NP,)),
            dma(()),
            dma((NP, SUB)),
            dma(()),
            dma((NP, SUB)),
            dma(()),
            dma(()),
            dma((CHIPS,)),
            dma((CHIPS,)),
            dma(()),
            dma(()),
        ],
        compiler_params=pltpu.CompilerParams(
            collective_id=0, has_side_effects=True, vmem_limit_bytes=66_000_000
        ),
    )(spectra, shifts, fractions, pixel_factors, spectral_factors)


def solution(mesh):
    return jax.shard_map(
        body,
        mesh=mesh,
        in_specs=(
            P("pix", "mz"),
            P("pix", "mz"),
            P("pix", "mz"),
            P("pix", None),
            P(None, ("mz", "pix")),
        ),
        out_specs=(P("pix", None), P(None, ("mz", "pix"))),
        check_vma=False,
    )
```

```python
import jax
import jax.numpy as jnp
from jax import lax
from jax.experimental import pallas as pl
from jax.experimental.pallas import tpu as pltpu
from jax.sharding import PartitionSpec as P

SEG = 2048
RANK = 32
EPSILON = 1e-06
ROWS = 16
BINS = 24576
SEGS = BINS // SEG
NZ, NY = 8, 4
OWN = 768
PW = 256
NPZ = OWN // PW
NP = NZ * NPZ
GROUP = NY * ROWS
LAGS = (5, 13, 21, 24)
LATE = 3
LATE_FAR = (1, 4, 7, 10)
SEND_FAR = (-1, 0, 1, 5)
SUB = 2
SUB_ROWS = RANK // SUB
DIRECT = 2
CHUNK = 1024
GROUP_BINS = NY * OWN
EARLY = 6
LATE_CHUNKS = (NZ - EARLY) * (GROUP_BINS // CHUNK)
CHIPS = 16
MESH = pl.DeviceIdType.MESH
F32 = jnp.float32
BF16 = jnp.bfloat16
exact_mode = lax.Precision.HIGHEST
NT = (((1,), (1,)), ((), ()))


def halves(v):
    hi = v.astype(BF16)
    return hi, (v - hi.astype(F32)).astype(BF16)


def kernel(
    x_hbm, sh_hbm, fr_hbm, f_hbm, hin_hbm, w_ref, hout_ref,
    sh_ref, fr_ref, f_ref, hin_ref,
    xp, shb, frb, ws, wg, wgb, cbuf, cout, hbuf, hc, fbuf, lhs, gsend, gbuf, acc,
    f_all, t0s, t0r, t1s, t1r, t3s, t3r,
    xsem, halo_s, halo_r, f_s, f_r, hc_s, hc_r, g_s, g_r,
    y_s, y_r, c_s, c_r, h_s, x_r, t0_s, t0_r, t1_s, t1_r, t3_s, t3_r,
    seen, seen_edge, told, told_edge,
):
    p, m = lax.axis_index("pix"), lax.axis_index("mz")
    z, y = lax.div(p, NY), lax.rem(p, NY)
    mh, ml = lax.div(m, 8), lax.rem(m, 8)
    low_side = z < NZ // 2
    inner = jnp.where(low_side, p + NY, p - NY)
    outer = jnp.where(low_side, p - NY, p + NY)
    depth = jnp.where(low_side, NZ // 2 - 1 - z, z - NZ // 2)
    center = depth == 0
    has_outer = depth < NZ // 2 - 1

    def by_depth(values):
        a, b, c, d = values
        return jnp.where(depth == 0, a, jnp.where(depth == 1, b, jnp.where(depth == 2, c, d)))

    lag = by_depth(LAGS)
    seam = ((mh == 0) & (z == NZ - 1)) | ((mh == 1) & (z == 0))
    across = (m == 7) | (m == 8)
    seam_pix = jnp.where(mh == 0, y, (NZ - 1) * NY + y)
    seam_dev = (seam_pix, lax.rem(m + 8, 16))
    seam_edge = (seam_pix, jnp.where(mh == 0, 8, 7))

    def y_dev(r):
        return (z * NY + lax.rem(y + r, NY), m)

    def m_dev(r):
        return (p, mh * 8 + lax.rem(ml + r, 8))

    far = (p, lax.rem(m + 8, 16))

    def rcopy(src, dst, send, recv, dev):
        return pltpu.make_async_remote_copy(
            src_ref=src, dst_ref=dst, send_sem=send, recv_sem=recv, device_id=dev, device_id_type=MESH
        )

    small = [
        pltpu.make_async_copy(a, b, xsem.at[k])
        for k, (a, b) in enumerate(
            ((sh_hbm, sh_ref), (fr_hbm, fr_ref), (f_hbm, f_ref), (hin_hbm, hin_ref))
        )
    ]
    lo, hi = 3 * GROUP_BINS - 128, 4 * GROUP_BINS + 128
    parts = [
        pltpu.make_async_copy(
            x_hbm.at[:, pl.ds(a, b - a)], xp.at[:, pl.ds(128 + a, b - a)], xsem.at[4 + k]
        )
        for k, (a, b) in enumerate(((lo, hi), (hi, BINS), (0, lo)))
    ]
    for c in small[:2] + parts + small[2:]:
        c.start()

    barrier = pltpu.get_barrier_semaphore()

    def greet(dev):
        pl.semaphore_signal(barrier, inc=1, device_id=dev, device_id_type=MESH)

    core = lax.rem(ml, 2)
    partner = (p, m + 1 - 2 * core)

    def plane_dev(k):
        return (
            z * NY + lax.rem(y + lax.div(k, 4), NY),
            mh * 8 + lax.rem(ml + 2 * lax.rem(k, 4), 8),
        )

    for k in range(1, CHIPS):
        greet(plane_dev(k))
    greet(partner)

    def column_dev(k):
        return (lax.rem(z + k, NZ) * NY + y, m)

    for k in range(1, NZ):
        greet(column_dev(k))

    @pl.when((core == 0) & (ml > 0))
    def _():
        greet((p, m - 1))

    @pl.when((core == 1) & (ml < 7))
    def _():
        greet((p, m + 1))

    @pl.when(seam)
    def _():
        greet(seam_dev)

    @pl.when(seam & across)
    def _():
        greet(seam_edge)

    acc[...] = jnp.zeros_like(acc)

    @pl.when(m == 0)
    def _():
        xp[:, 0:128] = jnp.zeros((ROWS, 128), F32)

    @pl.when(m == 15)
    def _():
        xp[:, 128 + BINS :] = jnp.zeros((ROWS, 128), F32)

    small[0].wait()
    small[1].wait()
    for s in range(SEGS):
        shb[s] = jnp.broadcast_to(sh_ref[:, s : s + 1], (ROWS, 128))
        frb[s] = jnp.broadcast_to(fr_ref[:, s : s + 1], (ROWS, 128))

    def group_z(g):
        step = lax.div(g, 2)
        return jnp.where(lax.rem(g, 2) == 0, NZ // 2 - 1 - step, NZ // 2 + step)

    def piece(i):
        return group_z(lax.div(i, NPZ)) * NPZ + lax.rem(i, NPZ)

    def own_bins(t):
        return first_bin(0, t)

    def first_bin(r, t):
        zq, j = lax.div(t, NPZ), lax.rem(t, NPZ)
        return pl.multiple_of(zq * GROUP_BINS + lax.rem(y + r, NY) * OWN + j * PW, 128)

    def warp(c):
        width = CHUNK + 256
        b = pl.multiple_of(c * CHUNK, 128)
        seg = lax.div(b, SEG)
        d, f = shb[seg], frb[seg]

        def wide(v, lanes):
            return jnp.concatenate([v] * (lanes // 128), axis=1)

        v = xp[:, pl.ds(b, width)]
        v = jnp.where(wide(d, width) < 0, pltpu.roll(v, 4, 1), v)
        shifted = [v] + [pltpu.roll(v, width - k, 1) for k in range(1, 5)]
        shifted = [u[:, 128 : 128 + CHUNK] for u in shifted]
        rest = wide(d & 3, CHUNK)
        high, odd = rest >= 2, (rest & 1) != 0

        def pick(k):
            return jnp.where(
                high,
                jnp.where(odd, shifted[k + 3], shifted[k + 2]),
                jnp.where(odd, shifted[k + 1], shifted[k]),
            )

        f = wide(f, CHUNK)
        ws[:, pl.ds(b, CHUNK)] = (1.0 - f) * pick(0) + f * pick(1)

    def warp_group(g):
        zq = group_z(g)

        for k in range(GROUP_BINS // CHUNK):
            warp(zq * (GROUP_BINS // CHUNK) + k)

    def y_copy(r, t):
        src = ws.at[:, pl.ds(first_bin(r, t), PW)]
        return rcopy(src, wg.at[t, NY - r - 1], y_s.at[r - 1], y_r.at[t], y_dev(r))

    def send_group(g):
        zq = group_z(g)
        for j in range(NPZ):
            for r in range(1, NY):
                y_copy(r, zq * NPZ + j).start()

    parts[0].wait()
    with jax.named_scope("warps"):
        warp_group(0)
    small[2].wait()
    f_all[...] = jnp.concatenate([f_ref[...], jnp.zeros((ROWS, 128 - RANK), F32)], axis=1)
    with jax.named_scope("barrier"):
        pl.semaphore_wait(
            barrier,
            CHIPS
            + NZ
            - 1
            + jnp.where((ml == 0) | (ml == 7), 0, 1)
            + jnp.where(seam, 1, 0)
            + jnp.where(seam & across, 1, 0),
        )

    def signal(sem, dev):
        pl.semaphore_signal(sem, inc=1, device_id=dev, device_id_type=MESH)

    @pl.when(seam)
    def _():
        signal(seen, seam_dev)

    @pl.when(seam & across)
    def _():
        signal(seen_edge, seam_edge)

    f_copies = [
        rcopy(f_all, fbuf.at[NY - r - 1], f_s, f_r, y_dev(r)) for r in range(1, NY)
    ]
    for c in f_copies:
        c.start()
    send_group(0)
    parts[1].wait()
    parts[2].wait()
    small[3].wait()

    to_right = rcopy(
        xp.at[:, pl.ds(BINS, 128)], xp.at[:, pl.ds(0, 128)], halo_s.at[0], halo_r.at[0], (p, m + 1)
    )
    to_left = rcopy(
        xp.at[:, pl.ds(128, 128)], xp.at[:, pl.ds(128 + BINS, 128)], halo_s.at[1], halo_r.at[1], (p, m - 1)
    )

    @pl.when((m < 15) & (m != 7))
    def _():
        to_right.start()

    @pl.when((m > 0) & (m != 8))
    def _():
        to_left.start()

    def send_far():
        @pl.when(m == 7)
        def _():
            to_right.start()

        @pl.when(m == 8)
        def _():
            to_left.start()

    near = jnp.where(low_side, NZ // 2 - 1, NZ // 2)

    h_part = rcopy(hin_ref, hc.at[z], hc_s, hc_r.at[z], (jnp.where(center, inner, near * NY + y), m))

    def h_relay(zk):
        return rcopy(hc.at[zk], hc.at[zk], hc_s, hc_r.at[zk], (inner, m))

    @pl.when(depth <= 1)
    def _():
        h_part.start()

    @pl.when(center)
    def _():
        hc[z] = hin_ref[...]

    def early(g, carry):
        warp_group(g)
        send_group(g)

        @pl.when(((g == 1) & (depth == 2)) | ((g == 2) & (depth == 3)))
        def _():
            h_part.start()

        return carry

    with jax.named_scope("warps"):
        lax.fori_loop(1, EARLY, early, 0)

    with jax.named_scope("fwait"):
        rcopy(fbuf, fbuf, f_s, f_r, y_dev(1)).wait_recv()

    @pl.when(seam)
    def _():
        pl.semaphore_wait(seen, 1)
        for k in range(1, NZ):
            signal(told, column_dev(k))

    @pl.when(seam & across)
    def _():
        pl.semaphore_wait(seen_edge, 1)
        send_far()
        for k in range(1, NZ):
            signal(told_edge, column_dev(k))

    def send_far_told():
        pl.semaphore_wait(told_edge, 1)
        send_far()

    fg = jnp.concatenate([f_all[...], fbuf[...].reshape(GROUP - ROWS, 128)], axis=0)[:, 0:RANK]
    gy = lax.dot_general(fg, fg, (((0,), (0,)), ((), ())), precision=exact_mode, preferred_element_type=F32)
    f_hi, f_lo = halves(fg.T)
    lhs[...] = jnp.concatenate([f_hi, f_hi, f_lo], axis=1)

    g_half = rcopy(gsend, gbuf.at[depth], g_s, g_r.at[depth], (near * NY + y, m))
    g_other = rcopy(gsend, gbuf.at[0], g_s, g_r.at[0], (inner, m))

    def outward(k):
        return jnp.where(low_side, NZ // 2 - 1 - k, NZ // 2 + k)

    def warp_late(e):
        chunks = GROUP_BINS // CHUNK
        g = EARLY + lax.div(e, chunks)

        @pl.when((e == 0) & (m > 0))
        def _():
            to_right.wait_recv()

        @pl.when((e == 2 * chunks - 1) & (m < 15))
        def _():
            to_left.wait_recv()

        warp(group_z(g) * chunks + lax.rem(e, chunks))

        @pl.when(lax.rem(e, chunks) == chunks - 1)
        def _():
            send_group(g)

    @pl.when(jnp.logical_not(center))
    def _():
        gsend[...] = gy
        g_half.start()

    def relay(k):
        h_relay(outward(k)).wait_recv()
        h_relay(outward(k)).start()

    @pl.when(center)
    def _():
        with jax.named_scope("relay"):
            relay(1)
            relay(2)
            total = gy
            for k in range(1, NZ // 2):
                rcopy(gsend, gbuf.at[k], g_s, g_r.at[k], (inner, m)).wait_recv()
                total = total + gbuf[k]
            gsend[...] = total
            gbuf[NZ // 2] = total
            g_other.start()
            relay(3)

        def late(e, carry):
            warp_late(e)
            return carry

        @pl.when(across)
        def _():
            send_far_told()

        @pl.when(jnp.logical_not(across))
        def _():
            lax.fori_loop(0, LATE_CHUNKS, late, 0)

    late_from = jnp.where(across, by_depth(LATE_FAR), jnp.where(center, -LATE_CHUNKS, LATE))
    send_far_step = jnp.where(across & jnp.logical_not(seam), by_depth(SEND_FAR), -1)

    def rows_of(q):
        return pl.ds(q * SUB_ROWS, SUB_ROWS)

    def c_copy(t, q):
        dst = cbuf.at[0, t, rows_of(q)]
        return rcopy(cout.at[t, rows_of(q)], dst, c_s, c_r.at[t, q], (inner, m))

    def cx_copy(t, q):
        dst = cbuf.at[1, t, rows_of(q)]
        return rcopy(cout.at[t, rows_of(q)], dst, c_s, x_r.at[t, q], (inner, m))

    def c_send(t, q):
        @pl.when(center)
        def _():
            cx_copy(t, q).start()

        @pl.when(jnp.logical_not(center))
        def _():
            c_copy(t, q).start()

    def h_copy(t, q, dev):
        part = hbuf.at[t, rows_of(q)]
        return rcopy(part, part, h_s, x_r.at[t, q], dev)

    def step(i, carry):
        @pl.when(i < NP)
        def _():
            t = piece(i)
            with jax.named_scope("ywait"):
                rcopy(wg.at[t], wg.at[t], y_s.at[0], y_r.at[t], y_dev(1)).wait_recv()
            mine = ws[:, pl.ds(own_bins(t), PW)]
            w_hi, w_lo = halves(jnp.concatenate([mine, wg[t].reshape(GROUP - ROWS, PW)], axis=0))
            both = jnp.concatenate([w_hi, w_lo], axis=0)
            wgb[t] = both
            n = jnp.dot(lhs[...], jnp.concatenate([both, w_hi], axis=0), preferred_element_type=F32)

            @pl.when(i == send_far_step)
            def _():
                send_far_told()

            @pl.when(has_outer)
            def _():
                for q in range(SUB):
                    with jax.named_scope("cwait"):
                        c_copy(t, q).wait_recv()
                    part = n[q * SUB_ROWS : (q + 1) * SUB_ROWS]
                    cout[t, rows_of(q)] = part + cbuf[0, t, rows_of(q)]
                    c_send(t, q)

            @pl.when(jnp.logical_not(has_outer))
            def _():
                cout[t] = n
                for q in range(SUB):
                    c_send(t, q)

            late = i - late_from

            @pl.when((late >= 0) & (late < LATE_CHUNKS))
            def _():
                warp_late(late)

        k = i - lag

        @pl.when((k >= 0) & (k < NP))
        def _():
            t = piece(k)

            @pl.when(center)
            def _():
                zq, j = lax.div(t, NPZ), lax.rem(t, NPZ)

                @pl.when(k == 0)
                def _():
                    g_other.wait_recv()
                    gbuf[NZ // 2] = gbuf[NZ // 2] + gbuf[0]

                @pl.when((j == 0) & (lax.div(zq, NZ // 2) != lax.div(z, NZ // 2)))
                def _():
                    with jax.named_scope("hcwait"):
                        h_relay(zq).wait_recv()

                own = hc[zq, :, pl.ds(pl.multiple_of(j * PW, 128), PW)]
                bottom = jnp.dot(gbuf[NZ // 2], own, precision=exact_mode, preferred_element_type=F32) + EPSILON
                ratio = own / bottom
                for q in range(SUB):
                    with jax.named_scope("xcwait"):
                        cx_copy(t, q).wait_recv()
                    r = rows_of(q)
                    hbuf[t, r] = ratio[q * SUB_ROWS : (q + 1) * SUB_ROWS] * (cout[t, r] + cbuf[1, t, r])

                    @pl.when(k >= NP - DIRECT)
                    def _():
                        for far_out in (3, 2):
                            h_copy(t, q, (outward(far_out) * NY + y, m)).start()

                    h_copy(t, q, (outer, m)).start()

            @pl.when(jnp.logical_not(center))
            def _():
                for q in range(SUB):
                    with jax.named_scope("hwait"):
                        h_copy(t, q, (outer, m)).wait_recv()

                    @pl.when(has_outer & (k < NP - DIRECT))
                    def _():
                        h_copy(t, q, (outer, m)).start()

            h = hbuf[t]
            h_hi, h_lo = halves(h)
            right = jnp.concatenate([h_hi, h_lo], axis=0)
            left = jnp.concatenate([wgb[t], right], axis=0)
            acc[...] += lax.dot_general(left, right, NT, preferred_element_type=F32)

            @pl.when(lax.div(t, NPZ) == z)
            def _():
                hout_ref[:, pl.ds(pl.multiple_of(lax.rem(t, NPZ) * PW, 128), PW)] = h

        return carry

    lax.fori_loop(0, NP + LAGS[-1], step, 0)

    both = acc[:, 0:RANK] + acc[:, RANK : 2 * RANK]
    proj = both[0:GROUP] + both[GROUP : 2 * GROUP]
    base = 2 * GROUP
    gram = both[base : base + RANK] + both[base + RANK : base + 2 * RANK]
    gram8 = jnp.concatenate([gram[8 * q : 8 * q + 8] for q in range(4)], axis=1)
    for k in range(NY):
        rows = proj[k * ROWS : (k + 1) * ROWS]
        t0s[k, 0:8] = gram8
        t0s[k, 8:12] = jnp.concatenate([rows[4 * q : 4 * q + 4] for q in range(4)], axis=1)
    t0_copy = rcopy(t0s, t0r, t0_s, t0_r, partner)
    t0_copy.start()
    with jax.named_scope("t0wait"):
        t0_copy.wait_recv()
    t1s[...] = t0s[...] + t0r[...]

    me = y * 4 + lax.div(ml, 2)

    def t_copy(k):
        return rcopy(t1s.at[lax.div(k, 4)], t1r.at[me], t1_s.at[k], t1_r.at[k], plane_dev(k))

    t1_copies = [t_copy(k) for k in range(1, CHIPS)]
    for c in t1_copies:
        c.start()
    t1r[me] = t1s[0]
    with jax.named_scope("t1wait"):
        for c in t1_copies:
            c.wait_recv()
    sums = [t1r[k] for k in range(CHIPS)]
    while len(sums) > 1:
        sums = [a + b for a, b in zip(sums[::2], sums[1::2])]
    t3s[...] = sums[0]
    @pl.when(jnp.logical_not(seam))
    def _():
        pl.semaphore_wait(told, 1)

    t3_copy = rcopy(t3s, t3r, t3_s, t3_r, far)
    t3_copy.start()
    with jax.named_scope("t3wait"):
        t3_copy.wait_recv()
    total = sums[0] + t3r[...]
    gram_sum = jnp.concatenate([total[0:8, 32 * q : 32 * q + 32] for q in range(4)], axis=0)
    proj_sum = jnp.concatenate([total[8:12, 32 * q : 32 * q + 32] for q in range(4)], axis=0)
    f = f_ref[...]
    g_hi, g_lo = halves(gram_sum)
    own_hi, own_lo = halves(f)
    bottom = EPSILON + jnp.dot(
        jnp.concatenate([own_hi, own_hi, own_lo], axis=1),
        jnp.concatenate([g_hi, g_lo, g_hi], axis=0),
        preferred_element_type=F32,
    )
    w_ref[...] = f * proj_sum / bottom

    rcopy(fbuf, fbuf, f_s, f_r, y_dev(1)).wait_send()
    for c in t1_copies + [t0_copy, t3_copy]:
        c.wait_send()

    @pl.when(m < 15)
    def _():
        to_right.wait_send()

    @pl.when(m > 0)
    def _():
        to_left.wait_send()

    g_half.wait_send()
    h_part.wait_send()

    @pl.when(center)
    def _():
        part = hc.at[pl.ds(0, NZ // 2 - 1)]
        rcopy(part, part, hc_s, hc_s, (inner, m)).wait_send()

    for r in range(1, NY):
        rcopy(wg.at[:, r - 1], wg.at[:, r - 1], y_s.at[r - 1], y_s.at[r - 1], y_dev(r)).wait_send()
    rcopy(cout, cout, c_s, c_s, (inner, m)).wait_send()

    def h_sent(pieces):
        part = hbuf.at[pl.ds(0, pieces)]
        rcopy(part, part, h_s, h_s, (outer, m)).wait_send()

    @pl.when(center)
    def _():
        h_sent(NP)
        h_sent(2 * DIRECT)

    @pl.when(has_outer & jnp.logical_not(center))
    def _():
        h_sent(NP - DIRECT)


def body(spectra, shifts, fractions, pixel_factors, spectral_factors):
    vmem = pl.BlockSpec(memory_space=pltpu.VMEM)
    dma = pltpu.SemaphoreType.DMA
    return pl.pallas_call(
        kernel,
        out_shape=(
            pltpu.VMEM((ROWS, RANK), F32),
            pltpu.VMEM((RANK, OWN), F32),
        ),
        in_specs=[pl.BlockSpec(memory_space=pltpu.HBM)] * 5,
        out_specs=(vmem, vmem),
        scratch_shapes=[
            pltpu.VMEM((ROWS, SEGS), jnp.int32),
            pltpu.VMEM((ROWS, SEGS), F32),
            pltpu.VMEM((ROWS, RANK), F32),
            pltpu.VMEM((RANK, OWN), F32),
            pltpu.VMEM((ROWS, BINS + 256), F32),
            pltpu.VMEM((SEGS, ROWS, 128), jnp.int32),
            pltpu.VMEM((SEGS, ROWS, 128), F32),
            pltpu.VMEM((ROWS, BINS), F32),
            pltpu.VMEM((NP, NY - 1, ROWS, PW), F32),
            pltpu.VMEM((NP, 2 * GROUP, PW), BF16),
            pltpu.VMEM((2, NP, RANK, PW), F32),
            pltpu.VMEM((NP, RANK, PW), F32),
            pltpu.VMEM((NP, RANK, PW), F32),
            pltpu.VMEM((NZ, RANK, OWN), F32),
            pltpu.VMEM((NY - 1, ROWS, 128), F32),
            pltpu.VMEM((RANK, 3 * GROUP), BF16),
            pltpu.VMEM((RANK, RANK), F32),
            pltpu.VMEM((NZ // 2 + 1, RANK, RANK), F32),
            pltpu.VMEM((2 * GROUP + 2 * RANK, 2 * RANK), F32),
            pltpu.VMEM((ROWS, 128), F32),
            pltpu.VMEM((NY, 12, 128), F32),
            pltpu.VMEM((NY, 12, 128), F32),
            pltpu.VMEM((NY, 12, 128), F32),
            pltpu.VMEM((CHIPS, 12, 128), F32),
            pltpu.VMEM((12, 128), F32),
            pltpu.VMEM((12, 128), F32),
            dma((7,)),
            dma((2,)),
            dma((2,)),
            dma(()),
            dma(()),
            dma(()),
            dma((NZ,)),
            dma(()),
            dma((NZ // 2,)),
            dma((NY - 1,)),
            dma((NP,)),
            dma(()),
            dma((NP, SUB)),
            dma(()),
            dma((NP, SUB)),
            dma(()),
            dma(()),
            dma((CHIPS,)),
            dma((CHIPS,)),
            dma(()),
            dma(()),
            pltpu.SemaphoreType.REGULAR,
            pltpu.SemaphoreType.REGULAR,
            pltpu.SemaphoreType.REGULAR,
            pltpu.SemaphoreType.REGULAR,
        ],
        compiler_params=pltpu.CompilerParams(
            collective_id=0, has_side_effects=True, vmem_limit_bytes=66_000_000
        ),
    )(spectra, shifts, fractions, pixel_factors, spectral_factors)


def solution(mesh):
    return jax.shard_map(
        body,
        mesh=mesh,
        in_specs=(
            P("pix", "mz"),
            P("pix", "mz"),
            P("pix", "mz"),
            P("pix", None),
            P(None, ("mz", "pix")),
        ),
        out_specs=(P("pix", None), P(None, ("mz", "pix"))),
        check_vma=False,
    )
```

```python
import jax
import jax.numpy as jnp
from jax import lax
from jax.experimental import pallas as pl
from jax.experimental.pallas import tpu as pltpu
from jax.sharding import PartitionSpec as P

SEG = 2048
RANK = 32
EPSILON = 1e-06
ROWS = 16
BINS = 24576
SEGS = BINS // SEG
NZ, NY = 8, 4
OWN = 768
PW = 256
NPZ = OWN // PW
NP = NZ * NPZ
GROUP = NY * ROWS
LAGS = (5, 13, 21, 24)
LATE = 2
LATE_FAR = (2, 7, 11, 16)
SEND_FAR = (-1, 0, 1, 6)
SUB = 2
SUB_ROWS = RANK // SUB
DIRECT = 2
CHUNK = 1024
GROUP_BINS = NY * OWN
EARLY = 6
LATE_CHUNKS = (NZ - EARLY) * (GROUP_BINS // CHUNK)
CHIPS = 16
MESH = pl.DeviceIdType.MESH
F32 = jnp.float32
BF16 = jnp.bfloat16
exact_mode = lax.Precision.HIGHEST
NT = (((1,), (1,)), ((), ()))


def halves(v):
    hi = v.astype(BF16)
    return hi, (v - hi.astype(F32)).astype(BF16)


def kernel(
    x_hbm, sh_hbm, fr_hbm, f_hbm, hin_hbm, w_ref, hout_ref,
    sh_ref, fr_ref, f_ref, hin_ref,
    xp, shb, frb, ws, wg, wgb, cbuf, cout, hbuf, hc, fbuf, lhs, gsend, gbuf, acc,
    f_all, t0s, t0r, t1s, t1r, t3s, t3r,
    xsem, halo_s, halo_r, f_s, f_r, hc_s, hc_r, g_s, g_r,
    y_s, y_r, c_s, c_r, h_s, x_r, t0_s, t0_r, t1_s, t1_r, t3_s, t3_r,
    seen, seen_edge, told, told_edge,
):
    p, m = lax.axis_index("pix"), lax.axis_index("mz")
    z, y = lax.div(p, NY), lax.rem(p, NY)
    mh, ml = lax.div(m, 8), lax.rem(m, 8)
    low_side = z < NZ // 2
    inner = jnp.where(low_side, p + NY, p - NY)
    outer = jnp.where(low_side, p - NY, p + NY)
    depth = jnp.where(low_side, NZ // 2 - 1 - z, z - NZ // 2)
    center = depth == 0
    has_outer = depth < NZ // 2 - 1

    def by_depth(values):
        a, b, c, d = values
        return jnp.where(depth == 0, a, jnp.where(depth == 1, b, jnp.where(depth == 2, c, d)))

    lag = by_depth(LAGS)
    seam = ((mh == 0) & (z == NZ - 1)) | ((mh == 1) & (z == 0))
    across = (m == 7) | (m == 8)
    seam_pix = jnp.where(mh == 0, y, (NZ - 1) * NY + y)
    seam_dev = (seam_pix, lax.rem(m + 8, 16))
    seam_edge = (seam_pix, jnp.where(mh == 0, 8, 7))

    def y_dev(r):
        return (z * NY + lax.rem(y + r, NY), m)

    def m_dev(r):
        return (p, mh * 8 + lax.rem(ml + r, 8))

    far = (p, lax.rem(m + 8, 16))

    def rcopy(src, dst, send, recv, dev):
        return pltpu.make_async_remote_copy(
            src_ref=src, dst_ref=dst, send_sem=send, recv_sem=recv, device_id=dev, device_id_type=MESH
        )

    small = [
        pltpu.make_async_copy(a, b, xsem.at[k])
        for k, (a, b) in enumerate(
            ((sh_hbm, sh_ref), (fr_hbm, fr_ref), (f_hbm, f_ref), (hin_hbm, hin_ref))
        )
    ]
    lo, hi = 3 * GROUP_BINS - 128, 4 * GROUP_BINS + 128
    parts = [
        pltpu.make_async_copy(
            x_hbm.at[:, pl.ds(a, b - a)], xp.at[:, pl.ds(128 + a, b - a)], xsem.at[4 + k]
        )
        for k, (a, b) in enumerate(((lo, hi), (hi, BINS), (0, lo)))
    ]
    for c in small[:2] + parts + small[2:]:
        c.start()

    barrier = pltpu.get_barrier_semaphore()

    def greet(dev):
        pl.semaphore_signal(barrier, inc=1, device_id=dev, device_id_type=MESH)

    core = lax.rem(ml, 2)
    partner = (p, m + 1 - 2 * core)

    def plane_dev(k):
        return (
            z * NY + lax.rem(y + lax.div(k, 4), NY),
            mh * 8 + lax.rem(ml + 2 * lax.rem(k, 4), 8),
        )

    for k in range(1, CHIPS):
        greet(plane_dev(k))
    greet(partner)

    def column_dev(k):
        return (lax.rem(z + k, NZ) * NY + y, m)

    for k in range(1, NZ):
        greet(column_dev(k))

    @pl.when((core == 0) & (ml > 0))
    def _():
        greet((p, m - 1))

    @pl.when((core == 1) & (ml < 7))
    def _():
        greet((p, m + 1))

    @pl.when(seam)
    def _():
        greet(seam_dev)

    @pl.when(seam & across)
    def _():
        greet(seam_edge)

    acc[...] = jnp.zeros_like(acc)

    @pl.when(m == 0)
    def _():
        xp[:, 0:128] = jnp.zeros((ROWS, 128), F32)

    @pl.when(m == 15)
    def _():
        xp[:, 128 + BINS :] = jnp.zeros((ROWS, 128), F32)

    small[0].wait()
    small[1].wait()
    for s in range(SEGS):
        shb[s] = jnp.broadcast_to(sh_ref[:, s : s + 1], (ROWS, 128))
        frb[s] = jnp.broadcast_to(fr_ref[:, s : s + 1], (ROWS, 128))

    def group_z(g):
        step = lax.div(g, 2)
        flip = jnp.where((m == 8) & (g >= EARLY), 1, 0)
        return jnp.where(lax.rem(g, 2) == flip, NZ // 2 - 1 - step, NZ // 2 + step)

    def piece(i):
        return group_z(lax.div(i, NPZ)) * NPZ + lax.rem(i, NPZ)

    def own_bins(t):
        return first_bin(0, t)

    def first_bin(r, t):
        zq, j = lax.div(t, NPZ), lax.rem(t, NPZ)
        return pl.multiple_of(zq * GROUP_BINS + lax.rem(y + r, NY) * OWN + j * PW, 128)

    def warp(c):
        width = CHUNK + 256
        b = pl.multiple_of(c * CHUNK, 128)
        seg = lax.div(b, SEG)
        d, f = shb[seg], frb[seg]

        def wide(v, lanes):
            return jnp.concatenate([v] * (lanes // 128), axis=1)

        v = xp[:, pl.ds(b, width)]
        v = jnp.where(wide(d, width) < 0, pltpu.roll(v, 4, 1), v)
        shifted = [v] + [pltpu.roll(v, width - k, 1) for k in range(1, 5)]
        shifted = [u[:, 128 : 128 + CHUNK] for u in shifted]
        rest = wide(d & 3, CHUNK)
        high, odd = rest >= 2, (rest & 1) != 0

        def pick(k):
            return jnp.where(
                high,
                jnp.where(odd, shifted[k + 3], shifted[k + 2]),
                jnp.where(odd, shifted[k + 1], shifted[k]),
            )

        f = wide(f, CHUNK)
        ws[:, pl.ds(b, CHUNK)] = (1.0 - f) * pick(0) + f * pick(1)

    def warp_group(g):
        zq = group_z(g)

        for k in range(GROUP_BINS // CHUNK):
            warp(zq * (GROUP_BINS // CHUNK) + k)

    def y_copy(r, t):
        src = ws.at[:, pl.ds(first_bin(r, t), PW)]
        return rcopy(src, wg.at[t, NY - r - 1], y_s.at[r - 1], y_r.at[t], y_dev(r))

    def send_group(g):
        zq = group_z(g)
        for j in range(NPZ):
            for r in range(1, NY):
                y_copy(r, zq * NPZ + j).start()

    parts[0].wait()
    with jax.named_scope("warps"):
        warp_group(0)
    small[2].wait()
    f_all[...] = jnp.concatenate([f_ref[...], jnp.zeros((ROWS, 128 - RANK), F32)], axis=1)
    with jax.named_scope("barrier"):
        pl.semaphore_wait(
            barrier,
            CHIPS
            + NZ
            - 1
            + jnp.where((ml == 0) | (ml == 7), 0, 1)
            + jnp.where(seam, 1, 0)
            + jnp.where(seam & across, 1, 0),
        )

    def signal(sem, dev):
        pl.semaphore_signal(sem, inc=1, device_id=dev, device_id_type=MESH)

    @pl.when(seam)
    def _():
        signal(seen, seam_dev)

    @pl.when(seam & across)
    def _():
        signal(seen_edge, seam_edge)

    f_copies = [
        rcopy(f_all, fbuf.at[NY - r - 1], f_s, f_r, y_dev(r)) for r in range(1, NY)
    ]
    for c in f_copies:
        c.start()
    send_group(0)
    parts[1].wait()
    parts[2].wait()
    small[3].wait()

    to_right = rcopy(
        xp.at[:, pl.ds(BINS, 128)], xp.at[:, pl.ds(0, 128)], halo_s.at[0], halo_r.at[0], (p, m + 1)
    )
    to_left = rcopy(
        xp.at[:, pl.ds(128, 128)], xp.at[:, pl.ds(128 + BINS, 128)], halo_s.at[1], halo_r.at[1], (p, m - 1)
    )

    @pl.when((m < 15) & (m != 7))
    def _():
        to_right.start()

    @pl.when((m > 0) & (m != 8))
    def _():
        to_left.start()

    def send_far():
        @pl.when(m == 7)
        def _():
            to_right.start()

        @pl.when(m == 8)
        def _():
            to_left.start()

    near = jnp.where(low_side, NZ // 2 - 1, NZ // 2)

    h_part = rcopy(hin_ref, hc.at[z], hc_s, hc_r.at[z], (jnp.where(center, inner, near * NY + y), m))

    def h_relay(zk):
        return rcopy(hc.at[zk], hc.at[zk], hc_s, hc_r.at[zk], (inner, m))

    @pl.when(depth <= 1)
    def _():
        h_part.start()

    @pl.when(center)
    def _():
        hc[z] = hin_ref[...]

    def early(g, carry):
        warp_group(g)
        send_group(g)

        @pl.when(((g == 1) & (depth == 2)) | ((g == 2) & (depth == 3)))
        def _():
            h_part.start()

        return carry

    with jax.named_scope("warps"):
        lax.fori_loop(1, EARLY, early, 0)

    with jax.named_scope("fwait"):
        rcopy(fbuf, fbuf, f_s, f_r, y_dev(1)).wait_recv()

    @pl.when(seam)
    def _():
        pl.semaphore_wait(seen, 1)
        for k in range(1, NZ):
            signal(told, column_dev(k))

    @pl.when(seam & across)
    def _():
        pl.semaphore_wait(seen_edge, 1)
        send_far()
        for k in range(1, NZ):
            signal(told_edge, column_dev(k))

    def send_far_told():
        pl.semaphore_wait(told_edge, 1)
        send_far()

    fg = jnp.concatenate([f_all[...], fbuf[...].reshape(GROUP - ROWS, 128)], axis=0)[:, 0:RANK]
    gy = lax.dot_general(fg, fg, (((0,), (0,)), ((), ())), precision=exact_mode, preferred_element_type=F32)
    f_hi, f_lo = halves(fg.T)
    lhs[...] = jnp.concatenate([f_hi, f_hi, f_lo], axis=1)

    g_half = rcopy(gsend, gbuf.at[depth], g_s, g_r.at[depth], (near * NY + y, m))
    g_other = rcopy(gsend, gbuf.at[0], g_s, g_r.at[0], (inner, m))

    def outward(k):
        return jnp.where(low_side, NZ // 2 - 1 - k, NZ // 2 + k)

    def warp_late(e):
        chunks = GROUP_BINS // CHUNK
        g = EARLY + lax.div(e, chunks)
        k = lax.rem(e, chunks)
        left, right = jnp.where(m == 8, LATE_CHUNKS - 1, 0), jnp.where(m == 8, 0, LATE_CHUNKS - 1)

        @pl.when((e == left) & (m > 0))
        def _():
            to_right.wait_recv()

        @pl.when((e == right) & (m < 15))
        def _():
            to_left.wait_recv()

        warp(group_z(g) * chunks + jnp.where(m == 8, chunks - 1 - k, k))

        @pl.when(lax.rem(e, chunks) == chunks - 1)
        def _():
            send_group(g)

    @pl.when(jnp.logical_not(center))
    def _():
        gsend[...] = gy
        g_half.start()

    def relay(k):
        h_relay(outward(k)).wait_recv()
        h_relay(outward(k)).start()

    @pl.when(center)
    def _():
        with jax.named_scope("relay"):
            relay(1)
            relay(2)
            total = gy
            for k in range(1, NZ // 2):
                rcopy(gsend, gbuf.at[k], g_s, g_r.at[k], (inner, m)).wait_recv()
                total = total + gbuf[k]
            gsend[...] = total
            gbuf[NZ // 2] = total
            g_other.start()
            relay(3)

        def late(e, carry):
            warp_late(e)
            return carry

        @pl.when(across)
        def _():
            send_far_told()

        lax.fori_loop(0, LATE_CHUNKS - 1, late, 0)

        @pl.when(jnp.logical_not(across))
        def _():
            warp_late(LATE_CHUNKS - 1)

    late_from = jnp.where(center, -LATE_CHUNKS, LATE)
    late_far = jnp.where(across, by_depth(LATE_FAR), -1)
    late_near = LATE_CHUNKS - jnp.where(across, 1, 0)
    send_far_step = jnp.where(across & jnp.logical_not(seam), by_depth(SEND_FAR), -1)

    def rows_of(q):
        return pl.ds(q * SUB_ROWS, SUB_ROWS)

    def c_copy(t, q):
        dst = cbuf.at[0, t, rows_of(q)]
        return rcopy(cout.at[t, rows_of(q)], dst, c_s, c_r.at[t, q], (inner, m))

    def cx_copy(t, q):
        dst = cbuf.at[1, t, rows_of(q)]
        return rcopy(cout.at[t, rows_of(q)], dst, c_s, x_r.at[t, q], (inner, m))

    def c_send(t, q):
        @pl.when(center)
        def _():
            cx_copy(t, q).start()

        @pl.when(jnp.logical_not(center))
        def _():
            c_copy(t, q).start()

    def h_copy(t, q, dev):
        part = hbuf.at[t, rows_of(q)]
        return rcopy(part, part, h_s, x_r.at[t, q], dev)

    def step(i, carry):
        @pl.when(i < NP)
        def _():
            t = piece(i)
            with jax.named_scope("ywait"):
                rcopy(wg.at[t], wg.at[t], y_s.at[0], y_r.at[t], y_dev(1)).wait_recv()
            mine = ws[:, pl.ds(own_bins(t), PW)]
            w_hi, w_lo = halves(jnp.concatenate([mine, wg[t].reshape(GROUP - ROWS, PW)], axis=0))
            both = jnp.concatenate([w_hi, w_lo], axis=0)
            wgb[t] = both
            n = jnp.dot(lhs[...], jnp.concatenate([both, w_hi], axis=0), preferred_element_type=F32)

            @pl.when(i == send_far_step)
            def _():
                send_far_told()

            @pl.when(has_outer)
            def _():
                for q in range(SUB):
                    with jax.named_scope("cwait"):
                        c_copy(t, q).wait_recv()
                    part = n[q * SUB_ROWS : (q + 1) * SUB_ROWS]
                    cout[t, rows_of(q)] = part + cbuf[0, t, rows_of(q)]
                    c_send(t, q)

            @pl.when(jnp.logical_not(has_outer))
            def _():
                cout[t] = n
                for q in range(SUB):
                    c_send(t, q)

            late = i - late_from

            @pl.when(((late >= 0) & (late < late_near)) | (i == late_far))
            def _():
                warp_late(jnp.where(i == late_far, LATE_CHUNKS - 1, late))

        k = i - lag

        @pl.when((k >= 0) & (k < NP))
        def _():
            t = piece(k)

            @pl.when(center)
            def _():
                zq, j = lax.div(t, NPZ), lax.rem(t, NPZ)

                @pl.when(k == 0)
                def _():
                    g_other.wait_recv()
                    gbuf[NZ // 2] = gbuf[NZ // 2] + gbuf[0]

                @pl.when((j == 0) & (lax.div(zq, NZ // 2) != lax.div(z, NZ // 2)))
                def _():
                    with jax.named_scope("hcwait"):
                        h_relay(zq).wait_recv()

                own = hc[zq, :, pl.ds(pl.multiple_of(j * PW, 128), PW)]
                bottom = jnp.dot(gbuf[NZ // 2], own, precision=exact_mode, preferred_element_type=F32) + EPSILON
                ratio = own / bottom
                for q in range(SUB):
                    with jax.named_scope("xcwait"):
                        cx_copy(t, q).wait_recv()
                    r = rows_of(q)
                    hbuf[t, r] = ratio[q * SUB_ROWS : (q + 1) * SUB_ROWS] * (cout[t, r] + cbuf[1, t, r])

                    @pl.when(k >= NP - DIRECT)
                    def _():
                        for far_out in (3, 2):
                            h_copy(t, q, (outward(far_out) * NY + y, m)).start()

                    h_copy(t, q, (outer, m)).start()

            @pl.when(jnp.logical_not(center))
            def _():
                for q in range(SUB):
                    with jax.named_scope("hwait"):
                        h_copy(t, q, (outer, m)).wait_recv()

                    @pl.when(has_outer & (k < NP - DIRECT))
                    def _():
                        h_copy(t, q, (outer, m)).start()

            h = hbuf[t]
            h_hi, h_lo = halves(h)
            right = jnp.concatenate([h_hi, h_lo], axis=0)
            left = jnp.concatenate([wgb[t], right], axis=0)
            acc[...] += lax.dot_general(left, right, NT, preferred_element_type=F32)

            @pl.when(lax.div(t, NPZ) == z)
            def _():
                hout_ref[:, pl.ds(pl.multiple_of(lax.rem(t, NPZ) * PW, 128), PW)] = h

        return carry

    lax.fori_loop(0, NP + LAGS[-1], step, 0)

    both = acc[:, 0:RANK] + acc[:, RANK : 2 * RANK]
    proj = both[0:GROUP] + both[GROUP : 2 * GROUP]
    base = 2 * GROUP
    gram = both[base : base + RANK] + both[base + RANK : base + 2 * RANK]
    gram8 = jnp.concatenate([gram[8 * q : 8 * q + 8] for q in range(4)], axis=1)
    for k in range(NY):
        rows = proj[k * ROWS : (k + 1) * ROWS]
        t0s[k, 0:8] = gram8
        t0s[k, 8:12] = jnp.concatenate([rows[4 * q : 4 * q + 4] for q in range(4)], axis=1)
    t0_copy = rcopy(t0s, t0r, t0_s, t0_r, partner)
    t0_copy.start()
    with jax.named_scope("t0wait"):
        t0_copy.wait_recv()
    t1s[...] = t0s[...] + t0r[...]

    me = y * 4 + lax.div(ml, 2)

    def t_copy(k):
        return rcopy(t1s.at[lax.div(k, 4)], t1r.at[me], t1_s.at[k], t1_r.at[k], plane_dev(k))

    t1_copies = [t_copy(k) for k in range(1, CHIPS)]
    for c in t1_copies:
        c.start()
    t1r[me] = t1s[0]
    with jax.named_scope("t1wait"):
        for c in t1_copies:
            c.wait_recv()
    sums = [t1r[k] for k in range(CHIPS)]
    while len(sums) > 1:
        sums = [a + b for a, b in zip(sums[::2], sums[1::2])]
    t3s[...] = sums[0]
    @pl.when(jnp.logical_not(seam))
    def _():
        pl.semaphore_wait(told, 1)

    t3_copy = rcopy(t3s, t3r, t3_s, t3_r, far)
    t3_copy.start()
    with jax.named_scope("t3wait"):
        t3_copy.wait_recv()
    total = sums[0] + t3r[...]
    gram_sum = jnp.concatenate([total[0:8, 32 * q : 32 * q + 32] for q in range(4)], axis=0)
    proj_sum = jnp.concatenate([total[8:12, 32 * q : 32 * q + 32] for q in range(4)], axis=0)
    f = f_ref[...]
    g_hi, g_lo = halves(gram_sum)
    own_hi, own_lo = halves(f)
    bottom = EPSILON + jnp.dot(
        jnp.concatenate([own_hi, own_hi, own_lo], axis=1),
        jnp.concatenate([g_hi, g_lo, g_hi], axis=0),
        preferred_element_type=F32,
    )
    w_ref[...] = f * proj_sum / bottom

    rcopy(fbuf, fbuf, f_s, f_r, y_dev(1)).wait_send()
    for c in t1_copies + [t0_copy, t3_copy]:
        c.wait_send()

    @pl.when(m < 15)
    def _():
        to_right.wait_send()

    @pl.when(m > 0)
    def _():
        to_left.wait_send()

    g_half.wait_send()
    h_part.wait_send()

    @pl.when(center)
    def _():
        part = hc.at[pl.ds(0, NZ // 2 - 1)]
        rcopy(part, part, hc_s, hc_s, (inner, m)).wait_send()

    for r in range(1, NY):
        rcopy(wg.at[:, r - 1], wg.at[:, r - 1], y_s.at[r - 1], y_s.at[r - 1], y_dev(r)).wait_send()
    rcopy(cout, cout, c_s, c_s, (inner, m)).wait_send()

    def h_sent(pieces):
        part = hbuf.at[pl.ds(0, pieces)]
        rcopy(part, part, h_s, h_s, (outer, m)).wait_send()

    @pl.when(center)
    def _():
        h_sent(NP)
        h_sent(2 * DIRECT)

    @pl.when(has_outer & jnp.logical_not(center))
    def _():
        h_sent(NP - DIRECT)


def body(spectra, shifts, fractions, pixel_factors, spectral_factors):
    vmem = pl.BlockSpec(memory_space=pltpu.VMEM)
    dma = pltpu.SemaphoreType.DMA
    return pl.pallas_call(
        kernel,
        out_shape=(
            pltpu.VMEM((ROWS, RANK), F32),
            pltpu.VMEM((RANK, OWN), F32),
        ),
        in_specs=[pl.BlockSpec(memory_space=pltpu.HBM)] * 5,
        out_specs=(vmem, vmem),
        scratch_shapes=[
            pltpu.VMEM((ROWS, SEGS), jnp.int32),
            pltpu.VMEM((ROWS, SEGS), F32),
            pltpu.VMEM((ROWS, RANK), F32),
            pltpu.VMEM((RANK, OWN), F32),
            pltpu.VMEM((ROWS, BINS + 256), F32),
            pltpu.VMEM((SEGS, ROWS, 128), jnp.int32),
            pltpu.VMEM((SEGS, ROWS, 128), F32),
            pltpu.VMEM((ROWS, BINS), F32),
            pltpu.VMEM((NP, NY - 1, ROWS, PW), F32),
            pltpu.VMEM((NP, 2 * GROUP, PW), BF16),
            pltpu.VMEM((2, NP, RANK, PW), F32),
            pltpu.VMEM((NP, RANK, PW), F32),
            pltpu.VMEM((NP, RANK, PW), F32),
            pltpu.VMEM((NZ, RANK, OWN), F32),
            pltpu.VMEM((NY - 1, ROWS, 128), F32),
            pltpu.VMEM((RANK, 3 * GROUP), BF16),
            pltpu.VMEM((RANK, RANK), F32),
            pltpu.VMEM((NZ // 2 + 1, RANK, RANK), F32),
            pltpu.VMEM((2 * GROUP + 2 * RANK, 2 * RANK), F32),
            pltpu.VMEM((ROWS, 128), F32),
            pltpu.VMEM((NY, 12, 128), F32),
            pltpu.VMEM((NY, 12, 128), F32),
            pltpu.VMEM((NY, 12, 128), F32),
            pltpu.VMEM((CHIPS, 12, 128), F32),
            pltpu.VMEM((12, 128), F32),
            pltpu.VMEM((12, 128), F32),
            dma((7,)),
            dma((2,)),
            dma((2,)),
            dma(()),
            dma(()),
            dma(()),
            dma((NZ,)),
            dma(()),
            dma((NZ // 2,)),
            dma((NY - 1,)),
            dma((NP,)),
            dma(()),
            dma((NP, SUB)),
            dma(()),
            dma((NP, SUB)),
            dma(()),
            dma(()),
            dma((CHIPS,)),
            dma((CHIPS,)),
            dma(()),
            dma(()),
            pltpu.SemaphoreType.REGULAR,
            pltpu.SemaphoreType.REGULAR,
            pltpu.SemaphoreType.REGULAR,
            pltpu.SemaphoreType.REGULAR,
        ],
        compiler_params=pltpu.CompilerParams(
            collective_id=0, has_side_effects=True, vmem_limit_bytes=66_000_000
        ),
    )(spectra, shifts, fractions, pixel_factors, spectral_factors)


def solution(mesh):
    return jax.shard_map(
        body,
        mesh=mesh,
        in_specs=(
            P("pix", "mz"),
            P("pix", "mz"),
            P("pix", "mz"),
            P("pix", None),
            P(None, ("mz", "pix")),
        ),
        out_specs=(P("pix", None), P(None, ("mz", "pix"))),
        check_vma=False,
    )
```

```python
import jax
import jax.numpy as jnp
from jax import lax
from jax.experimental import pallas as pl
from jax.experimental.pallas import tpu as pltpu
from jax.sharding import PartitionSpec as P

SEG = 2048
RANK = 32
EPSILON = 1e-06
ROWS = 16
BINS = 24576
SEGS = BINS // SEG
NZ, NY = 8, 4
OWN = 768
PW = 256
NPZ = OWN // PW
NP = NZ * NPZ
GROUP = NY * ROWS
LAGS = (5, 13, 21, 24)
LATE = 2
LATE_FAR = (5, 8, 12, 17)
SEND_FAR = (-1, 0, 0, 2)
SUB = 2
SUB_ROWS = RANK // SUB
DIRECT = 2
CHUNK = 1024
GROUP_BINS = NY * OWN
EARLY = 6
LATE_CHUNKS = (NZ - EARLY) * (GROUP_BINS // CHUNK)
CHIPS = 16
MESH = pl.DeviceIdType.MESH
F32 = jnp.float32
BF16 = jnp.bfloat16
exact_mode = lax.Precision.HIGHEST
NT = (((1,), (1,)), ((), ()))


def halves(v):
    hi = v.astype(BF16)
    return hi, (v - hi.astype(F32)).astype(BF16)


def kernel(
    x_hbm, sh_hbm, fr_hbm, f_hbm, hin_hbm, w_ref, hout_ref,
    sh_ref, fr_ref, f_ref, hin_ref,
    xp, shb, frb, ws, wg, wgb, cbuf, cout, hbuf, hc, fbuf, lhs, gsend, gbuf, acc,
    f_all, t0s, t0r, t1s, t1r, t3s, t3r,
    xsem, halo_s, halo_r, f_s, f_r, hc_s, hc_r, g_s, g_r,
    y_s, y_r, c_s, c_r, h_s, x_r, t0_s, t0_r, t1_s, t1_r, t3_s, t3_r,
    seen, seen_edge, told, told_edge,
):
    p, m = lax.axis_index("pix"), lax.axis_index("mz")
    z, y = lax.div(p, NY), lax.rem(p, NY)
    mh, ml = lax.div(m, 8), lax.rem(m, 8)
    low_side = z < NZ // 2
    inner = jnp.where(low_side, p + NY, p - NY)
    outer = jnp.where(low_side, p - NY, p + NY)
    depth = jnp.where(low_side, NZ // 2 - 1 - z, z - NZ // 2)
    center = depth == 0
    has_outer = depth < NZ // 2 - 1

    def by_depth(values):
        a, b, c, d = values
        return jnp.where(depth == 0, a, jnp.where(depth == 1, b, jnp.where(depth == 2, c, d)))

    lag = by_depth(LAGS)
    seam = ((mh == 0) & (z == NZ - 1)) | ((mh == 1) & (z == 0))
    across = (m == 7) | (m == 8)
    seam_pix = jnp.where(mh == 0, y, (NZ - 1) * NY + y)
    seam_dev = (seam_pix, lax.rem(m + 8, 16))
    seam_edge = (seam_pix, jnp.where(mh == 0, 8, 7))

    def y_dev(r):
        return (z * NY + lax.rem(y + r, NY), m)

    def m_dev(r):
        return (p, mh * 8 + lax.rem(ml + r, 8))

    far = (p, lax.rem(m + 8, 16))

    def rcopy(src, dst, send, recv, dev):
        return pltpu.make_async_remote_copy(
            src_ref=src, dst_ref=dst, send_sem=send, recv_sem=recv, device_id=dev, device_id_type=MESH
        )

    small = [
        pltpu.make_async_copy(a, b, xsem.at[k])
        for k, (a, b) in enumerate(
            ((sh_hbm, sh_ref), (fr_hbm, fr_ref), (f_hbm, f_ref), (hin_hbm, hin_ref))
        )
    ]
    lo, hi = 3 * GROUP_BINS - 128, 4 * GROUP_BINS + 128
    parts = [
        pltpu.make_async_copy(
            x_hbm.at[:, pl.ds(a, b - a)], xp.at[:, pl.ds(128 + a, b - a)], xsem.at[4 + k]
        )
        for k, (a, b) in enumerate(((lo, hi), (hi, BINS), (0, lo)))
    ]
    for c in small[:2] + parts + small[2:]:
        c.start()

    barrier = pltpu.get_barrier_semaphore()

    def greet(dev):
        pl.semaphore_signal(barrier, inc=1, device_id=dev, device_id_type=MESH)

    core = lax.rem(ml, 2)
    partner = (p, m + 1 - 2 * core)

    def plane_dev(k):
        return (
            z * NY + lax.rem(y + lax.div(k, 4), NY),
            mh * 8 + lax.rem(ml + 2 * lax.rem(k, 4), 8),
        )

    for k in range(1, CHIPS):
        greet(plane_dev(k))
    greet(partner)

    def column_dev(k):
        return (lax.rem(z + k, NZ) * NY + y, m)

    for k in range(1, NZ):
        greet(column_dev(k))

    @pl.when((core == 0) & (ml > 0))
    def _():
        greet((p, m - 1))

    @pl.when((core == 1) & (ml < 7))
    def _():
        greet((p, m + 1))

    @pl.when(seam)
    def _():
        greet(seam_dev)

    @pl.when(seam & across)
    def _():
        greet(seam_edge)

    acc[...] = jnp.zeros_like(acc)

    @pl.when(m == 0)
    def _():
        xp[:, 0:128] = jnp.zeros((ROWS, 128), F32)

    @pl.when(m == 15)
    def _():
        xp[:, 128 + BINS :] = jnp.zeros((ROWS, 128), F32)

    small[0].wait()
    small[1].wait()
    for s in range(SEGS):
        shb[s] = jnp.broadcast_to(sh_ref[:, s : s + 1], (ROWS, 128))
        frb[s] = jnp.broadcast_to(fr_ref[:, s : s + 1], (ROWS, 128))

    def group_z(g):
        step = lax.div(g, 2)
        flip = jnp.where((m == 8) & (g >= EARLY), 1, 0)
        return jnp.where(lax.rem(g, 2) == flip, NZ // 2 - 1 - step, NZ // 2 + step)

    def piece(i):
        return group_z(lax.div(i, NPZ)) * NPZ + lax.rem(i, NPZ)

    def own_bins(t):
        return first_bin(0, t)

    def first_bin(r, t):
        zq, j = lax.div(t, NPZ), lax.rem(t, NPZ)
        return pl.multiple_of(zq * GROUP_BINS + lax.rem(y + r, NY) * OWN + j * PW, 128)

    def warp(c):
        width = CHUNK + 256
        b = pl.multiple_of(c * CHUNK, 128)
        seg = lax.div(b, SEG)
        d, f = shb[seg], frb[seg]

        def wide(v, lanes):
            return jnp.concatenate([v] * (lanes // 128), axis=1)

        v = xp[:, pl.ds(b, width)]
        v = jnp.where(wide(d, width) < 0, pltpu.roll(v, 4, 1), v)
        shifted = [v] + [pltpu.roll(v, width - k, 1) for k in range(1, 5)]
        shifted = [u[:, 128 : 128 + CHUNK] for u in shifted]
        rest = wide(d & 3, CHUNK)
        high, odd = rest >= 2, (rest & 1) != 0

        def pick(k):
            return jnp.where(
                high,
                jnp.where(odd, shifted[k + 3], shifted[k + 2]),
                jnp.where(odd, shifted[k + 1], shifted[k]),
            )

        f = wide(f, CHUNK)
        ws[:, pl.ds(b, CHUNK)] = (1.0 - f) * pick(0) + f * pick(1)

    def warp_group(g):
        zq = group_z(g)

        for k in range(GROUP_BINS // CHUNK):
            warp(zq * (GROUP_BINS // CHUNK) + k)

    def y_copy(r, t):
        src = ws.at[:, pl.ds(first_bin(r, t), PW)]
        return rcopy(src, wg.at[t, NY - r - 1], y_s.at[r - 1], y_r.at[t], y_dev(r))

    def send_group(g):
        zq = group_z(g)
        for j in range(NPZ):
            for r in range(1, NY):
                y_copy(r, zq * NPZ + j).start()

    parts[0].wait()
    with jax.named_scope("warps"):
        warp_group(0)
    small[2].wait()
    f_all[...] = jnp.concatenate([f_ref[...], jnp.zeros((ROWS, 128 - RANK), F32)], axis=1)
    with jax.named_scope("barrier"):
        pl.semaphore_wait(
            barrier,
            CHIPS
            + NZ
            - 1
            + jnp.where((ml == 0) | (ml == 7), 0, 1)
            + jnp.where(seam, 1, 0)
            + jnp.where(seam & across, 1, 0),
        )

    def signal(sem, dev):
        pl.semaphore_signal(sem, inc=1, device_id=dev, device_id_type=MESH)

    @pl.when(seam)
    def _():
        signal(seen, seam_dev)

    @pl.when(seam & across)
    def _():
        signal(seen_edge, seam_edge)

    f_copies = [
        rcopy(f_all, fbuf.at[NY - r - 1], f_s, f_r, y_dev(r)) for r in range(1, NY)
    ]
    for c in f_copies:
        c.start()
    send_group(0)
    parts[1].wait()
    parts[2].wait()
    small[3].wait()

    to_right = rcopy(
        xp.at[:, pl.ds(BINS, 128)], xp.at[:, pl.ds(0, 128)], halo_s.at[0], halo_r.at[0], (p, m + 1)
    )
    to_left = rcopy(
        xp.at[:, pl.ds(128, 128)], xp.at[:, pl.ds(128 + BINS, 128)], halo_s.at[1], halo_r.at[1], (p, m - 1)
    )

    @pl.when((m < 15) & (m != 7))
    def _():
        to_right.start()

    @pl.when((m > 0) & (m != 8))
    def _():
        to_left.start()

    def send_far():
        @pl.when(m == 7)
        def _():
            to_right.start()

        @pl.when(m == 8)
        def _():
            to_left.start()

    @pl.when(seam & across)
    def _():
        pl.semaphore_wait(seen_edge, 1)
        send_far()
        for k in range(1, NZ):
            signal(told_edge, column_dev(k))

    def send_far_told():
        pl.semaphore_wait(told_edge, 1)
        send_far()

    near = jnp.where(low_side, NZ // 2 - 1, NZ // 2)

    h_part = rcopy(hin_ref, hc.at[z], hc_s, hc_r.at[z], (jnp.where(center, inner, near * NY + y), m))

    def h_relay(zk):
        return rcopy(hc.at[zk], hc.at[zk], hc_s, hc_r.at[zk], (inner, m))

    @pl.when(depth <= 1)
    def _():
        h_part.start()

    @pl.when(center)
    def _():
        hc[z] = hin_ref[...]

    def early(g, carry):
        warp_group(g)
        send_group(g)

        @pl.when(((g == 1) & (depth == 2)) | ((g == 2) & (depth == 3)))
        def _():
            h_part.start()

        return carry

    with jax.named_scope("warps"):
        lax.fori_loop(1, EARLY, early, 0)

    with jax.named_scope("fwait"):
        rcopy(fbuf, fbuf, f_s, f_r, y_dev(1)).wait_recv()

    @pl.when(seam)
    def _():
        pl.semaphore_wait(seen, 1)
        for k in range(1, NZ):
            signal(told, column_dev(k))

    fg = jnp.concatenate([f_all[...], fbuf[...].reshape(GROUP - ROWS, 128)], axis=0)[:, 0:RANK]
    gy = lax.dot_general(fg, fg, (((0,), (0,)), ((), ())), precision=exact_mode, preferred_element_type=F32)
    f_hi, f_lo = halves(fg.T)
    lhs[...] = jnp.concatenate([f_hi, f_hi, f_lo], axis=1)

    g_half = rcopy(gsend, gbuf.at[depth], g_s, g_r.at[depth], (near * NY + y, m))
    g_other = rcopy(gsend, gbuf.at[0], g_s, g_r.at[0], (inner, m))

    def outward(k):
        return jnp.where(low_side, NZ // 2 - 1 - k, NZ // 2 + k)

    def warp_late(e):
        chunks = GROUP_BINS // CHUNK
        g = EARLY + lax.div(e, chunks)
        k = lax.rem(e, chunks)
        left, right = jnp.where(m == 8, LATE_CHUNKS - 1, 0), jnp.where(m == 8, 0, LATE_CHUNKS - 1)

        @pl.when((e == left) & (m > 0))
        def _():
            to_right.wait_recv()

        @pl.when((e == right) & (m < 15))
        def _():
            to_left.wait_recv()

        warp(group_z(g) * chunks + jnp.where(m == 8, chunks - 1 - k, k))

        @pl.when(lax.rem(e, chunks) == chunks - 1)
        def _():
            send_group(g)

    @pl.when(jnp.logical_not(center))
    def _():
        gsend[...] = gy
        g_half.start()

    def relay(k):
        h_relay(outward(k)).wait_recv()
        h_relay(outward(k)).start()

    @pl.when(center)
    def _():
        @pl.when(across)
        def _():
            send_far_told()

        with jax.named_scope("relay"):
            relay(1)
            relay(2)
            total = gy
            for k in range(1, NZ // 2):
                rcopy(gsend, gbuf.at[k], g_s, g_r.at[k], (inner, m)).wait_recv()
                total = total + gbuf[k]
            gsend[...] = total
            gbuf[NZ // 2] = total
            g_other.start()
            relay(3)

        def late(e, carry):
            warp_late(e)
            return carry

        lax.fori_loop(0, LATE_CHUNKS - 1, late, 0)

        @pl.when(jnp.logical_not(across))
        def _():
            warp_late(LATE_CHUNKS - 1)

    late_from = jnp.where(center, -LATE_CHUNKS, LATE)
    late_far = jnp.where(across, by_depth(LATE_FAR), -1)
    late_near = LATE_CHUNKS - jnp.where(across, 1, 0)
    send_far_step = jnp.where(across & jnp.logical_not(seam), by_depth(SEND_FAR), -1)

    def rows_of(q):
        return pl.ds(q * SUB_ROWS, SUB_ROWS)

    def c_copy(t, q):
        dst = cbuf.at[0, t, rows_of(q)]
        return rcopy(cout.at[t, rows_of(q)], dst, c_s, c_r.at[t, q], (inner, m))

    def cx_copy(t, q):
        dst = cbuf.at[1, t, rows_of(q)]
        return rcopy(cout.at[t, rows_of(q)], dst, c_s, x_r.at[t, q], (inner, m))

    def c_send(t, q):
        @pl.when(center)
        def _():
            cx_copy(t, q).start()

        @pl.when(jnp.logical_not(center))
        def _():
            c_copy(t, q).start()

    def h_copy(t, q, dev):
        part = hbuf.at[t, rows_of(q)]
        return rcopy(part, part, h_s, x_r.at[t, q], dev)

    def step(i, carry):
        @pl.when(i < NP)
        def _():
            t = piece(i)
            with jax.named_scope("ywait"):
                rcopy(wg.at[t], wg.at[t], y_s.at[0], y_r.at[t], y_dev(1)).wait_recv()
            mine = ws[:, pl.ds(own_bins(t), PW)]
            w_hi, w_lo = halves(jnp.concatenate([mine, wg[t].reshape(GROUP - ROWS, PW)], axis=0))
            both = jnp.concatenate([w_hi, w_lo], axis=0)
            wgb[t] = both
            n = jnp.dot(lhs[...], jnp.concatenate([both, w_hi], axis=0), preferred_element_type=F32)

            @pl.when(i == send_far_step)
            def _():
                send_far_told()

            @pl.when(has_outer)
            def _():
                for q in range(SUB):
                    with jax.named_scope("cwait"):
                        c_copy(t, q).wait_recv()
                    part = n[q * SUB_ROWS : (q + 1) * SUB_ROWS]
                    cout[t, rows_of(q)] = part + cbuf[0, t, rows_of(q)]
                    c_send(t, q)

            @pl.when(jnp.logical_not(has_outer))
            def _():
                cout[t] = n
                for q in range(SUB):
                    c_send(t, q)

            late = i - late_from

            @pl.when(((late >= 0) & (late < late_near)) | (i == late_far))
            def _():
                warp_late(jnp.where(i == late_far, LATE_CHUNKS - 1, late))

        k = i - lag

        @pl.when((k >= 0) & (k < NP))
        def _():
            t = piece(k)

            @pl.when(center)
            def _():
                zq, j = lax.div(t, NPZ), lax.rem(t, NPZ)

                @pl.when(k == 0)
                def _():
                    g_other.wait_recv()
                    gbuf[NZ // 2] = gbuf[NZ // 2] + gbuf[0]

                @pl.when((j == 0) & (lax.div(zq, NZ // 2) != lax.div(z, NZ // 2)))
                def _():
                    with jax.named_scope("hcwait"):
                        h_relay(zq).wait_recv()

                own = hc[zq, :, pl.ds(pl.multiple_of(j * PW, 128), PW)]
                bottom = jnp.dot(gbuf[NZ // 2], own, precision=exact_mode, preferred_element_type=F32) + EPSILON
                ratio = own / bottom
                for q in range(SUB):
                    with jax.named_scope("xcwait"):
                        cx_copy(t, q).wait_recv()
                    r = rows_of(q)
                    hbuf[t, r] = ratio[q * SUB_ROWS : (q + 1) * SUB_ROWS] * (cout[t, r] + cbuf[1, t, r])

                    @pl.when(k >= NP - DIRECT)
                    def _():
                        for far_out in (3, 2):
                            h_copy(t, q, (outward(far_out) * NY + y, m)).start()

                    h_copy(t, q, (outer, m)).start()

            @pl.when(jnp.logical_not(center))
            def _():
                for q in range(SUB):
                    with jax.named_scope("hwait"):
                        h_copy(t, q, (outer, m)).wait_recv()

                    @pl.when(has_outer & (k < NP - DIRECT))
                    def _():
                        h_copy(t, q, (outer, m)).start()

            h = hbuf[t]
            h_hi, h_lo = halves(h)
            right = jnp.concatenate([h_hi, h_lo], axis=0)
            left = jnp.concatenate([wgb[t], right], axis=0)
            acc[...] += lax.dot_general(left, right, NT, preferred_element_type=F32)

            @pl.when(lax.div(t, NPZ) == z)
            def _():
                hout_ref[:, pl.ds(pl.multiple_of(lax.rem(t, NPZ) * PW, 128), PW)] = h

        return carry

    lax.fori_loop(0, NP + LAGS[-1], step, 0)

    both = acc[:, 0:RANK] + acc[:, RANK : 2 * RANK]
    proj = both[0:GROUP] + both[GROUP : 2 * GROUP]
    base = 2 * GROUP
    gram = both[base : base + RANK] + both[base + RANK : base + 2 * RANK]
    gram8 = jnp.concatenate([gram[8 * q : 8 * q + 8] for q in range(4)], axis=1)
    for k in range(NY):
        rows = proj[k * ROWS : (k + 1) * ROWS]
        t0s[k, 0:8] = gram8
        t0s[k, 8:12] = jnp.concatenate([rows[4 * q : 4 * q + 4] for q in range(4)], axis=1)
    t0_copy = rcopy(t0s, t0r, t0_s, t0_r, partner)
    t0_copy.start()
    with jax.named_scope("t0wait"):
        t0_copy.wait_recv()
    t1s[...] = t0s[...] + t0r[...]

    me = y * 4 + lax.div(ml, 2)

    def t_copy(k):
        return rcopy(t1s.at[lax.div(k, 4)], t1r.at[me], t1_s.at[k], t1_r.at[k], plane_dev(k))

    t1_copies = [t_copy(k) for k in range(1, CHIPS)]
    for c in t1_copies:
        c.start()
    t1r[me] = t1s[0]
    with jax.named_scope("t1wait"):
        for c in t1_copies:
            c.wait_recv()
    sums = [t1r[k] for k in range(CHIPS)]
    while len(sums) > 1:
        sums = [a + b for a, b in zip(sums[::2], sums[1::2])]
    t3s[...] = sums[0]
    @pl.when(jnp.logical_not(seam))
    def _():
        pl.semaphore_wait(told, 1)

    t3_copy = rcopy(t3s, t3r, t3_s, t3_r, far)
    t3_copy.start()
    with jax.named_scope("t3wait"):
        t3_copy.wait_recv()
    total = sums[0] + t3r[...]
    gram_sum = jnp.concatenate([total[0:8, 32 * q : 32 * q + 32] for q in range(4)], axis=0)
    proj_sum = jnp.concatenate([total[8:12, 32 * q : 32 * q + 32] for q in range(4)], axis=0)
    f = f_ref[...]
    g_hi, g_lo = halves(gram_sum)
    own_hi, own_lo = halves(f)
    bottom = EPSILON + jnp.dot(
        jnp.concatenate([own_hi, own_hi, own_lo], axis=1),
        jnp.concatenate([g_hi, g_lo, g_hi], axis=0),
        preferred_element_type=F32,
    )
    w_ref[...] = f * proj_sum / bottom

    rcopy(fbuf, fbuf, f_s, f_r, y_dev(1)).wait_send()
    for c in t1_copies + [t0_copy, t3_copy]:
        c.wait_send()

    @pl.when(m < 15)
    def _():
        to_right.wait_send()

    @pl.when(m > 0)
    def _():
        to_left.wait_send()

    g_half.wait_send()
    h_part.wait_send()

    @pl.when(center)
    def _():
        part = hc.at[pl.ds(0, NZ // 2 - 1)]
        rcopy(part, part, hc_s, hc_s, (inner, m)).wait_send()

    for r in range(1, NY):
        rcopy(wg.at[:, r - 1], wg.at[:, r - 1], y_s.at[r - 1], y_s.at[r - 1], y_dev(r)).wait_send()
    rcopy(cout, cout, c_s, c_s, (inner, m)).wait_send()

    def h_sent(pieces):
        part = hbuf.at[pl.ds(0, pieces)]
        rcopy(part, part, h_s, h_s, (outer, m)).wait_send()

    @pl.when(center)
    def _():
        h_sent(NP)
        h_sent(2 * DIRECT)

    @pl.when(has_outer & jnp.logical_not(center))
    def _():
        h_sent(NP - DIRECT)


def body(spectra, shifts, fractions, pixel_factors, spectral_factors):
    vmem = pl.BlockSpec(memory_space=pltpu.VMEM)
    dma = pltpu.SemaphoreType.DMA
    return pl.pallas_call(
        kernel,
        out_shape=(
            pltpu.VMEM((ROWS, RANK), F32),
            pltpu.VMEM((RANK, OWN), F32),
        ),
        in_specs=[pl.BlockSpec(memory_space=pltpu.HBM)] * 5,
        out_specs=(vmem, vmem),
        scratch_shapes=[
            pltpu.VMEM((ROWS, SEGS), jnp.int32),
            pltpu.VMEM((ROWS, SEGS), F32),
            pltpu.VMEM((ROWS, RANK), F32),
            pltpu.VMEM((RANK, OWN), F32),
            pltpu.VMEM((ROWS, BINS + 256), F32),
            pltpu.VMEM((SEGS, ROWS, 128), jnp.int32),
            pltpu.VMEM((SEGS, ROWS, 128), F32),
            pltpu.VMEM((ROWS, BINS), F32),
            pltpu.VMEM((NP, NY - 1, ROWS, PW), F32),
            pltpu.VMEM((NP, 2 * GROUP, PW), BF16),
            pltpu.VMEM((2, NP, RANK, PW), F32),
            pltpu.VMEM((NP, RANK, PW), F32),
            pltpu.VMEM((NP, RANK, PW), F32),
            pltpu.VMEM((NZ, RANK, OWN), F32),
            pltpu.VMEM((NY - 1, ROWS, 128), F32),
            pltpu.VMEM((RANK, 3 * GROUP), BF16),
            pltpu.VMEM((RANK, RANK), F32),
            pltpu.VMEM((NZ // 2 + 1, RANK, RANK), F32),
            pltpu.VMEM((2 * GROUP + 2 * RANK, 2 * RANK), F32),
            pltpu.VMEM((ROWS, 128), F32),
            pltpu.VMEM((NY, 12, 128), F32),
            pltpu.VMEM((NY, 12, 128), F32),
            pltpu.VMEM((NY, 12, 128), F32),
            pltpu.VMEM((CHIPS, 12, 128), F32),
            pltpu.VMEM((12, 128), F32),
            pltpu.VMEM((12, 128), F32),
            dma((7,)),
            dma((2,)),
            dma((2,)),
            dma(()),
            dma(()),
            dma(()),
            dma((NZ,)),
            dma(()),
            dma((NZ // 2,)),
            dma((NY - 1,)),
            dma((NP,)),
            dma(()),
            dma((NP, SUB)),
            dma(()),
            dma((NP, SUB)),
            dma(()),
            dma(()),
            dma((CHIPS,)),
            dma((CHIPS,)),
            dma(()),
            dma(()),
            pltpu.SemaphoreType.REGULAR,
            pltpu.SemaphoreType.REGULAR,
            pltpu.SemaphoreType.REGULAR,
            pltpu.SemaphoreType.REGULAR,
        ],
        compiler_params=pltpu.CompilerParams(
            collective_id=0, has_side_effects=True, vmem_limit_bytes=66_000_000
        ),
    )(spectra, shifts, fractions, pixel_factors, spectral_factors)


def solution(mesh):
    return jax.shard_map(
        body,
        mesh=mesh,
        in_specs=(
            P("pix", "mz"),
            P("pix", "mz"),
            P("pix", "mz"),
            P("pix", None),
            P(None, ("mz", "pix")),
        ),
        out_specs=(P("pix", None), P(None, ("mz", "pix"))),
        check_vma=False,
    )
```

```python
import jax
import jax.numpy as jnp
from jax import lax
from jax.experimental import pallas as pl
from jax.experimental.pallas import tpu as pltpu
from jax.sharding import PartitionSpec as P

SEG = 2048
RANK = 32
EPSILON = 1e-06
ROWS = 16
BINS = 24576
SEGS = BINS // SEG
NZ, NY = 8, 4
OWN = 768
PW = 256
NPZ = OWN // PW
NP = NZ * NPZ
GROUP = NY * ROWS
LAGS = (5, 13, 21, 24)
LATE = 2
LATE_FAR = (8, 12, 16, 20)
SEND_FAR = (-1, 0, 2, 6)
SUB = 2
SUB_ROWS = RANK // SUB
DIRECT = 2
CHUNK = 1024
GROUP_BINS = NY * OWN
EARLY = 6
LATE_CHUNKS = (NZ - EARLY) * (GROUP_BINS // CHUNK)
CHIPS = 16
MESH = pl.DeviceIdType.MESH
F32 = jnp.float32
BF16 = jnp.bfloat16
exact_mode = lax.Precision.HIGHEST
NT = (((1,), (1,)), ((), ()))


def halves(v):
    hi = v.astype(BF16)
    return hi, (v - hi.astype(F32)).astype(BF16)


def kernel(
    x_hbm, sh_hbm, fr_hbm, f_hbm, hin_hbm, w_ref, hout_ref,
    sh_ref, fr_ref, f_ref, hin_ref,
    xp, shb, frb, ws, wg, wgb, cbuf, cout, hbuf, hc, fbuf, lhs, gsend, gbuf, acc,
    f_all, t0s, t0r, t1s, t1r, t3s, t3r,
    xsem, halo_s, halo_r, f_s, f_r, hc_s, hc_r, g_s, g_r,
    y_s, y_r, c_s, c_r, h_s, x_r, t0_s, t0_r, t1_s, t1_r, t3_s, t3_r,
    seen, seen_edge, told, told_edge,
):
    p, m = lax.axis_index("pix"), lax.axis_index("mz")
    z, y = lax.div(p, NY), lax.rem(p, NY)
    mh, ml = lax.div(m, 8), lax.rem(m, 8)
    low_side = z < NZ // 2
    inner = jnp.where(low_side, p + NY, p - NY)
    outer = jnp.where(low_side, p - NY, p + NY)
    depth = jnp.where(low_side, NZ // 2 - 1 - z, z - NZ // 2)
    center = depth == 0
    has_outer = depth < NZ // 2 - 1

    def by_depth(values):
        a, b, c, d = values
        return jnp.where(depth == 0, a, jnp.where(depth == 1, b, jnp.where(depth == 2, c, d)))

    lag = by_depth(LAGS)
    seam = ((mh == 0) & (z == NZ - 1)) | ((mh == 1) & (z == 0))
    across = (m == 7) | (m == 8)
    seam_pix = jnp.where(mh == 0, y, (NZ - 1) * NY + y)
    seam_dev = (seam_pix, lax.rem(m + 8, 16))
    seam_edge = (seam_pix, jnp.where(mh == 0, 8, 7))

    def y_dev(r):
        return (z * NY + lax.rem(y + r, NY), m)

    def m_dev(r):
        return (p, mh * 8 + lax.rem(ml + r, 8))

    far = (p, lax.rem(m + 8, 16))

    def rcopy(src, dst, send, recv, dev):
        return pltpu.make_async_remote_copy(
            src_ref=src, dst_ref=dst, send_sem=send, recv_sem=recv, device_id=dev, device_id_type=MESH
        )

    small = [
        pltpu.make_async_copy(a, b, xsem.at[k])
        for k, (a, b) in enumerate(
            ((sh_hbm, sh_ref), (fr_hbm, fr_ref), (f_hbm, f_ref), (hin_hbm, hin_ref))
        )
    ]
    lo, hi = 3 * GROUP_BINS - 128, 4 * GROUP_BINS + 128
    parts = [
        pltpu.make_async_copy(
            x_hbm.at[:, pl.ds(a, b - a)], xp.at[:, pl.ds(128 + a, b - a)], xsem.at[4 + k]
        )
        for k, (a, b) in enumerate(((lo, hi), (hi, BINS), (0, lo)))
    ]
    for c in small[:2] + parts + small[2:]:
        c.start()

    barrier = pltpu.get_barrier_semaphore()

    def greet(dev):
        pl.semaphore_signal(barrier, inc=1, device_id=dev, device_id_type=MESH)

    core = lax.rem(ml, 2)
    partner = (p, m + 1 - 2 * core)

    def plane_dev(k):
        return (
            z * NY + lax.rem(y + lax.div(k, 4), NY),
            mh * 8 + lax.rem(ml + 2 * lax.rem(k, 4), 8),
        )

    for k in range(1, CHIPS):
        greet(plane_dev(k))
    greet(partner)

    def column_dev(k):
        return (lax.rem(z + k, NZ) * NY + y, m)

    for k in range(1, NZ):
        greet(column_dev(k))

    @pl.when((core == 0) & (ml > 0))
    def _():
        greet((p, m - 1))

    @pl.when((core == 1) & (ml < 7))
    def _():
        greet((p, m + 1))

    @pl.when(seam)
    def _():
        greet(seam_dev)

    @pl.when(seam & across)
    def _():
        greet(seam_edge)

    acc[...] = jnp.zeros_like(acc)

    @pl.when(m == 0)
    def _():
        xp[:, 0:128] = jnp.zeros((ROWS, 128), F32)

    @pl.when(m == 15)
    def _():
        xp[:, 128 + BINS :] = jnp.zeros((ROWS, 128), F32)

    small[0].wait()
    small[1].wait()
    for s in range(SEGS):
        shb[s] = jnp.broadcast_to(sh_ref[:, s : s + 1], (ROWS, 128))
        frb[s] = jnp.broadcast_to(fr_ref[:, s : s + 1], (ROWS, 128))

    def group_z(g):
        step = lax.div(g, 2)
        flip = jnp.where((m == 8) & (g >= EARLY), 1, 0)
        return jnp.where(lax.rem(g, 2) == flip, NZ // 2 - 1 - step, NZ // 2 + step)

    def piece(i):
        return group_z(lax.div(i, NPZ)) * NPZ + lax.rem(i, NPZ)

    def own_bins(t):
        return first_bin(0, t)

    def first_bin(r, t):
        zq, j = lax.div(t, NPZ), lax.rem(t, NPZ)
        return pl.multiple_of(zq * GROUP_BINS + lax.rem(y + r, NY) * OWN + j * PW, 128)

    def warp(c):
        width = CHUNK + 256
        b = pl.multiple_of(c * CHUNK, 128)
        seg = lax.div(b, SEG)
        d, f = shb[seg], frb[seg]

        def wide(v, lanes):
            return jnp.concatenate([v] * (lanes // 128), axis=1)

        v = xp[:, pl.ds(b, width)]
        v = jnp.where(wide(d, width) < 0, pltpu.roll(v, 4, 1), v)
        shifted = [v] + [pltpu.roll(v, width - k, 1) for k in range(1, 5)]
        shifted = [u[:, 128 : 128 + CHUNK] for u in shifted]
        rest = wide(d & 3, CHUNK)
        high, odd = rest >= 2, (rest & 1) != 0

        def pick(k):
            return jnp.where(
                high,
                jnp.where(odd, shifted[k + 3], shifted[k + 2]),
                jnp.where(odd, shifted[k + 1], shifted[k]),
            )

        f = wide(f, CHUNK)
        ws[:, pl.ds(b, CHUNK)] = (1.0 - f) * pick(0) + f * pick(1)

    def warp_group(g):
        zq = group_z(g)

        for k in range(GROUP_BINS // CHUNK):
            warp(zq * (GROUP_BINS // CHUNK) + k)

    def y_copy(r, t):
        src = ws.at[:, pl.ds(first_bin(r, t), PW)]
        return rcopy(src, wg.at[t, NY - r - 1], y_s.at[r - 1], y_r.at[t], y_dev(r))

    def send_group(g):
        zq = group_z(g)
        for j in range(NPZ):
            for r in range(1, NY):
                y_copy(r, zq * NPZ + j).start()

    parts[0].wait()
    with jax.named_scope("warps"):
        warp_group(0)
    small[2].wait()
    f_all[...] = jnp.concatenate([f_ref[...], jnp.zeros((ROWS, 128 - RANK), F32)], axis=1)
    with jax.named_scope("barrier"):
        pl.semaphore_wait(
            barrier,
            CHIPS
            + NZ
            - 1
            + jnp.where((ml == 0) | (ml == 7), 0, 1)
            + jnp.where(seam, 1, 0)
            + jnp.where(seam & across, 1, 0),
        )

    def signal(sem, dev):
        pl.semaphore_signal(sem, inc=1, device_id=dev, device_id_type=MESH)

    @pl.when(seam)
    def _():
        signal(seen, seam_dev)

    @pl.when(seam & across)
    def _():
        signal(seen_edge, seam_edge)

    f_copies = [
        rcopy(f_all, fbuf.at[NY - r - 1], f_s, f_r, y_dev(r)) for r in range(1, NY)
    ]
    for c in f_copies:
        c.start()
    send_group(0)
    parts[1].wait()
    parts[2].wait()
    small[3].wait()

    to_right = rcopy(
        xp.at[:, pl.ds(BINS, 128)], xp.at[:, pl.ds(0, 128)], halo_s.at[0], halo_r.at[0], (p, m + 1)
    )
    to_left = rcopy(
        xp.at[:, pl.ds(128, 128)], xp.at[:, pl.ds(128 + BINS, 128)], halo_s.at[1], halo_r.at[1], (p, m - 1)
    )

    @pl.when((m < 15) & (m != 7))
    def _():
        to_right.start()

    @pl.when((m > 0) & (m != 8))
    def _():
        to_left.start()

    def send_far():
        @pl.when(m == 7)
        def _():
            to_right.start()

        @pl.when(m == 8)
        def _():
            to_left.start()

    near = jnp.where(low_side, NZ // 2 - 1, NZ // 2)

    h_part = rcopy(hin_ref, hc.at[z], hc_s, hc_r.at[z], (jnp.where(center, inner, near * NY + y), m))

    def h_relay(zk):
        return rcopy(hc.at[zk], hc.at[zk], hc_s, hc_r.at[zk], (inner, m))

    @pl.when(depth <= 1)
    def _():
        h_part.start()

    @pl.when(center)
    def _():
        hc[z] = hin_ref[...]

    def early(g, carry):
        warp_group(g)
        send_group(g)

        @pl.when(((g == 1) & (depth == 2)) | ((g == 2) & (depth == 3)))
        def _():
            h_part.start()

        return carry

    with jax.named_scope("warps"):
        lax.fori_loop(1, EARLY, early, 0)

    with jax.named_scope("fwait"):
        rcopy(fbuf, fbuf, f_s, f_r, y_dev(1)).wait_recv()

    @pl.when(seam)
    def _():
        pl.semaphore_wait(seen, 1)
        for k in range(1, NZ):
            signal(told, column_dev(k))

    @pl.when(seam & across)
    def _():
        pl.semaphore_wait(seen_edge, 1)
        send_far()
        for k in range(1, NZ):
            signal(told_edge, column_dev(k))

    def send_far_told():
        pl.semaphore_wait(told_edge, 1)
        send_far()

    fg = jnp.concatenate([f_all[...], fbuf[...].reshape(GROUP - ROWS, 128)], axis=0)[:, 0:RANK]
    gy = lax.dot_general(fg, fg, (((0,), (0,)), ((), ())), precision=exact_mode, preferred_element_type=F32)
    f_hi, f_lo = halves(fg.T)
    lhs[...] = jnp.concatenate([f_hi, f_hi, f_lo], axis=1)

    g_half = rcopy(gsend, gbuf.at[depth], g_s, g_r.at[depth], (near * NY + y, m))
    g_other = rcopy(gsend, gbuf.at[0], g_s, g_r.at[0], (inner, m))

    def outward(k):
        return jnp.where(low_side, NZ // 2 - 1 - k, NZ // 2 + k)

    def warp_late(e):
        chunks = GROUP_BINS // CHUNK
        g = EARLY + lax.div(e, chunks)
        k = lax.rem(e, chunks)
        left, right = jnp.where(m == 8, LATE_CHUNKS - 1, 0), jnp.where(m == 8, 0, LATE_CHUNKS - 1)

        @pl.when((e == left) & (m > 0))
        def _():
            to_right.wait_recv()

        @pl.when((e == right) & (m < 15))
        def _():
            to_left.wait_recv()

        warp(group_z(g) * chunks + jnp.where(m == 8, chunks - 1 - k, k))

        @pl.when(lax.rem(e, chunks) == chunks - 1)
        def _():
            send_group(g)

    @pl.when(jnp.logical_not(center))
    def _():
        gsend[...] = gy
        g_half.start()

    def relay(k):
        h_relay(outward(k)).wait_recv()
        h_relay(outward(k)).start()

    @pl.when(center)
    def _():
        with jax.named_scope("relay"):
            relay(1)
            relay(2)
            total = gy
            for k in range(1, NZ // 2):
                rcopy(gsend, gbuf.at[k], g_s, g_r.at[k], (inner, m)).wait_recv()
                total = total + gbuf[k]
            gsend[...] = total
            gbuf[NZ // 2] = total
            g_other.start()
            relay(3)

        def late(e, carry):
            warp_late(e)
            return carry

        @pl.when(across)
        def _():
            send_far_told()

        lax.fori_loop(0, LATE_CHUNKS - 1, late, 0)

        @pl.when(jnp.logical_not(across))
        def _():
            warp_late(LATE_CHUNKS - 1)

    late_from = jnp.where(center, -LATE_CHUNKS, LATE)
    late_far = jnp.where(across, by_depth(LATE_FAR), -1)
    late_near = LATE_CHUNKS - jnp.where(across, 1, 0)
    send_far_step = jnp.where(across & jnp.logical_not(seam), by_depth(SEND_FAR), -1)

    def rows_of(q):
        return pl.ds(q * SUB_ROWS, SUB_ROWS)

    def c_copy(t, q):
        dst = cbuf.at[0, t, rows_of(q)]
        return rcopy(cout.at[t, rows_of(q)], dst, c_s, c_r.at[t, q], (inner, m))

    def cx_copy(t, q):
        dst = cbuf.at[1, t, rows_of(q)]
        return rcopy(cout.at[t, rows_of(q)], dst, c_s, x_r.at[t, q], (inner, m))

    def c_send(t, q):
        @pl.when(center)
        def _():
            cx_copy(t, q).start()

        @pl.when(jnp.logical_not(center))
        def _():
            c_copy(t, q).start()

    def h_copy(t, q, dev):
        part = hbuf.at[t, rows_of(q)]
        return rcopy(part, part, h_s, x_r.at[t, q], dev)

    def step(i, carry):
        @pl.when(i < NP)
        def _():
            t = piece(i)
            with jax.named_scope("ywait"):
                rcopy(wg.at[t], wg.at[t], y_s.at[0], y_r.at[t], y_dev(1)).wait_recv()
            mine = ws[:, pl.ds(own_bins(t), PW)]
            w_hi, w_lo = halves(jnp.concatenate([mine, wg[t].reshape(GROUP - ROWS, PW)], axis=0))
            both = jnp.concatenate([w_hi, w_lo], axis=0)
            wgb[t] = both
            n = jnp.dot(lhs[...], jnp.concatenate([both, w_hi], axis=0), preferred_element_type=F32)

            @pl.when(i == send_far_step)
            def _():
                send_far_told()

            @pl.when(has_outer)
            def _():
                for q in range(SUB):
                    with jax.named_scope("cwait"):
                        c_copy(t, q).wait_recv()
                    part = n[q * SUB_ROWS : (q + 1) * SUB_ROWS]
                    cout[t, rows_of(q)] = part + cbuf[0, t, rows_of(q)]
                    c_send(t, q)

            @pl.when(jnp.logical_not(has_outer))
            def _():
                cout[t] = n
                for q in range(SUB):
                    c_send(t, q)

            late = i - late_from

            @pl.when(((late >= 0) & (late < late_near)) | (i == late_far))
            def _():
                warp_late(jnp.where(i == late_far, LATE_CHUNKS - 1, late))

        k = i - lag

        @pl.when((k >= 0) & (k < NP))
        def _():
            t = piece(k)

            @pl.when(center)
            def _():
                zq, j = lax.div(t, NPZ), lax.rem(t, NPZ)

                @pl.when(k == 0)
                def _():
                    g_other.wait_recv()
                    gbuf[NZ // 2] = gbuf[NZ // 2] + gbuf[0]

                @pl.when((j == 0) & (lax.div(zq, NZ // 2) != lax.div(z, NZ // 2)))
                def _():
                    with jax.named_scope("hcwait"):
                        h_relay(zq).wait_recv()

                own = hc[zq, :, pl.ds(pl.multiple_of(j * PW, 128), PW)]
                bottom = jnp.dot(gbuf[NZ // 2], own, precision=exact_mode, preferred_element_type=F32) + EPSILON
                ratio = own / bottom
                for q in range(SUB):
                    with jax.named_scope("xcwait"):
                        cx_copy(t, q).wait_recv()
                    r = rows_of(q)
                    hbuf[t, r] = ratio[q * SUB_ROWS : (q + 1) * SUB_ROWS] * (cout[t, r] + cbuf[1, t, r])

                    @pl.when(k >= NP - DIRECT)
                    def _():
                        for far_out in (3, 2):
                            h_copy(t, q, (outward(far_out) * NY + y, m)).start()

                    h_copy(t, q, (outer, m)).start()

            @pl.when(jnp.logical_not(center))
            def _():
                for q in range(SUB):
                    with jax.named_scope("hwait"):
                        h_copy(t, q, (outer, m)).wait_recv()

                    @pl.when(has_outer & (k < NP - DIRECT))
                    def _():
                        h_copy(t, q, (outer, m)).start()

            h = hbuf[t]
            h_hi, h_lo = halves(h)
            right = jnp.concatenate([h_hi, h_lo], axis=0)
            left = jnp.concatenate([wgb[t], right], axis=0)
            acc[...] += lax.dot_general(left, right, NT, preferred_element_type=F32)

            @pl.when(lax.div(t, NPZ) == z)
            def _():
                hout_ref[:, pl.ds(pl.multiple_of(lax.rem(t, NPZ) * PW, 128), PW)] = h

        return carry

    lax.fori_loop(0, NP + LAGS[-1], step, 0)

    both = acc[:, 0:RANK] + acc[:, RANK : 2 * RANK]
    proj = both[0:GROUP] + both[GROUP : 2 * GROUP]
    base = 2 * GROUP
    gram = both[base : base + RANK] + both[base + RANK : base + 2 * RANK]
    gram8 = jnp.concatenate([gram[8 * q : 8 * q + 8] for q in range(4)], axis=1)
    for k in range(NY):
        rows = proj[k * ROWS : (k + 1) * ROWS]
        t0s[k, 0:8] = gram8
        t0s[k, 8:12] = jnp.concatenate([rows[4 * q : 4 * q + 4] for q in range(4)], axis=1)
    t0_copy = rcopy(t0s, t0r, t0_s, t0_r, partner)
    t0_copy.start()
    with jax.named_scope("t0wait"):
        t0_copy.wait_recv()
    t1s[...] = t0s[...] + t0r[...]

    me = y * 4 + lax.div(ml, 2)

    def t_copy(k):
        return rcopy(t1s.at[lax.div(k, 4)], t1r.at[me], t1_s.at[k], t1_r.at[k], plane_dev(k))

    t1_copies = [t_copy(k) for k in range(1, CHIPS)]
    for c in t1_copies:
        c.start()
    t1r[me] = t1s[0]
    with jax.named_scope("t1wait"):
        for c in t1_copies:
            c.wait_recv()
    sums = [t1r[k] for k in range(CHIPS)]
    while len(sums) > 1:
        sums = [a + b for a, b in zip(sums[::2], sums[1::2])]
    t3s[...] = sums[0]
    @pl.when(jnp.logical_not(seam))
    def _():
        pl.semaphore_wait(told, 1)

    t3_copy = rcopy(t3s, t3r, t3_s, t3_r, far)
    t3_copy.start()
    with jax.named_scope("t3wait"):
        t3_copy.wait_recv()
    total = sums[0] + t3r[...]
    gram_sum = jnp.concatenate([total[0:8, 32 * q : 32 * q + 32] for q in range(4)], axis=0)
    proj_sum = jnp.concatenate([total[8:12, 32 * q : 32 * q + 32] for q in range(4)], axis=0)
    f = f_ref[...]
    g_hi, g_lo = halves(gram_sum)
    own_hi, own_lo = halves(f)
    bottom = EPSILON + jnp.dot(
        jnp.concatenate([own_hi, own_hi, own_lo], axis=1),
        jnp.concatenate([g_hi, g_lo, g_hi], axis=0),
        preferred_element_type=F32,
    )
    w_ref[...] = f * proj_sum / bottom

    rcopy(fbuf, fbuf, f_s, f_r, y_dev(1)).wait_send()
    for c in t1_copies + [t0_copy, t3_copy]:
        c.wait_send()

    @pl.when(m < 15)
    def _():
        to_right.wait_send()

    @pl.when(m > 0)
    def _():
        to_left.wait_send()

    g_half.wait_send()
    h_part.wait_send()

    @pl.when(center)
    def _():
        part = hc.at[pl.ds(0, NZ // 2 - 1)]
        rcopy(part, part, hc_s, hc_s, (inner, m)).wait_send()

    for r in range(1, NY):
        rcopy(wg.at[:, r - 1], wg.at[:, r - 1], y_s.at[r - 1], y_s.at[r - 1], y_dev(r)).wait_send()
    rcopy(cout, cout, c_s, c_s, (inner, m)).wait_send()

    def h_sent(pieces):
        part = hbuf.at[pl.ds(0, pieces)]
        rcopy(part, part, h_s, h_s, (outer, m)).wait_send()

    @pl.when(center)
    def _():
        h_sent(NP)
        h_sent(2 * DIRECT)

    @pl.when(has_outer & jnp.logical_not(center))
    def _():
        h_sent(NP - DIRECT)


def body(spectra, shifts, fractions, pixel_factors, spectral_factors):
    vmem = pl.BlockSpec(memory_space=pltpu.VMEM)
    dma = pltpu.SemaphoreType.DMA
    return pl.pallas_call(
        kernel,
        out_shape=(
            pltpu.VMEM((ROWS, RANK), F32),
            pltpu.VMEM((RANK, OWN), F32),
        ),
        in_specs=[pl.BlockSpec(memory_space=pltpu.HBM)] * 5,
        out_specs=(vmem, vmem),
        scratch_shapes=[
            pltpu.VMEM((ROWS, SEGS), jnp.int32),
            pltpu.VMEM((ROWS, SEGS), F32),
            pltpu.VMEM((ROWS, RANK), F32),
            pltpu.VMEM((RANK, OWN), F32),
            pltpu.VMEM((ROWS, BINS + 256), F32),
            pltpu.VMEM((SEGS, ROWS, 128), jnp.int32),
            pltpu.VMEM((SEGS, ROWS, 128), F32),
            pltpu.VMEM((ROWS, BINS), F32),
            pltpu.VMEM((NP, NY - 1, ROWS, PW), F32),
            pltpu.VMEM((NP, 2 * GROUP, PW), BF16),
            pltpu.VMEM((2, NP, RANK, PW), F32),
            pltpu.VMEM((NP, RANK, PW), F32),
            pltpu.VMEM((NP, RANK, PW), F32),
            pltpu.VMEM((NZ, RANK, OWN), F32),
            pltpu.VMEM((NY - 1, ROWS, 128), F32),
            pltpu.VMEM((RANK, 3 * GROUP), BF16),
            pltpu.VMEM((RANK, RANK), F32),
            pltpu.VMEM((NZ // 2 + 1, RANK, RANK), F32),
            pltpu.VMEM((2 * GROUP + 2 * RANK, 2 * RANK), F32),
            pltpu.VMEM((ROWS, 128), F32),
            pltpu.VMEM((NY, 12, 128), F32),
            pltpu.VMEM((NY, 12, 128), F32),
            pltpu.VMEM((NY, 12, 128), F32),
            pltpu.VMEM((CHIPS, 12, 128), F32),
            pltpu.VMEM((12, 128), F32),
            pltpu.VMEM((12, 128), F32),
            dma((7,)),
            dma((2,)),
            dma((2,)),
            dma(()),
            dma(()),
            dma(()),
            dma((NZ,)),
            dma(()),
            dma((NZ // 2,)),
            dma((NY - 1,)),
            dma((NP,)),
            dma(()),
            dma((NP, SUB)),
            dma(()),
            dma((NP, SUB)),
            dma(()),
            dma(()),
            dma((CHIPS,)),
            dma((CHIPS,)),
            dma(()),
            dma(()),
            pltpu.SemaphoreType.REGULAR,
            pltpu.SemaphoreType.REGULAR,
            pltpu.SemaphoreType.REGULAR,
            pltpu.SemaphoreType.REGULAR,
        ],
        compiler_params=pltpu.CompilerParams(
            collective_id=0, has_side_effects=True, vmem_limit_bytes=66_000_000
        ),
    )(spectra, shifts, fractions, pixel_factors, spectral_factors)


def solution(mesh):
    return jax.shard_map(
        body,
        mesh=mesh,
        in_specs=(
            P("pix", "mz"),
            P("pix", "mz"),
            P("pix", "mz"),
            P("pix", None),
            P(None, ("mz", "pix")),
        ),
        out_specs=(P("pix", None), P(None, ("mz", "pix"))),
        check_vma=False,
    )
```
